128 devices in a mesh: batch: 1, col: 16 (over z, y), row: 8 (over x, core).
Axes of the slice: x: 4, y: 4, z: 4, core: 2. Of those that a mesh axis runs over, the one named last changes fastest.
Arguments:
- chol_fac: float32 [8192, 8192], P(('batch', 'row'), 'col')
- chol_bar: float32 [8192, 8192], P(('batch', 'row'), 'col')
Outputs:
- output: float32 [8192, 8192], P(('batch', 'row'), 'col')
All inputs are finite; a program needn't handle non-finite values.
Results may differ from the reference program's by a relative error of at most 0.001.
Values are sent between devices in bfloat16 or wider.
A program may use at most 1 GiB of HBM per device.

```python
import jax
import jax.numpy as jnp
from jax import lax

BLOCK_SIZE = 128
FEAT_DIM = 77
ROW_DEVS = 8
COL_DEVS = 16
MAT_SIZE = 8192

ROW_BLOCKS = MAT_SIZE // (BLOCK_SIZE * ROW_DEVS)
COL_BLOCKS = MAT_SIZE // (BLOCK_SIZE * COL_DEVS)


def to_stored(matrix):
    rows_done = matrix.reshape(ROW_BLOCKS, ROW_DEVS, BLOCK_SIZE, MAT_SIZE).transpose(1, 0, 2, 3).reshape(MAT_SIZE, MAT_SIZE)
    return rows_done.reshape(MAT_SIZE, COL_BLOCKS, COL_DEVS, BLOCK_SIZE).transpose(0, 2, 1, 3).reshape(MAT_SIZE, MAT_SIZE)


def from_stored(matrix):
    rows_done = matrix.reshape(ROW_DEVS, ROW_BLOCKS, BLOCK_SIZE, MAT_SIZE).transpose(1, 0, 2, 3).reshape(MAT_SIZE, MAT_SIZE)
    return rows_done.reshape(MAT_SIZE, COL_DEVS, COL_BLOCKS, BLOCK_SIZE).transpose(0, 2, 1, 3).reshape(MAT_SIZE, MAT_SIZE)


def phi_part(matrix):
    idx_row = jnp.arange(matrix.shape[-2])[:, None]
    idx_col = jnp.arange(matrix.shape[-1])[None, :]
    return jnp.where(idx_row > idx_col, matrix, jnp.where(idx_row == idx_col, 0.5 * matrix, 0.0))


def setup_inputs(seed: int = 0, part: int = 0) -> dict:
    base_key = jax.random.fold_in(jax.random.key(seed), part)
    point_key, bar_key = jax.random.split(base_key)
    points = jax.random.normal(point_key, (MAT_SIZE, FEAT_DIM), jnp.float32)
    sq_norm = jnp.sum(points * points, axis=1)
    cross_dot = jnp.dot(points, points.T, precision=lax.Precision.HIGHEST, preferred_element_type=jnp.float32)
    dist_sq = jnp.maximum(sq_norm[:, None] + sq_norm[None, :] - 2.0 * cross_dot, 0.0)
    kernel = jnp.exp(-0.5 * dist_sq / FEAT_DIM) + 0.5 * jnp.eye(MAT_SIZE, dtype=jnp.float32)
    low_fac = jnp.tril(jnp.linalg.cholesky(kernel))
    low_bar = jnp.tril(jax.random.normal(bar_key, (MAT_SIZE, MAT_SIZE), jnp.float32))
    return {'chol_fac': to_stored(low_fac), 'chol_bar': to_stored(low_bar)}


def reference(chol_fac, chol_bar):
    low_fac = from_stored(chol_fac)
    low_bar = from_stored(chol_bar)
    inner_mat = phi_part(jnp.dot(low_fac.T, low_bar, precision=lax.Precision.HIGHEST, preferred_element_type=jnp.float32))
    left_solved = lax.linalg.triangular_solve(low_fac, inner_mat, left_side=True, lower=True, transpose_a=True)
    full_grad = lax.linalg.triangular_solve(low_fac, left_solved, left_side=False, lower=True)
    return to_stored(phi_part(full_grad + full_grad.T))
```

```python
import jax
import jax.numpy as jnp
from jax import lax
from jax.experimental import pallas as pl
from jax.experimental.pallas import tpu as pltpu
from jax.sharding import PartitionSpec as P

B, Q, H, K, N = 128, 256, 512, 1024, 2048
U, R = 4, 8
GROUPS = tuple(range(U))
OFF = tuple(K * u - B * u * (u - 1) for u in GROUPS)
ROWS = OFF[-1] + Q
HI = lax.Precision.HIGHEST
MESH = pl.DeviceIdType.MESH
VM = pl.BlockSpec(memory_space=pltpu.VMEM)
HB = pl.BlockSpec(memory_space=pl.ANY)
ALL = slice(None)


def mm(a, b):
    return jnp.dot(a, b, precision=HI, preferred_element_type=jnp.float32)


def mm_t(a, b):
    return lax.dot_general(a, b, (((0,), (0,)), ((), ())), precision=HI, preferred_element_type=jnp.float32)


def mod4(v):
    return lax.rem(v + U, U)


def at(start, size=B):
    return pl.ds(start if isinstance(start, int) else pl.multiple_of(start, B), size)


def group(u):
    return slice(OFF[u], OFF[u] + K - Q * u)


def wide(ref, rows, zs=GROUPS):
    return jnp.concatenate([ref[z, rows] for z in zs], axis=1)


def phi(block, ahead):
    diff = B * ahead + lax.broadcasted_iota(jnp.int32, (B, B), 0) - lax.broadcasted_iota(jnp.int32, (B, B), 1)
    return jnp.where(diff > 0, block, jnp.where(diff == 0, 0.5 * block, 0.0))


def step(g):
    return next(g, g) is not g


def run(*gathers, behind=()):
    live = list(gathers)
    while live:
        live = [g for g in live if step(g)]
        for g in behind:
            step(g)


def chain(*gathers):
    for g in gathers:
        step(g)
        yield


class Net:
    def __init__(self, send_sems, recv_sems):
        self.send_sems, self.recv_sems = send_sems, recv_sems
        self.r, self.c = lax.axis_index('row'), lax.axis_index('col')
        self.x, self.core = self.r // 2, lax.rem(self.r, 2)
        self.z, self.y = self.c // U, lax.rem(self.c, U)
        self.right, self.left = self.device(x=mod4(self.x + 1)), self.device(x=mod4(self.x - 1))
        self.partner = self.device(core=1 - self.core)
        self.zy = [self.device(y=mod4(self.y + 1)), self.device(y=mod4(self.y - 1)),
                   self.device(z=mod4(self.z + 1)), self.device(z=mod4(self.z - 1))]
        self.far_z = self.device(z=mod4(self.z + 2))
        self.copies = []

    def device(self, **place):
        x, core, y, z = [place.get(k, getattr(self, k)) for k in ('x', 'core', 'y', 'z')]
        return {'col': U * z + y, 'row': 2 * x + core}

    def barrier(self, *peers):
        sem = pltpu.get_barrier_semaphore()
        for peer in peers:
            pl.semaphore_signal(sem, inc=1, device_id=peer, device_id_type=MESH)
        pl.semaphore_wait(sem, len(peers))

    def line(self):
        places = [(mod4(self.x + d // 2), lax.rem(self.core + d, 2)) for d in range(1, R)]
        return [(self.device(x=x, core=core), 2 * x + core) for x, core in places]

    def plane(self):
        places = [(mod4(self.z + d // U), mod4(self.y + d % U)) for d in range(1, U * U)]
        return [(self.device(z=z, y=y), U * z + y) for z, y in places]

    def copy(self, ref, peer, dst=None):
        k = len(self.copies)
        copy = pltpu.make_async_remote_copy(
            src_ref=ref, dst_ref=ref if dst is None else dst, send_sem=self.send_sems.at[k], recv_sem=self.recv_sems.at[k],
            device_id=peer, device_id_type=MESH)
        copy.start()
        self.copies.append(copy)
        return copy

    def drain(self):
        for copy in self.copies:
            copy.wait_send()

    def gather_x(self, ref, axis=1, first=0):
        half = ref.shape[1 - axis] // 2

        def view(r, part=None):
            other = ALL if part is None else pl.ds(part * half, half)
            return ref.at[(other, first + r) if axis else (r, other)]

        near_r, near_l, far = [2 * mod4(self.x + d) + self.core for d in (1, -1, 2)]
        to_right, to_left = self.copy(view(self.r), self.right), self.copy(view(self.r), self.left)
        over = [self.copy(view(self.r), self.partner)]
        yield
        to_right.wait_recv()
        far_0 = self.copy(view(near_l, 0), self.right)
        over.append(self.copy(view(near_l), self.partner))
        to_left.wait_recv()
        far_1 = self.copy(view(near_r, 1), self.left)
        over.append(self.copy(view(near_r), self.partner))
        yield
        far_0.wait_recv()
        over.append(self.copy(view(far, 0), self.partner))
        far_1.wait_recv()
        over.append(self.copy(view(far, 1), self.partner))
        yield
        for copy in over:
            copy.wait_recv()
        yield

    def gather_zy(self, ref, start, count):
        yp, ym, zp, zm = self.zy
        y, z, n = self.y, self.z, count // U
        y_m, y_p, z_m, z_p = mod4(y - 1), mod4(y + 1), mod4(z - 1), mod4(z + 1)

        def view(zs, part, ys=None, parts=1):
            return ref.at[zs, pl.ds(start + part * n, parts * n), ALL if ys is None else at(B * ys)]

        def both(first, second, to_first, to_second):
            return self.copy(first, to_first), self.copy(second, to_second)

        a = both(view(z, 0, y, 2), view(z, 0, y, 2), yp, ym)
        b = both(view(z, 2, y, 2), view(z, 2, y, 2), zp, zm)
        yield
        for copy in a:
            copy.wait_recv()
        a = both(view(z, 0, y_m), view(z, 1, y_p), yp, ym)
        for copy in b:
            copy.wait_recv()
        b = both(view(z_m, 2, y), view(z_p, 3, y), zp, zm)
        yield
        for copy in a:
            copy.wait_recv()
        a = both(view(z, 0, None, 2), view(z, 0, None, 2), zp, zm)
        for copy in b:
            copy.wait_recv()
        b = both(view(ALL, 2, y, 2), view(ALL, 2, y, 2), yp, ym)
        yield
        for copy in a:
            copy.wait_recv()
        a = both(view(z_m, 0), view(z_p, 1), zp, zm)
        for copy in b:
            copy.wait_recv()
        b = both(view(ALL, 2, y_m), view(ALL, 3, y_p), yp, ym)
        yield
        for copy in (*a, *b):
            copy.wait_recv()
        yield

    def gather_y(self, ref, start, count):
        half, y = count // 2, self.y
        yp, ym = self.zy[:2]

        def view(ys, part=None):
            return ref.at[pl.ds(start, count) if part is None else pl.ds(start + part * half, half), at(B * ys)]

        near = self.copy(view(y), yp), self.copy(view(y), ym)
        yield
        near[0].wait_recv()
        far_0 = self.copy(view(mod4(y - 1), 0), yp)
        near[1].wait_recv()
        far_1 = self.copy(view(mod4(y + 1), 1), ym)
        yield
        far_0.wait_recv()
        far_1.wait_recv()
        yield

    def spread_z(self, *parts):
        sent = []
        for d, peer in ((1, self.zy[2]), (-1, self.zy[3]), (2, self.far_z)):
            for src, dst in parts:
                sent.append((self.copy(src(mod4(self.z + d)), peer, dst(self.z)), dst(mod4(self.z - d))))
        yield
        over = []
        for copy, got in sent:
            copy.wait_recv()
            over.append(self.copy(got, self.partner))
        yield
        for copy in over:
            copy.wait_recv()
        yield

    def transpose(self, a, b, d, out):
        def on_line(k):
            return ALL, k

        def on_plane(k):
            return k // R, lax.rem(k, R)

        line, plane = (self.line(), self.r, on_line), (self.plane(), self.c, on_plane)
        for src, dst, (others, me, piece) in ((a, b, line), (b, d, plane), (d, out, line)):
            sent = [self.copy(src.at[piece(place)], peer, dst.at[piece(me)]) for peer, place in others]
            dst[piece(me)] = src[piece(me)]
            yield
            for copy in sent:
                copy.wait_recv()
        yield

    def reduce(self, acc, fwd, end, start, count, put, terms=None, width=None):
        half, lanes = count // 2, ALL if width is None else pl.ds(0, width)
        rows, lo, hi, mid = pl.ds(start, count), pl.ds(start, half), pl.ds(start + half, half), pl.ds(start // 2, half)
        me, right, left = (self.z, *self.zy[2:]) if terms is None else (self.x, self.right, self.left)
        far, nxt, prv = [mod4(me + d) for d in (2, 1, -1)]
        if terms is not None:
            over = self.copy(terms.at[:, 1 - self.core, rows, lanes], self.partner, acc.at[:, rows, lanes])
            yield
            over.wait_recv()

        def settle(k):
            if terms is not None:
                acc[k, rows, lanes] = acc[k, rows, lanes] + terms[k, self.core, rows, lanes]

        def send(k, part, to, ref, slot):
            return self.copy(acc.at[k, part, lanes], to, ref.at[slot, mid, lanes])

        settle(far)
        far_r, far_l = send(far, lo, right, fwd, 0), send(far, hi, left, fwd, 1)
        settle(nxt)
        settle(prv)
        last = [send(nxt, hi, right, end, 0), send(prv, lo, left, end, 1)]
        settle(me)
        yield
        far_r.wait_recv()
        acc[nxt, lo, lanes] = acc[nxt, lo, lanes] + fwd[0, mid, lanes]
        last.append(send(nxt, lo, right, end, 2))
        far_l.wait_recv()
        acc[prv, hi, lanes] = acc[prv, hi, lanes] + fwd[1, mid, lanes]
        last.append(send(prv, hi, left, end, 3))
        yield
        for copy in last:
            copy.wait_recv()
        blocks = count // B
        for k in range(blocks):
            one, two = (1, 2) if 2 * k < blocks else (0, 3)
            row = pl.ds(start // 2 + B * (k % (blocks // 2)), B)
            put(k, acc[me, pl.ds(start + B * k, B), lanes] + (end[one, row, lanes] + end[two, row, lanes]))
        yield


def invert(w_ref, l_ref, tmp_ref):
    row = lax.broadcasted_iota(jnp.int32, (Q, Q), 0)
    col = lax.broadcasted_iota(jnp.int32, (Q, Q), 1)
    w_ref[...] = jnp.zeros_like(w_ref)

    def block(ref, i, j, size):
        return ref[i // B:(i + size) // B, :, j:j + size].reshape(size, size)

    def put(i, j, size, val):
        w_ref[i // B:(i + size) // B, :, j:j + size] = val.reshape(size // B, B, size)

    corners = range(0, K, Q)
    for k in corners:
        a = block(l_ref, k, k, Q)
        diag = jnp.where(row == col, a, 0.0)
        down, across = 1.0 / jnp.sum(diag, axis=1, keepdims=True), 1.0 / jnp.sum(diag, axis=0, keepdims=True)
        low = (row // 2 == col // 2) & (row > col)
        put(k, k, Q, jnp.where(row == col, down, jnp.where(low, -a * down * across, 0.0)))
    size = 2
    while size < Q:
        pair = (row // (2 * size) == col // (2 * size)) & (row // size > col // size)
        for k in corners:
            tmp_ref[k // Q] = mm(jnp.where(pair, block(l_ref, k, k, Q), 0.0), block(w_ref, k, k, Q))
        yield
        for k in corners:
            w = block(w_ref, k, k, Q)
            put(k, k, Q, w - mm(w, tmp_ref[k // Q]))
        yield
        size *= 2
    while size < K:
        for j in range(0, K, 2 * size):
            i = j + size
            part = mm(block(l_ref, i, j, size), block(w_ref, j, j, size))
            put(i, j, size, -mm(block(w_ref, i, i, size), part))
            yield
        size *= 2


def inner(net, u, start, panel, top, bar, terms):
    def two(k, _):
        h, x = k // U, lax.rem(k, U)
        p = mm_t(panel[2 * h + x // 2, top:top + K - Q * u, at(Q * lax.rem(x, 2), Q)], bar[Q * u:, :B * (u + 1)])
        for e in range(2):
            for v in range(u + 1):
                val = p[B * e:B * (e + 1), B * v:B * (v + 1)]
                terms[x, e, at(start + Q * v + B * h), :] = phi(val, 2 * k + e - net.c) if v == u else val
        return 0

    lax.fori_loop(0, R, two, 0)


def front_kernel(l_ref, bar_ref, lr_ref, col_ref, s_ref, lv, lss, wss, tmp, terms, acc, fwd, end, dma_sems, send_sems, recv_sems):
    net = Net(send_sems, recv_sems)
    r, c, y, z, core = net.r, net.c, net.y, net.z, net.core
    half, zz = z // 2, lax.rem(z, 2)
    ways = (1, 2, 3)
    others = [net.device(y=mod4(y + d)) for d in ways]
    net.barrier(net.right, net.left, net.partner, *others, *net.zy[2:])

    strip = at(B * (U * zz + y))

    def own(u):
        return at(B * (2 * u + half)), at(B * u)

    sent = [net.copy(l_ref.at[own(mod4(y + d))], other, lss.at[r, :, strip]) for d, other in zip(ways, others)]
    lss[r, :, strip] = l_ref[own(y)]
    for u in GROUPS:
        lv[z, group(u), at(B * y)] = l_ref[Q * u:, B * u:B * (u + 1)]
    g = [net.gather_zy(lv, OFF[u], K - Q * u) for u in GROUPS]
    run(chain(g[3], g[2]))
    for copy in sent:
        copy.wait_recv()
    pair = net.copy(lss.at[r, :, at(H * zz, H)], net.device(z=2 * half + 1 - zz))
    run(chain(g[1], g[0], g[3], g[3]))
    pair.wait_recv()

    order = iter([2, 2, 3, 1, 3, 2, 1, 2, 0, 1, 0, 1, 0, 0])
    stores = []

    def tick():
        u = next(order, None)
        if u is not None:
            step(g[u])

    def keep(u):
        stores.append(pltpu.make_async_copy(lv.at[:, group(u)], lr_ref.at[:, group(u)], dma_sems.at[u]))
        stores[-1].start()

    def begin(u):
        start = ROWS - Q * (u + 1) * (u + 2) // 2
        inner(net, u, start, lv, OFF[u], bar_ref, terms)

        def put(k, val):
            v, h = k // 2, k % 2
            s_ref[h, B * (u * (u + 1) // 2 + v):B * (u * (u + 1) // 2 + v + 1), :] = val

        keep(u)
        return net.reduce(acc, fwd, end, start, Q * (u + 1), put, terms)

    strips = net.gather_x(lss, axis=0)
    step(strips)
    for _ in range(3):
        tick()
    step(strips)
    for _ in range(2):
        tick()
    step(strips)
    s3 = begin(3)
    run(strips)
    step(s3)
    for k, _ in enumerate(invert(wss, lss, tmp)):
        if k % 4 == 1:
            tick()
        if k % 6 == 5:
            step(s3)
    s2 = begin(2)
    step(s2)
    tick()

    mine = pl.ds(U * core, U)
    sent = [net.copy(wss.at[mine, :, at(B * (U * zz + mod4(y + d)))], other, col_ref.at[y, mine]) for d, other in zip(ways, others)]
    col_ref[y] = wss[:, :, strip]
    step(s2)
    tick()
    tick()
    s1 = begin(1)
    run(s3, s2)
    over = []
    for d, copy in zip(ways, sent):
        copy.wait_recv()
        over.append(net.copy(col_ref.at[mod4(y - d), mine], net.partner))
    run(s1)
    for _ in range(U):
        tick()
    keep(0)
    for copy in over:
        copy.wait_recv()
    for copy in stores:
        copy.wait()
    net.drain()


def levels_kernel(lr_ref, bar_ref, wc_ref, s_ref, sy_ref, w_ref, row_e, row_d, row_o, col_3,
                  own, a, b, d, back, la, lb, l0, l1, bv, cd, re, rd, co, ro, c3, x1, x2, x3, terms, acc, fwd, end, dma_sems, send_sems, recv_sems):
    net = Net(send_sems, recv_sems)
    r, c, y, z = net.r, net.c, net.y, net.z
    sems = iter(range(32))

    def local(a, b):
        copy = pltpu.make_async_copy(a, b, dma_sems.at[next(sems)])
        copy.start()
        return copy

    load_s = local(s_ref, a)
    load_0 = [local(lr_ref.at[:, group(0)], l0), local(bar_ref.at[:, 0:B], bv)]
    load_a = [local(lr_ref.at[0:2, OFF[u] + B:OFF[u] + Q], la.at[:, B * u:B * (u + 1)]) for u in GROUPS]
    load_b = [local(lr_ref.at[:, OFF[u] + Q:OFF[u] + H], lb.at[:, B * u:B * (u + 2)]) for u in (0, 2)]
    load_c = local(lr_ref.at[:, OFF[1] + Q:OFF[2]], l1)
    net.barrier(*[peer for peer, _ in net.line() + net.plane()])
    piece = a.shape[2]

    def block(ref, k, u, v):
        top = B * (u * (u + 1) // 2 + v)
        i, low = top // piece, top % piece
        first = ref[k, i, low:low + B]
        return first if low + B <= piece else jnp.concatenate([first, ref[k, i + 1, :low + B - piece]], axis=0)

    low = c < R
    stores = []
    for u in GROUPS:
        re[z, B * u:B * (u + 1), at(B * y)] = wc_ref[u, r]
    diag = net.gather_zy(re, 0, H)
    step(diag)
    load_s.wait()
    for u in range(1, U):
        for h in range(2):
            for v in range(u + 1):
                own[v, B * (2 * u + h):B * (2 * u + h + 1), :] = block(a, h, u, v)
    places = [local(own.at[v, Q * (v + 1):], sy_ref.at[K * v + Q * (v + 1):K * (v + 1), at(B * y)]) for v in range(U - 1)]
    for place in places:
        place.wait()
    early = [net.gather_y(sy_ref, K * v + Q * (v + 1), K - Q * (v + 1)) for v in range(U - 1)]
    late = [net.gather_y(sy_ref, K * v, Q * (v + 1)) for v in GROUPS]
    moves = chain(*[early[k] for k in (0, 1, 0, 2, 1, 0, 2, 1, 2)])
    half = pl.ds(2 * net.core, 2)
    step(moves)

    for u in GROUPS:
        load_a[u].wait()
        cd[u, 0:R] = jnp.where(low, wc_ref[u], 0.0)
        x1[u, r] = mm(wide(la, slice(B * u, B * (u + 1)), (0, 1)), cd[u, 0:R].reshape(K, B))
    strips = net.gather_x(x1)
    step(strips)
    for load in load_0:
        load.wait()
    inner(net, 0, 0, l0, 0, bv, terms)

    def put(k, val):
        a[k, 0, :B] = val

    run(strips, net.reduce(acc, fwd, end, 0, Q, put, terms), diag)
    flip = net.transpose(a, b, d, back)
    step(flip)
    stores.append(local(re, row_e))
    for u in GROUPS:
        w = -mm(wide(re, slice(B * u, B * (u + 1)), (2, 3)), x1[u].reshape(K, B))
        w = jnp.where(low, w, wc_ref[u, r])
        cd[u, R + r] = w
        rd[z, B * u:B * (u + 1), at(B * y)] = w
    rows = net.gather_zy(rd, 0, H)
    step(rows)
    run(net.gather_x(cd, first=R), behind=[rows, moves])
    stores.append(local(cd.at[:, pl.ds(U * z, U)], w_ref.at[0:U, z]))
    out = net.spread_z((lambda k: cd.at[:, pl.ds(U * k + 2 * net.core, 2)], lambda k: w_ref.at[0:U, k, half]))
    step(out)
    moves = chain(moves, moves, moves, out, out)
    step(flip)

    for q in range(2):
        load_b[q].wait()
        x2[2 * q:2 * q + 2, r] = mm(wide(lb, slice(Q * q, Q * (q + 1))), cd[2 * q].reshape(N, B)).reshape(2, B, B)
    run(net.gather_x(x2), rows, behind=[moves])
    step(flip)
    stores.append(local(rd, row_d))
    for q in range(2):
        at_u = slice(B * (2 * q + 1), B * (2 * q + 2))
        tops = (mm(wide(re, at_u, (0, 1)), x2[2 * q].reshape(K, B)), mm(wide(rd, at_u), x2[2 * q:2 * q + 2].reshape(N, B)))
        for i, w in enumerate(tops):
            co[2 * q + i, r] = -w
            ro[z, B * (2 * q + i):B * (2 * q + i + 1), at(B * y)] = -w
    rows = net.gather_zy(ro, 0, H)
    step(rows)
    run(net.gather_x(co), behind=[rows, moves])
    run(moves)
    parts = []
    for q in range(2):
        stores.append(local(co.at[2 * q + z // 2, pl.ds(U * lax.rem(z, 2), U)], w_ref.at[U + q, z]))
        parts.append((lambda k, q=q: co.at[2 * q + k // 2, pl.ds(U * lax.rem(k, 2) + 2 * net.core, 2)],
                      lambda k, q=q: w_ref.at[U + q, k, half]))
    out = net.spread_z(*parts)
    step(out)

    load_c.wait()
    x3[:, r] = mm(wide(l1, ALL), jnp.concatenate([co[0:2].reshape(N, B), cd[1].reshape(N, B)], 1)).reshape(U, B, Q)
    x3[:, r, :, :B] = x3[:, r, :, :B] + mm(wide(l0, slice(H, K)), cd[0].reshape(N, B)).reshape(U, B, B)
    strips = net.gather_x(x3)
    step(strips)

    step(flip)
    for h in range(2):
        own[0, B * h:B * (h + 1), :] = block(a, h, 0, 0)
    for s in range(2):
        for u in GROUPS:
            for v in range(u + 1):
                at_t = slice(B * (2 * v + s), B * (2 * v + s + 1))
                val = block(back, s, u, v).T
                own[u, at_t, :] = own[u, at_t, :] + val if u == v else val
    places = [local(own.at[v, 0:Q * (v + 1)], sy_ref.at[K * v:K * v + Q * (v + 1), at(B * y)]) for v in GROUPS]
    run(strips, rows)
    for place in places:
        place.wait()
    moves = chain(*[late[k] for k in (3, 2, 3, 1, 2, 3, 0, 1, 2, 0, 1, 0)])
    step(moves)
    step(moves)
    stores.append(local(ro, row_o))
    for i in GROUPS:
        u = 2 + i // 2
        at_u = slice(B * u, B * (u + 1))
        if i % 2 == 0:
            w = mm(wide(re, at_u, (0, 1)), x3[i].reshape(K, Q))
        else:
            w = mm(wide(rd, at_u), x3[i - 1:i + 1].reshape(N, Q))
        if i >= 2:
            w = w + mm(wide(ro, slice(B * i, B * (i + 1))), x3[0:2].reshape(N, Q))
        c3[i, r] = -w
    run(net.gather_x(c3), out, behind=[moves])
    run(moves)
    stores.append(local(c3, col_3))
    for copy in stores:
        copy.wait()
    net.drain()


def product_kernel(sy_ref, w_ref, c3_ref, m_ref, sy, w, c3, wide_w, acc, fwd, end, dma_sems, send_sems, recv_sems):
    net = Net(send_sems, recv_sems)
    z = net.z
    load_3, *loads = [pltpu.make_async_copy(a, b, dma_sems.at[k])
                      for k, (a, b) in enumerate(((c3_ref, c3), (w_ref, w), (sy_ref, sy)))]
    for load in (load_3, *loads):
        load.start()
    net.barrier(*net.zy[2:], net.far_z, net.partner)
    load_3.wait()
    half = pl.ds(2 * net.core, 2)
    parts = []
    for v in range(2):
        wide_w[v, z] = c3[2 * v + z // 2, pl.ds(U * lax.rem(z, 2), U)]
        parts.append((lambda k, v=v: c3.at[2 * v + k // 2, pl.ds(U * lax.rem(k, 2) + 2 * net.core, 2)],
                      lambda k, v=v: wide_w.at[v, k, half]))
    out = net.spread_z(*parts)
    step(out)
    m_ref[...] = jnp.zeros_like(m_ref)

    def block(v, col):
        if v >= 2 and col < 2:
            some = [wide_w[v - 2, k, :, :, B * col:B * (col + 1)] for k in GROUPS]
        else:
            some = [w[v if v == col else U + v // 2, k] for k in GROUPS]
        return jnp.concatenate([x.reshape(H, B) for x in some], axis=1)

    def terms(u, col, groups, more=False):
        part = sum(mm(sy[K * v + Q * u:K * v + Q * (u + 1), :], block(v, col)) for v in groups)
        for k in GROUPS:
            place = k, slice(Q * u, Q * (u + 1)), slice(B * col, B * (col + 1))
            val = part[:, B * k:B * (k + 1)]
            acc[place] = acc[place] + val if more else val

    def sum_of(u):
        def put(k, val):
            m_ref[Q * u + B * k:Q * u + B * (k + 1), :B * (u + 1)] = val

        return net.reduce(acc, fwd, end, Q * u, Q, put, width=B * (u + 1))

    for load in loads:
        load.wait()
    for u in GROUPS:
        for col in range(u + 1):
            terms(u, col, range(col, U if col >= 2 else 2))
        if u == 2:
            step(out)
    run(out)
    sums = []
    for u in GROUPS[::-1]:
        for col in range(min(u + 1, 2)):
            terms(u, col, range(2, U), True)
        for s in sums:
            step(s)
        sums.append(sum_of(u))
        step(sums[-1])
    run(*sums)
    net.drain()


def gradient_kernel(x_ref, own_ref, re_ref, rd_ref, ro_ref, t_ref,
                    wr, terms, acc, fwd, end, dma_sems, send_sems, recv_sems):
    net = Net(send_sems, recv_sems)
    r, c = net.r, net.c
    loads = [[(re_ref.at[0:2, B * u:B * (u + 1)], wr.at[0:2, OFF[u]:OFF[u] + B]),
              (rd_ref.at[:, B * u:B * (u + 1)], wr.at[:, OFF[u] + B:OFF[u] + Q])] for u in GROUPS]
    loads[2] += [(ro_ref.at[:, Q:], wr.at[:, OFF[2] + Q:OFF[3]])]
    loads[0] += [(ro_ref.at[:, :Q], wr.at[:, Q:H])]
    sems = iter(range(16))
    loads = [[pltpu.make_async_copy(a, b, dma_sems.at[next(sems)]) for a, b in some] for some in loads]
    for some in loads[::-1]:
        for load in some:
            load.start()
    net.barrier(net.right, net.left, net.partner, *net.zy)
    for i in GROUPS:
        for k, top in enumerate((H, OFF[1] + Q)):
            wr[net.z, top + B * i:top + B * (i + 1), at(B * net.y)] = own_ref[i, :, B * k:B * (k + 1)]
    rows_0, rows_1 = net.gather_zy(wr, H, H), net.gather_zy(wr, OFF[1] + Q, H)
    step(rows_1)
    step(rows_0)
    t_ref[...] = jnp.zeros_like(t_ref)

    def half_of(u, h):
        width = B * (u + 1)

        def two(x, _):
            a = wr[2 * h + x // 2, group(u), at(Q * lax.rem(x, 2), Q)]
            part = mm_t(a, x_ref[Q * u:, :width])
            for e in range(2):
                terms[x, e, Q * u + B * h:Q * u + B * (h + 1), :width] = part[B * e:B * (e + 1)]
            return 0

        lax.fori_loop(0, U, two, 0)

    def sum_of(u):
        wr[2:, OFF[u]:OFF[u] + B] = jnp.zeros((2, B, H), jnp.float32)
        for load in loads[u]:
            load.wait()
        half_of(u, 0)
        yield
        half_of(u, 1)

        def put(k, val):
            t = 2 * u + k
            for v in range(u + 1):
                t_ref[B * t:B * (t + 1), B * v:B * (v + 1)] = phi(val[:, B * v:B * (v + 1)], R * t + r - 2 * R * v - c)

        yield
        yield from net.reduce(acc, fwd, end, Q * u, Q, put, terms, B * (u + 1))

    s0, s1, s2, s3 = [sum_of(u) for u in GROUPS]
    run(chain(s3, s3, s3, rows_1, s2, s3, rows_1, s2, rows_1, s3, s2, rows_1, s2, s3, rows_0, s1, s2, s1, s1, rows_0, s1, s2,
              rows_0, s1, rows_0, s0, s1, s0, s0, s0, s0))
    run(s2, s1, s0)
    net.drain()


def call(kernel, ident, flops, args, in_specs, outs, out_specs, scratch, sems):
    return pl.pallas_call(
        kernel,
        out_shape=[jax.ShapeDtypeStruct(s, jnp.float32) for s in outs],
        in_specs=in_specs,
        out_specs=out_specs,
        scratch_shapes=[*(pltpu.VMEM(s, jnp.float32) for s in scratch), *(pltpu.SemaphoreType.DMA(s) for s in sems)],
        compiler_params=pltpu.CompilerParams(collective_id=ident, has_side_effects=True, vmem_limit_bytes=67 * 10 ** 6),
        cost_estimate=pl.CostEstimate(flops=flops, bytes_accessed=K, transcendentals=0),
    )(*args)


def solution(mesh):
    def local_pass(fac, bar):
        panel, rows, column = (U, ROWS, H), (U, H, H), (U, R, B, B)
        wide_col, cut = (U, R, B, Q), (2, R, ROWS // (2 * R), B)
        lr, wc, s_own = call(
            front_kernel, 0, 1, (fac, bar), [VM] * 2, (panel, column, (2, ROWS // 2, B)), [HB, VM, VM],
            (panel, (R, B, K), (R, B, K), (U, Q, Q), (U, 2, ROWS, B), (U, ROWS, B), (2, ROWS // 2, B), (U, ROWS // 2, B)),
            ((U,), (128,), (128,)))
        sy, w, row_e, row_d, row_o, col_3 = call(
            levels_kernel, 1, 1, (lr, bar, wc, s_own.reshape(cut)), [HB, HB, VM, HB],
            ((U * K, H), (6, U, U, B, B), rows, rows, rows, wide_col), [HB] * 6,
            ((U, K, B), cut, cut, cut, cut, (2, H, H), rows, (U, K, H), rows, (K, B), (U, 2 * R, B, B), rows, rows, column, rows,
             wide_col, column, column, wide_col, (U, 2, Q, B), (U, Q, B), (2, B, B), (U, B, B)),
            ((48,), (192,), (192,)))
        own = lax.dynamic_index_in_dim(col_3, lax.axis_index('row'), 1, keepdims=False)
        m, = call(
            product_kernel, 2, 1, (sy, w, col_3), [HB] * 3, ((K, H),), [VM],
            ((U * K, H), (6, U, U, B, B), wide_col, (2, U, U, B, Q), (U, K, H), (2, H, H), (U, H, H)), ((4,), (48,), (48,)))
        out, = call(
            gradient_kernel, 3, 1, (m, own, row_e, row_d, row_o), [VM] * 2 + [HB] * 3, ((K, H),), [VM],
            (panel, (U, 2, K, H), (U, K, H), (2, H, H), (U, H, H)), ((16,), (64,), (64,)))
        return out

    spec = P(('batch', 'row'), 'col')
    return jax.shard_map(local_pass, mesh=mesh, in_specs=(spec, spec), out_specs=spec, check_vma=False)
```

```python
import jax
import jax.numpy as jnp
from jax import lax
from jax.experimental import pallas as pl
from jax.experimental.pallas import tpu as pltpu
from jax.sharding import PartitionSpec as P

B, Q, H, K, N = 128, 256, 512, 1024, 2048
U, R = 4, 8
GROUPS = tuple(range(U))
OFF = tuple(K * u - B * u * (u - 1) for u in GROUPS)
ROWS = OFF[-1] + Q
HI = lax.Precision.HIGHEST
MESH = pl.DeviceIdType.MESH
VM = pl.BlockSpec(memory_space=pltpu.VMEM)
HB = pl.BlockSpec(memory_space=pl.ANY)
ALL = slice(None)


def mm(a, b):
    return jnp.dot(a, b, precision=HI, preferred_element_type=jnp.float32)


def mm_t(a, b):
    return lax.dot_general(a, b, (((0,), (0,)), ((), ())), precision=HI, preferred_element_type=jnp.float32)


def mod4(v):
    return lax.rem(v + U, U)


def at(start, size=B):
    return pl.ds(start if isinstance(start, int) else pl.multiple_of(start, B), size)


def group(u):
    return slice(OFF[u], OFF[u] + K - Q * u)


def wide(ref, rows, zs=GROUPS):
    return jnp.concatenate([ref[z, rows] for z in zs], axis=1)


def phi(block, ahead):
    diff = B * ahead + lax.broadcasted_iota(jnp.int32, (B, B), 0) - lax.broadcasted_iota(jnp.int32, (B, B), 1)
    return jnp.where(diff > 0, block, jnp.where(diff == 0, 0.5 * block, 0.0))


def step(g):
    return next(g, g) is not g


def run(*gathers, behind=()):
    live = list(gathers)
    while live:
        live = [g for g in live if step(g)]
        for g in behind:
            step(g)


def chain(*gathers):
    for g in gathers:
        step(g)
        yield


class Net:
    def __init__(self, send_sems, recv_sems):
        self.send_sems, self.recv_sems = send_sems, recv_sems
        self.r, self.c = lax.axis_index('row'), lax.axis_index('col')
        self.x, self.core = self.r // 2, lax.rem(self.r, 2)
        self.z, self.y = self.c // U, lax.rem(self.c, U)
        self.right, self.left = self.device(x=mod4(self.x + 1)), self.device(x=mod4(self.x - 1))
        self.partner = self.device(core=1 - self.core)
        self.zy = [self.device(y=mod4(self.y + 1)), self.device(y=mod4(self.y - 1)),
                   self.device(z=mod4(self.z + 1)), self.device(z=mod4(self.z - 1))]
        self.far_z = self.device(z=mod4(self.z + 2))
        self.copies = []

    def device(self, **place):
        x, core, y, z = [place.get(k, getattr(self, k)) for k in ('x', 'core', 'y', 'z')]
        return {'col': U * z + y, 'row': 2 * x + core}

    def barrier(self, *peers):
        sem = pltpu.get_barrier_semaphore()
        for peer in peers:
            pl.semaphore_signal(sem, inc=1, device_id=peer, device_id_type=MESH)
        pl.semaphore_wait(sem, len(peers))

    def line(self):
        places = [(mod4(self.x + d // 2), lax.rem(self.core + d, 2)) for d in range(1, R)]
        return [(self.device(x=x, core=core), 2 * x + core) for x, core in places]

    def plane(self):
        places = [(mod4(self.z + d // U), mod4(self.y + d % U)) for d in range(1, U * U)]
        return [(self.device(z=z, y=y), U * z + y) for z, y in places]

    def copy(self, ref, peer, dst=None):
        k = len(self.copies)
        copy = pltpu.make_async_remote_copy(
            src_ref=ref, dst_ref=ref if dst is None else dst, send_sem=self.send_sems.at[k], recv_sem=self.recv_sems.at[k],
            device_id=peer, device_id_type=MESH)
        copy.start()
        self.copies.append(copy)
        return copy

    def drain(self):
        for copy in self.copies:
            copy.wait_send()

    def gather_x(self, ref, axis=1, first=0):
        half = ref.shape[1 - axis] // 2

        def view(r, part=None):
            other = ALL if part is None else pl.ds(part * half, half)
            return ref.at[(other, first + r) if axis else (r, other)]

        near_r, near_l, far = [2 * mod4(self.x + d) + self.core for d in (1, -1, 2)]
        to_right, to_left = [], []
        for part in range(2):
            to_right.append(self.copy(view(self.r, part), self.right))
            to_left.append(self.copy(view(self.r, 1 - part), self.left))
        over = [self.copy(view(self.r), self.partner)]
        yield
        to_right[0].wait_recv()
        far_0 = self.copy(view(near_l, 0), self.right)
        to_left[0].wait_recv()
        far_1 = self.copy(view(near_r, 1), self.left)
        yield
        to_right[1].wait_recv()
        over.append(self.copy(view(near_l), self.partner))
        to_left[1].wait_recv()
        over.append(self.copy(view(near_r), self.partner))
        far_0.wait_recv()
        over.append(self.copy(view(far, 0), self.partner))
        far_1.wait_recv()
        over.append(self.copy(view(far, 1), self.partner))
        yield
        for copy in over:
            copy.wait_recv()
        yield

    def gather_zy(self, ref, start, count, first, thin=0):
        yp, ym, zp, zm = self.zy
        y, z = self.y, self.z
        y_m, y_p, z_m, z_p = mod4(y - 1), mod4(y + 1), mod4(z - 1), mod4(z + 1)

        def cut(top, size):
            return pl.ds(top, size // 2), pl.ds(top + size // 2, size // 2), pl.ds(top, size)

        a_0, a_1, a_all = cut(start + count - first, first)
        b_0, b_1, b_all = cut(start, count - first)
        c_0, c_1, c_all = cut(start + thin, count - first - thin)
        t_0, t_1, t_all = cut(start, thin)
        front = slice(0, 2)

        def both(zs, rows, to, ys=None, zs_back=None, rows_back=None, ys_back=None):
            lane, lane_back = [ALL if v is None else at(B * v) for v in (ys, ys_back)]
            forth = ref.at[zs, rows, lane]
            back = forth if rows_back is None else ref.at[zs_back, rows_back, lane_back]
            return self.copy(forth, to[0]), self.copy(back, to[1])

        def done(*copies):
            for copy in copies:
                copy.wait_recv()

        on_y, on_z = (yp, ym), (zp, zm)
        a, b = both(z, a_all, on_y, y), both(z, b_all, on_z, y)
        yield
        done(*a)
        a = both(z, a_0, on_y, y_m, z, a_1, y_p)
        done(*b)
        b = both(z_m, b_0, on_z, y, z_p, b_1, y)
        yield
        done(*a)
        a = both(z, a_all, on_z)
        done(*b)
        b = both(ALL, c_all, on_y, y)
        if thin:
            b += both(front, t_all, on_y, y)
        yield
        done(*a)
        a = both(z_m, a_0, on_z, None, z_p, a_1)
        done(*b)
        b = both(ALL, c_0, on_y, y_m, ALL, c_1, y_p)
        if thin:
            b += both(front, t_0, on_y, y_m, front, t_1, y_p)
        yield
        done(*a, *b)
        yield

    def gather_y(self, ref, start, count):
        half, y = count // 2, self.y
        yp, ym = self.zy[:2]

        def view(ys, part=None):
            return ref.at[pl.ds(start, count) if part is None else pl.ds(start + part * half, half), at(B * ys)]

        near = self.copy(view(y), yp), self.copy(view(y), ym)
        yield
        near[0].wait_recv()
        far_0 = self.copy(view(mod4(y - 1), 0), yp)
        near[1].wait_recv()
        far_1 = self.copy(view(mod4(y + 1), 1), ym)
        yield
        far_0.wait_recv()
        far_1.wait_recv()
        yield

    def spread_z(self, *parts):
        sent = []
        for d, peer in ((1, self.zy[2]), (-1, self.zy[3]), (2, self.far_z)):
            for src, dst in parts:
                sent.append((self.copy(src(mod4(self.z + d)), peer, dst(self.z)), dst(mod4(self.z - d))))
        yield
        over = []
        for copy, got in sent:
            copy.wait_recv()
            over.append(self.copy(got, self.partner))
        yield
        for copy in over:
            copy.wait_recv()
        yield

    def swap(self, src, dst, across):
        def piece(k):
            return (k // R, lax.rem(k, R)) if across else (ALL, k)

        others, me = (self.plane(), self.c) if across else (self.line(), self.r)
        sent = [self.copy(src.at[piece(place)], peer, dst.at[piece(me)]) for peer, place in others]
        dst[piece(me)] = src[piece(me)]
        yield
        for copy in sent:
            copy.wait_recv()
        yield

    def reduce(self, acc, fwd, end, start, count, put, terms=None, width=None):
        half, lanes = count // 2, ALL if width is None else pl.ds(0, width)
        rows, lo, hi, mid = pl.ds(start, count), pl.ds(start, half), pl.ds(start + half, half), pl.ds(start // 2, half)
        me, right, left = (self.z, *self.zy[2:]) if terms is None else (self.x, self.right, self.left)
        far, nxt, prv = [mod4(me + d) for d in (2, 1, -1)]
        if terms is not None:
            over = self.copy(terms.at[:, 1 - self.core, rows, lanes], self.partner, acc.at[:, rows, lanes])
            yield
            over.wait_recv()

        def settle(k):
            if terms is not None:
                acc[k, rows, lanes] = acc[k, rows, lanes] + terms[k, self.core, rows, lanes]

        def send(k, part, to, ref, slot):
            return self.copy(acc.at[k, part, lanes], to, ref.at[slot, mid, lanes])

        settle(far)
        far_r, far_l = send(far, lo, right, fwd, 0), send(far, hi, left, fwd, 1)
        settle(nxt)
        settle(prv)
        last = [send(nxt, hi, right, end, 0), send(prv, lo, left, end, 1)]
        settle(me)
        yield
        far_r.wait_recv()
        acc[nxt, lo, lanes] = acc[nxt, lo, lanes] + fwd[0, mid, lanes]
        last.append(send(nxt, lo, right, end, 2))
        far_l.wait_recv()
        acc[prv, hi, lanes] = acc[prv, hi, lanes] + fwd[1, mid, lanes]
        last.append(send(prv, hi, left, end, 3))
        yield
        for copy in last:
            copy.wait_recv()
        blocks = count // B
        for k in range(blocks):
            one, two = (1, 2) if 2 * k < blocks else (0, 3)
            row = pl.ds(start // 2 + B * (k % (blocks // 2)), B)
            put(k, acc[me, pl.ds(start + B * k, B), lanes] + (end[one, row, lanes] + end[two, row, lanes]))
        yield


def invert(w_ref, l_ref, tmp_ref):
    row = lax.broadcasted_iota(jnp.int32, (Q, Q), 0)
    col = lax.broadcasted_iota(jnp.int32, (Q, Q), 1)
    w_ref[...] = jnp.zeros_like(w_ref)

    def block(ref, i, j, size):
        return ref[i // B:(i + size) // B, :, j:j + size].reshape(size, size)

    def put(i, j, size, val):
        w_ref[i // B:(i + size) // B, :, j:j + size] = val.reshape(size // B, B, size)

    corners = range(0, K, Q)
    for k in corners:
        a = block(l_ref, k, k, Q)
        diag = jnp.where(row == col, a, 0.0)
        down, across = 1.0 / jnp.sum(diag, axis=1, keepdims=True), 1.0 / jnp.sum(diag, axis=0, keepdims=True)
        low = (row // 2 == col // 2) & (row > col)
        put(k, k, Q, jnp.where(row == col, down, jnp.where(low, -a * down * across, 0.0)))
    size = 2
    while size < Q:
        pair = (row // (2 * size) == col // (2 * size)) & (row // size > col // size)
        for k in corners:
            tmp_ref[k // Q] = mm(jnp.where(pair, block(l_ref, k, k, Q), 0.0), block(w_ref, k, k, Q))
        yield
        for k in corners:
            w = block(w_ref, k, k, Q)
            put(k, k, Q, w - mm(w, tmp_ref[k // Q]))
        yield
        size *= 2
    while size < K:
        for j in range(0, K, 2 * size):
            i = j + size
            part = mm(block(l_ref, i, j, size), block(w_ref, j, j, size))
            put(i, j, size, -mm(block(w_ref, i, i, size), part))
            yield
        size *= 2


def pieces(ref, u, v):
    top, n = B * (u * (u + 1) // 2 + v - 1), ref.shape[2]
    i, low = top // n, top % n
    cut = min(B, n - low)
    first = [(slice(0, cut), (i, slice(low, low + cut)))]
    return first if cut == B else first + [(slice(cut, B), (i + 1, slice(0, B - cut)))]


def inner(net, u, start, panel, top, bar, terms):
    def two(k, _):
        h, x = k // U, lax.rem(k, U)
        a, b = panel[2 * h + x // 2, top:top + K - Q * u, at(Q * lax.rem(x, 2), Q)], bar[Q * u:, :B * (u + 1)]
        p = mm_t(a, b) if u else mm_t(b, a)
        for e in range(2):
            for v in range(u + 1):
                val = p[B * e:B * (e + 1), B * v:B * (v + 1)] if u else p[:, B * e:B * (e + 1)].T
                terms[x, e, at(start + Q * v + B * h), :] = phi(val, 2 * k + e - net.c) if v == u else val
        return 0

    lax.fori_loop(0, R, two, 0)


def front_kernel(l_ref, bar_ref, lr_ref, col_ref, a_ref, b_ref, lv, lss, wss, tmp, terms, acc, fwd, end, dma_sems, send_sems, recv_sems):
    net = Net(send_sems, recv_sems)
    r, c, y, z, core = net.r, net.c, net.y, net.z, net.core
    half, zz = z // 2, lax.rem(z, 2)
    ways = (1, 2, 3)
    others = [net.device(y=mod4(y + d)) for d in ways]
    for u in GROUPS:
        lv[2:, OFF[u]:OFF[u] + B] = jnp.zeros((2, B, H), jnp.float32)
    net.barrier(*[peer for peer, _ in net.line()], *others, *net.zy[2:])

    strip = at(B * (U * zz + y))

    def own(u):
        return at(B * (2 * u + half)), at(B * u)

    sent = [net.copy(l_ref.at[own(mod4(y + d))], other, lss.at[r, :, strip]) for d, other in zip(ways, others)]
    lss[r, :, strip] = l_ref[own(y)]
    for u in GROUPS:
        lv[z, group(u), at(B * y)] = l_ref[Q * u:, B * u:B * (u + 1)]
    g = [net.gather_zy(lv, OFF[u], K - Q * u, (K - Q * u - 96) // 2, B) for u in GROUPS]
    run(chain(g[3], g[2]))
    for copy in sent:
        copy.wait_recv()
    pair = net.copy(lss.at[r, :, at(H * zz, H)], net.device(z=2 * half + 1 - zz))
    run(chain(g[1], g[0], g[3], g[3]))
    pair.wait_recv()

    order = iter([2, 2, 3, 1, 3, 2, 1, 2, 0, 1, 0, 1, 0, 0])
    stores = []

    def tick():
        u = next(order, None)
        if u is not None:
            step(g[u])

    def keep(u):
        stores.append(pltpu.make_async_copy(lv.at[:, group(u)], lr_ref.at[:, group(u)], dma_sems.at[u]))
        stores[-1].start()

    def begin(u):
        start = ROWS - Q * (u + 1) * (u + 2) // 2
        inner(net, u, start, lv, OFF[u], bar_ref, terms)

        def put(k, val):
            v, h = k // 2, k % 2
            for rows, place in pieces(a_ref, u, v):
                a_ref[(h, *place)] = val[rows]

        keep(u)
        return net.reduce(acc, fwd, end, start, Q * (u + 1), put, terms)

    strips = net.gather_x(lss, axis=0)
    step(strips)
    for _ in range(3):
        tick()
    step(strips)
    for _ in range(2):
        tick()
    step(strips)
    s3 = begin(3)
    run(strips)
    step(s3)
    for k, _ in enumerate(invert(wss, lss, tmp)):
        if k % 4 == 1:
            tick()
        if k % 6 == 5:
            step(s3)
    s2 = begin(2)
    step(s2)
    tick()

    sent = [net.copy(wss.at[r, :, at(B * (U * zz + mod4(y + d)))], other, col_ref.at[y, r]) for d, other in zip(ways, others)]
    col_ref[y, r] = wss[r, :, strip]
    step(s2)
    tick()
    tick()
    s1 = begin(1)
    run(s3, s2)
    for copy in sent:
        copy.wait_recv()
    columns = net.gather_x(col_ref)
    step(columns)
    run(s1, columns)
    flip = net.swap(a_ref, b_ref, False)
    step(flip)
    for _ in range(U):
        tick()
    step(flip)
    keep(0)
    for copy in stores:
        copy.wait()
    net.drain()


def levels_kernel(lr_ref, bar_ref, wc_ref, a, b, sy_ref, w_ref, row_e, row_d, row_o, col_3,
                  own, d, back, s_top, top_back, la, lb, l0, l1, bv, cd, re, rd, co, ro, c3, x1, x2, x3, terms, acc, fwd, end, dma_sems, send_sems, recv_sems, t_send, t_recv):
    net = Net(send_sems, recv_sems)
    r, c, y, z = net.r, net.c, net.y, net.z
    sems = iter(range(32))

    def local(a, b):
        copy = pltpu.make_async_copy(a, b, dma_sems.at[next(sems)])
        copy.start()
        return copy

    load_0 = [local(lr_ref.at[:, group(0)], l0), local(bar_ref.at[:, 0:B], bv)]
    load_a = [local(lr_ref.at[0:2, OFF[u] + B:OFF[u] + Q], la.at[:, B * u:B * (u + 1)]) for u in GROUPS]
    load_b = [local(lr_ref.at[:, OFF[u] + Q:OFF[u] + H], lb.at[:, B * u:B * (u + 2)]) for u in (0, 2)]
    load_c = local(lr_ref.at[:, OFF[1] + Q:OFF[2]], l1)
    net.barrier(*[peer for peer, _ in net.line() + net.plane()])
    half_c, row_c = c // R, lax.rem(c, R)
    swap = [{'row': row_c, 'col': r + R * h} for h in range(2)]
    away = [(row_c != r) | (half_c != h) for h in range(2)]

    def block(ref, h, u, v):
        return jnp.concatenate([ref[(h, *place)] for _, place in pieces(ref, u, v)], axis=0)

    def trade(h, slot):
        return pltpu.make_async_remote_copy(src_ref=s_top.at[h], dst_ref=top_back.at[slot], send_sem=t_send.at[h],
                                            recv_sem=t_recv.at[slot], device_id=swap[h], device_id_type=MESH)

    low = c < R
    stores = []
    for u in GROUPS:
        re[z, B * u:B * (u + 1), at(B * y)] = wc_ref[u, r]
    diag = net.gather_zy(re, 0, H, Q)
    step(diag)
    for u in range(1, U):
        for h in range(2):
            for v in range(u + 1):
                own[v, B * (2 * u + h):B * (2 * u + h + 1), :] = block(a, h, u, v)
    places = [local(own.at[v, Q * (v + 1):], sy_ref.at[K * v + Q * (v + 1):K * (v + 1), at(B * y)]) for v in range(U - 1)]
    for place in places:
        place.wait()
    early = [net.gather_y(sy_ref, K * v + Q * (v + 1), K - Q * (v + 1)) for v in range(U - 1)]
    late = net.gather_y(sy_ref, 3 * K, K)
    e0, e1, e2 = early
    half = pl.ds(2 * net.core, 2)
    step(e0)

    for u in GROUPS:
        load_a[u].wait()
        cd[u, 0:R] = jnp.where(low, wc_ref[u], 0.0)
        x1[u, r] = mm(wide(la, slice(B * u, B * (u + 1)), (0, 1)), cd[u, 0:R].reshape(K, B))
    strips = net.gather_x(x1)
    flip = net.swap(b, d, True)
    run(chain(strips, diag, strips, diag, flip))
    for load in load_0:
        load.wait()
    inner(net, 0, 0, l0, 0, bv, terms)

    def put(k, val):
        s_top[k] = val

    run(strips, net.reduce(acc, fwd, end, 0, Q, put, terms), behind=[chain(diag, e0, diag)])
    run(diag)
    for h in range(2):
        @pl.when(away[h])
        def _():
            trade(h, half_c).start()

        @pl.when(jnp.logical_not(away[h]))
        def _():
            top_back[h] = s_top[h]
    stores.append(local(re, row_e))
    for u in GROUPS:
        w = -mm(wide(re, slice(B * u, B * (u + 1)), (2, 3)), x1[u].reshape(K, B))
        w = jnp.where(low, w, wc_ref[u, r])
        cd[u, R + r] = w
        rd[z, B * u:B * (u + 1), at(B * y)] = w
    rows = net.gather_zy(rd, 0, H, Q)
    step(rows)
    run(net.gather_x(cd, first=R), behind=[chain(rows, e1, rows, e0)])
    stores.append(local(cd.at[:, pl.ds(U * z, U)], w_ref.at[0:U, z]))
    out = net.spread_z((lambda k: cd.at[:, pl.ds(U * k + 2 * net.core, 2)], lambda k: w_ref.at[0:U, k, half]))
    step(flip)
    flip = net.swap(d, back, False)
    step(flip)

    for q in range(2):
        load_b[q].wait()
        x2[2 * q:2 * q + 2, r] = mm(wide(lb, slice(Q * q, Q * (q + 1))), cd[2 * q].reshape(N, B)).reshape(2, B, B)
    run(net.gather_x(x2), behind=[chain(e1, rows, e2, e1)])
    run(rows)
    stores.append(local(rd, row_d))
    for q in range(2):
        at_u = slice(B * (2 * q + 1), B * (2 * q + 2))
        tops = (mm(wide(re, at_u, (0, 1)), x2[2 * q].reshape(K, B)), mm(wide(rd, at_u), x2[2 * q:2 * q + 2].reshape(N, B)))
        for i, w in enumerate(tops):
            co[2 * q + i, r] = -w
            ro[z, B * (2 * q + i):B * (2 * q + i + 1), at(B * y)] = -w
    rows = net.gather_zy(ro, 0, H, Q)
    step(rows)
    step(out)
    strips = net.gather_x(co)
    step(strips)

    step(flip)
    for h in range(2):
        own[0, B * h:B * (h + 1), :] = s_top[h]
    for s in range(2):
        @pl.when(away[s])
        def _():
            trade(s, s).wait_recv()
        for u in GROUPS:
            for v in range(u + 1):
                at_t = slice(B * (2 * v + s), B * (2 * v + s + 1))
                val = (block(back, s, u, v) if u else top_back[s]).T
                own[u, at_t, :] = own[u, at_t, :] + val if u == v else val
    places = [local(own.at[v, 0:Q * (v + 1)], sy_ref.at[K * v:K * v + Q * (v + 1), at(B * y)]) for v in GROUPS]
    run(strips, behind=[chain(rows, e2, rows, out)])
    for place in places:
        place.wait()
    step(late)
    parts = []
    for q in range(2):
        stores.append(local(co.at[2 * q + z // 2, pl.ds(U * lax.rem(z, 2), U)], w_ref.at[U + q, z]))
        parts.append((lambda k, q=q: co.at[2 * q + k // 2, pl.ds(U * lax.rem(k, 2) + 2 * net.core, 2)],
                      lambda k, q=q: w_ref.at[U + q, k, half]))
    out_o = net.spread_z(*parts)

    load_c.wait()
    x3[:, r] = mm(wide(l1, ALL), jnp.concatenate([co[0:2].reshape(N, B), cd[1].reshape(N, B)], 1)).reshape(U, B, Q)
    x3[:, r, :, :B] = x3[:, r, :, :B] + mm(wide(l0, slice(H, K)), cd[0].reshape(N, B)).reshape(U, B, B)
    run(net.gather_x(x3), behind=[chain(rows, late, out, e2)])
    run(rows)
    step(out_o)
    stores.append(local(ro, row_o))
    for i in GROUPS:
        u = 2 + i // 2
        at_u = slice(B * u, B * (u + 1))
        if i % 2 == 0:
            w = mm(wide(re, at_u, (0, 1)), x3[i].reshape(K, Q))
        else:
            w = mm(wide(rd, at_u), x3[i - 1:i + 1].reshape(N, Q))
        if i >= 2:
            w = w + mm(wide(ro, slice(B * i, B * (i + 1))), x3[0:2].reshape(N, Q))
        c3[i, r] = -w
    run(net.gather_x(c3), behind=[chain(late, out_o)])
    run(late, out_o)
    stores.append(local(c3, col_3))
    for h in range(2):
        @pl.when(away[h])
        def _():
            trade(h, half_c).wait_send()
    for copy in stores:
        copy.wait()
    net.drain()


def product_kernel(sy_ref, w_ref, c3_ref, m_ref, own_ref, sy, w, c3, wide_w, acc, fwd, end, dma_sems, send_sems, recv_sems):
    net = Net(send_sems, recv_sems)
    z = net.z
    start = [slice(K * v, K * v + Q * (v + 1)) for v in range(U - 1)]
    rest = [slice(K * v + Q * (v + 1), K * (v + 1)) for v in range(U - 1)] + [slice(3 * K, U * K)]
    loads = [(c3_ref, c3), *[(sy_ref.at[some], sy.at[some]) for some in (*start, *rest)], (w_ref, w)]
    loads = [pltpu.make_async_copy(a, b, dma_sems.at[k]) for k, (a, b) in enumerate(loads)]
    for load in loads:
        load.start()
    for load in loads[:U]:
        load.wait()
    net.barrier(*net.zy, net.far_z, net.partner)
    half = pl.ds(2 * net.core, 2)
    parts = []
    for v in range(2):
        wide_w[v, z] = c3[2 * v + z // 2, pl.ds(U * lax.rem(z, 2), U)]
        parts.append((lambda k, v=v: c3.at[2 * v + k // 2, pl.ds(U * lax.rem(k, 2) + 2 * net.core, 2)],
                      lambda k, v=v: wide_w.at[v, k, half]))
    out = net.spread_z(*parts)
    step(out)
    own_ref[...] = c3[:, net.r]
    m0, m1, m2 = moves = [net.gather_y(sy, K * v, Q * (v + 1)) for v in range(U - 1)]
    run(chain(m2, m1))
    m_ref[...] = jnp.zeros_like(m_ref)

    def block(v, col):
        if v >= 2 and col < 2:
            some = [wide_w[v - 2, k, :, :, B * col:B * (col + 1)] for k in GROUPS]
        else:
            some = [w[v if v == col else U + v // 2, k] for k in GROUPS]
        return jnp.concatenate([x.reshape(H, B) for x in some], axis=1)

    def terms(u, col, groups, more=False):
        part = sum(mm(sy[K * v + Q * u:K * v + Q * (u + 1), :], block(v, col)) for v in groups)
        for k in GROUPS:
            place = k, slice(Q * u, Q * (u + 1)), slice(B * col, B * (col + 1))
            val = part[:, B * k:B * (k + 1)]
            acc[place] = acc[place] + val if more else val

    def sum_of(u):
        def put(k, val):
            m_ref[Q * u + B * k:Q * u + B * (k + 1), :B * (u + 1)] = val

        return net.reduce(acc, fwd, end, Q * u, Q, put, width=B * (u + 1))

    for load in loads[U:]:
        load.wait()
    sums = []
    for u in GROUPS[::-1]:
        for col in range(u + 1):
            terms(u, col, range(col, U if col >= 2 else 2))
        if u == 3:
            run(chain(m2, m0, m1, m2, out))
            run(out)
        for col in range(min(u + 1, 2)):
            terms(u, col, range(2, U), True)
        for s in sums:
            step(s)
        sums.append(sum_of(u))
        step(sums[-1])
        run(chain(m1, m0))
    run(*moves, *sums)
    net.drain()


def gradient_kernel(x_ref, own_ref, re_ref, rd_ref, ro_ref, t_ref,
                    wr, terms, acc, fwd, end, dma_sems, send_sems, recv_sems):
    net = Net(send_sems, recv_sems)
    loads = [[(re_ref.at[0:2, B * u:B * (u + 1)], wr.at[0:2, OFF[u]:OFF[u] + B]),
              (rd_ref.at[:, B * u:B * (u + 1)], wr.at[:, OFF[u] + B:OFF[u] + Q])] for u in GROUPS]
    loads[2] += [(ro_ref.at[:, Q:], wr.at[:, OFF[2] + Q:OFF[3]])]
    loads[0] += [(ro_ref.at[:, :Q], wr.at[:, Q:H])]
    sems = iter(range(16))
    loads = [[pltpu.make_async_copy(a, b, dma_sems.at[next(sems)]) for a, b in some] for some in loads]
    for some in loads[::-1]:
        for load in some:
            load.start()
    net.barrier(net.right, net.left, net.partner, *net.zy)
    for i in GROUPS:
        for k, top in enumerate((H, OFF[1] + Q)):
            wr[net.z, top + B * i:top + B * (i + 1), at(B * net.y)] = own_ref[i, :, B * k:B * (k + 1)]
    rows_0, rows_1 = net.gather_zy(wr, H, H, Q), net.gather_zy(wr, OFF[1] + Q, H, Q)
    step(rows_1)
    step(rows_0)

    def half_of(u, h, top=0, rows=K):
        width = B * (u + 1)
        some = slice(OFF[u] + top, min(OFF[u] + top + rows, OFF[u] + K - Q * u))
        these = slice(Q * u + top, Q * u + top + some.stop - some.start)

        def two(x, _):
            a, b = wr[2 * h + x // 2, some, at(Q * lax.rem(x, 2), Q)], x_ref[these, :width]
            part = mm_t(a, b) if u else mm_t(b, a)
            for e in range(2):
                place = x, e, slice(Q * u + B * h, Q * u + B * (h + 1)), slice(0, width)
                val = part[B * e:B * (e + 1)] if u else part[:, B * e:B * (e + 1)].T
                terms[place] = terms[place] + val if top else val
            return 0

        lax.fori_loop(0, U, two, 0)

    def sum_of(u):
        wr[2:, OFF[u]:OFF[u] + B] = jnp.zeros((2, B, H), jnp.float32)
        for load in loads[u]:
            load.wait()
        for top in ((0,) if u else (0, H)):
            for h in range(2):
                half_of(u, h, top, K if u else H)
                yield

        def put(k, val):
            t_ref[B * (2 * u + k):B * (2 * u + k + 1), :B * (u + 1)] = val

        yield from net.reduce(acc, fwd, end, Q * u, Q, put, terms, B * (u + 1))

    s0, s1, s2, s3 = [sum_of(u) for u in GROUPS]
    run(chain(s3, s3, s3, rows_1, s2, s3, rows_1, s2, rows_1, s3, s2, rows_1, s2, s3, rows_0, s1, s2, s1, s1, rows_0, s0, s1, s2,
              s0, s1, rows_0, s1, rows_0, s0, s0, s0, s0, s0, s0))
    run(s2, s1, s0)
    net.drain()


def call(kernel, ident, flops, args, in_specs, outs, out_specs, scratch, sems):
    return pl.pallas_call(
        kernel,
        out_shape=[jax.ShapeDtypeStruct(s, jnp.float32) for s in outs],
        in_specs=in_specs,
        out_specs=out_specs,
        scratch_shapes=[*(pltpu.VMEM(s, jnp.float32) for s in scratch), *(pltpu.SemaphoreType.DMA(s) for s in sems)],
        compiler_params=pltpu.CompilerParams(collective_id=ident, has_side_effects=True, vmem_limit_bytes=67 * 10 ** 6),
        cost_estimate=pl.CostEstimate(flops=flops, bytes_accessed=K, transcendentals=0),
    )(*args)


def solution(mesh):
    def local_pass(fac, bar):
        panel, rows, column = (U, ROWS, H), (U, H, H), (U, R, B, B)
        wide_col, cut = (U, R, B, Q), (2, R, (ROWS - Q) // (2 * R), B)
        lr, wc, a, b = call(
            front_kernel, 0, 1, (fac, bar), [VM] * 2, (panel, column, cut, cut), [HB] + [VM] * 3,
            (panel, (R, B, K), (R, B, K), (U, Q, Q), (U, 2, ROWS, B), (U, ROWS, B), (2, ROWS // 2, B), (U, ROWS // 2, B)),
            ((U,), (144,), (144,)))
        sy, w, row_e, row_d, row_o, col_3 = call(
            levels_kernel, 1, 1, (lr, bar, wc, a, b), [HB, HB, VM, VM, VM],
            ((U * K, H), (6, U, U, B, B), rows, rows, rows, wide_col), [HB] * 6,
            ((U, K, B), cut, cut, (2, B, B), (2, B, B), (2, H, H), rows, (U, K, H), rows, (K, B), (U, 2 * R, B, B), rows, rows, column, rows,
             wide_col, column, column, wide_col, (U, 2, Q, B), (U, Q, B), (2, B, B), (U, B, B)),
            ((48,), (208,), (208,), (2,), (2,)))
        m, own = call(
            product_kernel, 2, 1, (sy, w, col_3), [HB] * 3, ((K, H), (U, B, Q)), [VM] * 2,
            ((U * K, H), (6, U, U, B, B), wide_col, (2, U, U, B, Q), (U, K, H), (2, H, H), (U, H, H)), ((16,), (48,), (48,)))
        out, = call(
            gradient_kernel, 3, 1, (m, own, row_e, row_d, row_o), [VM] * 2 + [HB] * 3, ((K, H),), [VM],
            (panel, (U, 2, K, H), (U, K, H), (2, H, H), (U, H, H)), ((16,), (64,), (64,)))
        row, col = lax.broadcasted_iota(jnp.int32, out.shape, 0), lax.broadcasted_iota(jnp.int32, out.shape, 1)
        row_all = (row // B * R + lax.axis_index('row')) * B + row % B
        col_all = (col // B * 2 * R + lax.axis_index('col')) * B + col % B
        return jnp.where(row_all > col_all, out, jnp.where(row_all == col_all, 0.5 * out, 0.0))

    spec = P(('batch', 'row'), 'col')
    return jax.shard_map(local_pass, mesh=mesh, in_specs=(spec, spec), out_specs=spec, check_vma=False)
```

```python
import jax
import jax.numpy as jnp
from jax import lax
from jax.experimental import pallas as pl
from jax.experimental.pallas import tpu as pltpu
from jax.sharding import PartitionSpec as P

B, Q, H, K, N = 128, 256, 512, 1024, 2048
U, R = 4, 8
GROUPS = tuple(range(U))
OFF = tuple(K * u - B * u * (u - 1) for u in GROUPS)
ROWS = OFF[-1] + Q
HI = lax.Precision.HIGHEST
MESH = pl.DeviceIdType.MESH
VM = pl.BlockSpec(memory_space=pltpu.VMEM)
HB = pl.BlockSpec(memory_space=pl.ANY)
ALL = slice(None)


def mm(a, b):
    return jnp.dot(a, b, precision=HI, preferred_element_type=jnp.float32)


def mm_t(a, b):
    return lax.dot_general(a, b, (((0,), (0,)), ((), ())), precision=HI, preferred_element_type=jnp.float32)


def mod4(v):
    return lax.rem(v + U, U)


def at(start, size=B):
    return pl.ds(start if isinstance(start, int) else pl.multiple_of(start, B), size)


def group(u):
    return slice(OFF[u], OFF[u] + K - Q * u)


def wide(ref, rows, zs=GROUPS):
    return jnp.concatenate([ref[z, rows] for z in zs], axis=1)


def phi(block, ahead):
    diff = B * ahead + lax.broadcasted_iota(jnp.int32, (B, B), 0) - lax.broadcasted_iota(jnp.int32, (B, B), 1)
    return jnp.where(diff > 0, block, jnp.where(diff == 0, 0.5 * block, 0.0))


def step(g):
    return next(g, g) is not g


def run(*gathers, behind=()):
    live = list(gathers)
    while live:
        live = [g for g in live if step(g)]
        for g in behind:
            step(g)


def chain(*gathers):
    for g in gathers:
        step(g)
        yield


class Net:
    def __init__(self, send_sems, recv_sems):
        self.send_sems, self.recv_sems = send_sems, recv_sems
        self.r, self.c = lax.axis_index('row'), lax.axis_index('col')
        self.x, self.core = self.r // 2, lax.rem(self.r, 2)
        self.z, self.y = self.c // U, lax.rem(self.c, U)
        self.right, self.left = self.device(x=mod4(self.x + 1)), self.device(x=mod4(self.x - 1))
        self.partner = self.device(core=1 - self.core)
        self.zy = [self.device(y=mod4(self.y + 1)), self.device(y=mod4(self.y - 1)),
                   self.device(z=mod4(self.z + 1)), self.device(z=mod4(self.z - 1))]
        self.far_z = self.device(z=mod4(self.z + 2))
        self.copies = []

    def device(self, **place):
        x, core, y, z = [place.get(k, getattr(self, k)) for k in ('x', 'core', 'y', 'z')]
        return {'col': U * z + y, 'row': 2 * x + core}

    def barrier(self, *peers):
        sem = pltpu.get_barrier_semaphore()
        for peer in peers:
            pl.semaphore_signal(sem, inc=1, device_id=peer, device_id_type=MESH)
        pl.semaphore_wait(sem, len(peers))

    def line(self):
        places = [(mod4(self.x + d // 2), lax.rem(self.core + d, 2)) for d in range(1, R)]
        return [(self.device(x=x, core=core), 2 * x + core) for x, core in places]

    def plane(self):
        places = [(mod4(self.z + d // U), mod4(self.y + d % U)) for d in range(1, U * U)]
        return [(self.device(z=z, y=y), U * z + y) for z, y in places]

    def copy(self, ref, peer, dst=None):
        k = len(self.copies)
        copy = pltpu.make_async_remote_copy(
            src_ref=ref, dst_ref=ref if dst is None else dst, send_sem=self.send_sems.at[k], recv_sem=self.recv_sems.at[k],
            device_id=peer, device_id_type=MESH)
        copy.start()
        self.copies.append(copy)
        return copy

    def drain(self):
        for copy in self.copies:
            copy.wait_send()

    def gather_x(self, ref, axis=1, first=0):
        half = ref.shape[1 - axis] // 2

        def view(r, part=None):
            other = ALL if part is None else pl.ds(part * half, half)
            return ref.at[(other, first + r) if axis else (r, other)]

        near_r, near_l, far = [2 * mod4(self.x + d) + self.core for d in (1, -1, 2)]
        to_right, to_left = [], []
        for part in range(2):
            to_right.append(self.copy(view(self.r, part), self.right))
            to_left.append(self.copy(view(self.r, 1 - part), self.left))
        over = [self.copy(view(self.r), self.partner)]
        yield
        to_right[0].wait_recv()
        far_0 = self.copy(view(near_l, 0), self.right)
        to_left[0].wait_recv()
        far_1 = self.copy(view(near_r, 1), self.left)
        yield
        to_right[1].wait_recv()
        over.append(self.copy(view(near_l), self.partner))
        to_left[1].wait_recv()
        over.append(self.copy(view(near_r), self.partner))
        far_0.wait_recv()
        over.append(self.copy(view(far, 0), self.partner))
        far_1.wait_recv()
        over.append(self.copy(view(far, 1), self.partner))
        yield
        for copy in over:
            copy.wait_recv()
        yield

    def gather_zy(self, ref, start, count, first, thin=0):
        yp, ym, zp, zm = self.zy
        y, z = self.y, self.z
        y_m, y_p, z_m, z_p = mod4(y - 1), mod4(y + 1), mod4(z - 1), mod4(z + 1)

        def cut(top, size):
            return pl.ds(top, size // 2), pl.ds(top + size // 2, size // 2), pl.ds(top, size)

        a_0, a_1, a_all = cut(start + count - first, first)
        b_0, b_1, b_all = cut(start, count - first)
        c_0, c_1, c_all = cut(start + thin, count - first - thin)
        t_0, t_1, t_all = cut(start, thin)
        front = slice(0, 2)

        def both(zs, rows, to, ys=None, zs_back=None, rows_back=None, ys_back=None):
            lane, lane_back = [ALL if v is None else at(B * v) for v in (ys, ys_back)]
            forth = ref.at[zs, rows, lane]
            back = forth if rows_back is None else ref.at[zs_back, rows_back, lane_back]
            return self.copy(forth, to[0]), self.copy(back, to[1])

        def done(*copies):
            for copy in copies:
                copy.wait_recv()

        on_y, on_z = (yp, ym), (zp, zm)
        a, b = both(z, a_all, on_y, y), both(z, b_all, on_z, y)
        yield
        done(*a)
        a = both(z, a_0, on_y, y_m, z, a_1, y_p)
        done(*b)
        b = both(z_m, b_0, on_z, y, z_p, b_1, y)
        yield
        done(*a)
        a = both(z, a_all, on_z)
        done(*b)
        b = both(ALL, c_all, on_y, y) if count > first + thin else ()
        if thin:
            b += both(front, t_all, on_y, y)
        yield
        done(*a)
        a = both(z_m, a_0, on_z, None, z_p, a_1)
        done(*b)
        b = both(ALL, c_0, on_y, y_m, ALL, c_1, y_p) if count > first + thin else ()
        if thin:
            b += both(front, t_0, on_y, y_m, front, t_1, y_p)
        yield
        done(*a, *b)
        yield

    def gather_y(self, ref, start, count):
        half, y = count // 2, self.y
        yp, ym = self.zy[:2]

        def view(ys, part=None):
            return ref.at[pl.ds(start, count) if part is None else pl.ds(start + part * half, half), at(B * ys)]

        near = self.copy(view(y), yp), self.copy(view(y), ym)
        yield
        near[0].wait_recv()
        far_0 = self.copy(view(mod4(y - 1), 0), yp)
        near[1].wait_recv()
        far_1 = self.copy(view(mod4(y + 1), 1), ym)
        yield
        far_0.wait_recv()
        far_1.wait_recv()
        yield

    def spread_z(self, *parts):
        sent = []
        for d, peer in ((1, self.zy[2]), (-1, self.zy[3]), (2, self.far_z)):
            for src, dst in parts:
                sent.append((self.copy(src(mod4(self.z + d)), peer, dst(self.z)), dst(mod4(self.z - d))))
        yield
        over = []
        for copy, got in sent:
            copy.wait_recv()
            over.append(self.copy(got, self.partner))
        yield
        for copy in over:
            copy.wait_recv()
        yield

    def swap(self, src, dst, across):
        def piece(k):
            return (k // R, lax.rem(k, R)) if across else (ALL, k)

        others, me = (self.plane(), self.c) if across else (self.line(), self.r)
        sent = [self.copy(src.at[piece(place)], peer, dst.at[piece(me)]) for peer, place in others]
        dst[piece(me)] = src[piece(me)]
        yield
        for copy in sent:
            copy.wait_recv()
        yield

    def reduce(self, acc, fwd, end, start, count, put, terms=None, width=None):
        half, lanes = count // 2, ALL if width is None else pl.ds(0, width)
        rows, lo, hi, mid = pl.ds(start, count), pl.ds(start, half), pl.ds(start + half, half), pl.ds(start // 2, half)
        me, right, left = (self.z, *self.zy[2:]) if terms is None else (self.x, self.right, self.left)
        far, nxt, prv = [mod4(me + d) for d in (2, 1, -1)]
        if terms is not None:
            over = self.copy(terms.at[:, 1 - self.core, rows, lanes], self.partner, acc.at[:, rows, lanes])
            yield
            over.wait_recv()

        def settle(k):
            if terms is not None:
                acc[k, rows, lanes] = acc[k, rows, lanes] + terms[k, self.core, rows, lanes]

        def send(k, part, to, ref, slot):
            return self.copy(acc.at[k, part, lanes], to, ref.at[slot, mid, lanes])

        settle(far)
        far_r, far_l = send(far, lo, right, fwd, 0), send(far, hi, left, fwd, 1)
        settle(nxt)
        settle(prv)
        last = [send(nxt, hi, right, end, 0), send(prv, lo, left, end, 1)]
        settle(me)
        yield
        far_r.wait_recv()
        acc[nxt, lo, lanes] = acc[nxt, lo, lanes] + fwd[0, mid, lanes]
        last.append(send(nxt, lo, right, end, 2))
        far_l.wait_recv()
        acc[prv, hi, lanes] = acc[prv, hi, lanes] + fwd[1, mid, lanes]
        last.append(send(prv, hi, left, end, 3))
        yield
        for copy in last:
            copy.wait_recv()
        blocks = count // B
        for k in range(blocks):
            one, two = (1, 2) if 2 * k < blocks else (0, 3)
            row = pl.ds(start // 2 + B * (k % (blocks // 2)), B)
            put(k, acc[me, pl.ds(start + B * k, B), lanes] + (end[one, row, lanes] + end[two, row, lanes]))
        yield


def invert(w_ref, l_ref, tmp_ref):
    row = lax.broadcasted_iota(jnp.int32, (Q, Q), 0)
    col = lax.broadcasted_iota(jnp.int32, (Q, Q), 1)
    w_ref[...] = jnp.zeros_like(w_ref)

    def block(ref, i, j, size):
        return ref[i // B:(i + size) // B, :, j:j + size].reshape(size, size)

    def put(i, j, size, val):
        w_ref[i // B:(i + size) // B, :, j:j + size] = val.reshape(size // B, B, size)

    corners = range(0, K, Q)
    for k in corners:
        a = block(l_ref, k, k, Q)
        diag = jnp.where(row == col, a, 0.0)
        down, across = 1.0 / jnp.sum(diag, axis=1, keepdims=True), 1.0 / jnp.sum(diag, axis=0, keepdims=True)
        low = (row // 2 == col // 2) & (row > col)
        put(k, k, Q, jnp.where(row == col, down, jnp.where(low, -a * down * across, 0.0)))
    size = 2
    while size < Q:
        pair = (row // (2 * size) == col // (2 * size)) & (row // size > col // size)
        for k in corners:
            tmp_ref[k // Q] = mm(jnp.where(pair, block(l_ref, k, k, Q), 0.0), block(w_ref, k, k, Q))
        yield
        for k in corners:
            w = block(w_ref, k, k, Q)
            put(k, k, Q, w - mm(w, tmp_ref[k // Q]))
        yield
        size *= 2
    while size < K:
        for j in range(0, K, 2 * size):
            i = j + size
            part = mm(block(l_ref, i, j, size), block(w_ref, j, j, size))
            put(i, j, size, -mm(block(w_ref, i, i, size), part))
            yield
        size *= 2


def pieces(ref, u, v):
    top, n = B * (u * (u + 1) // 2 + v - 1), ref.shape[2]
    i, low = top // n, top % n
    cut = min(B, n - low)
    first = [(slice(0, cut), (i, slice(low, low + cut)))]
    return first if cut == B else first + [(slice(cut, B), (i + 1, slice(0, B - cut)))]


def inner(net, u, start, panel, top, bar, terms):
    def two(k, _):
        h, x = k // U, lax.rem(k, U)
        a, b = panel[2 * h + x // 2, top:top + K - Q * u, at(Q * lax.rem(x, 2), Q)], bar[Q * u:, :B * (u + 1)]
        p = mm_t(a, b) if u else mm_t(b, a)
        for e in range(2):
            for v in range(u + 1):
                val = p[B * e:B * (e + 1), B * v:B * (v + 1)] if u else p[:, B * e:B * (e + 1)].T
                terms[x, e, at(start + Q * v + B * h), :] = phi(val, 2 * k + e - net.c) if v == u else val
        return 0

    lax.fori_loop(0, R, two, 0)


def front_kernel(l_ref, bar_ref, lr_ref, col_ref, a_ref, b_ref, lv, lss, wss, tmp, terms, acc, fwd, end, dma_sems, send_sems, recv_sems):
    net = Net(send_sems, recv_sems)
    r, c, y, z, core = net.r, net.c, net.y, net.z, net.core
    half, zz = z // 2, lax.rem(z, 2)
    ways = (1, 2, 3)
    others = [net.device(y=mod4(y + d)) for d in ways]
    for u in GROUPS:
        lv[2:, OFF[u]:OFF[u] + B] = jnp.zeros((2, B, H), jnp.float32)
    net.barrier(*[peer for peer, _ in net.line()], *others, *net.zy[2:])

    strip = at(B * (U * zz + y))

    def own(u):
        return at(B * (2 * u + half)), at(B * u)

    sent = [net.copy(l_ref.at[own(mod4(y + d))], other, lss.at[r, :, strip]) for d, other in zip(ways, others)]
    lss[r, :, strip] = l_ref[own(y)]
    for u in GROUPS:
        lv[z, group(u), at(B * y)] = l_ref[Q * u:, B * u:B * (u + 1)]
    g = [net.gather_zy(lv, OFF[u], K - Q * u, (K - Q * u - 96) // 2, B) for u in GROUPS]
    run(chain(g[3], g[2]))
    for copy in sent:
        copy.wait_recv()
    pair = net.copy(lss.at[r, :, at(H * zz, H)], net.device(z=2 * half + 1 - zz))
    run(chain(g[1], g[0], g[3], g[3]))
    pair.wait_recv()

    order = iter([2, 2, 3, 1, 3, 2, 1, 2, 0, 1, 0, 1])
    stores = []

    def tick():
        u = next(order, None)
        if u is not None:
            step(g[u])

    def keep(u):
        stores.append(pltpu.make_async_copy(lv.at[:, group(u)], lr_ref.at[:, group(u)], dma_sems.at[u]))
        stores[-1].start()

    def begin(u):
        start = ROWS - Q * (u + 1) * (u + 2) // 2
        inner(net, u, start, lv, OFF[u], bar_ref, terms)

        def put(k, val):
            v, h = k // 2, k % 2
            for rows, place in pieces(a_ref, u, v):
                a_ref[(h, *place)] = val[rows]

        keep(u)
        return net.reduce(acc, fwd, end, start, Q * (u + 1), put, terms)

    strips = net.gather_x(lss, axis=0)
    step(strips)
    for _ in range(3):
        tick()
    step(strips)
    for _ in range(2):
        tick()
    step(strips)
    s3 = begin(3)
    run(strips)
    step(s3)
    for k, _ in enumerate(invert(wss, lss, tmp)):
        if k % 4 == 1:
            tick()
        if k % 6 == 5:
            step(s3)
    s2 = begin(2)
    step(s2)
    tick()

    sent = [net.copy(wss.at[r, :, at(B * (U * zz + mod4(y + d)))], other, col_ref.at[y, r]) for d, other in zip(ways, others)]
    col_ref[y, r] = wss[r, :, strip]
    step(s2)
    tick()
    tick()
    s1 = begin(1)
    run(chain(s3, s1, s2, s1))
    for copy in sent:
        copy.wait_recv()
    columns = net.gather_x(col_ref)
    flip = net.swap(a_ref, b_ref, False)
    run(chain(columns, s2, s1, g[0], columns, s1, flip, columns, columns, g[0], flip))
    keep(0)
    for copy in stores:
        copy.wait()
    net.drain()


def levels_kernel(lr_ref, bar_ref, wc_ref, a, b, sy_ref, w_ref, row_e, row_d, row_o, col_3,
                  own, d, back, s_top, top_back, la, lb, l0, l1, bv, cd, re, rd, co, ro, c3, x1, x2, x3, terms, acc, fwd, end, dma_sems, send_sems, recv_sems, t_send, t_recv):
    net = Net(send_sems, recv_sems)
    r, c, y, z = net.r, net.c, net.y, net.z
    sems = iter(range(32))

    def local(a, b):
        copy = pltpu.make_async_copy(a, b, dma_sems.at[next(sems)])
        copy.start()
        return copy

    load_a = [local(lr_ref.at[0:2, OFF[u] + B:OFF[u] + Q], la.at[:, B * u:B * (u + 1)]) for u in GROUPS]
    load_0 = [local(lr_ref.at[:, group(0)], l0), local(bar_ref.at[:, 0:B], bv)]
    load_b = [local(lr_ref.at[:, OFF[u] + Q:OFF[u] + H], lb.at[:, B * u:B * (u + 2)]) for u in (0, 2)]
    load_c = local(lr_ref.at[:, OFF[1] + Q:OFF[2]], l1)
    net.barrier(*[peer for peer, _ in net.line() + net.plane()])
    half_c, row_c = c // R, lax.rem(c, R)
    swap = [{'row': row_c, 'col': r + R * h} for h in range(2)]
    away = [(row_c != r) | (half_c != h) for h in range(2)]

    def block(ref, h, u, v):
        return jnp.concatenate([ref[(h, *place)] for _, place in pieces(ref, u, v)], axis=0)

    def trade(h, slot):
        return pltpu.make_async_remote_copy(src_ref=s_top.at[h], dst_ref=top_back.at[slot], send_sem=t_send.at[h],
                                            recv_sem=t_recv.at[slot], device_id=swap[h], device_id_type=MESH)

    low = c < R
    stores = []
    for u in GROUPS:
        re[z, B * u:B * (u + 1), at(B * y)] = wc_ref[u, r]
    diag = net.gather_zy(re, 0, H, Q)
    step(diag)
    early = [net.gather_y(sy_ref, K * v + Q * (v + 1), K - Q * (v + 1)) for v in range(U - 1)]
    late = net.gather_y(sy_ref, 3 * K, K)
    e0, e1, e2 = early
    half = pl.ds(2 * net.core, 2)

    def odd(rows):
        return jnp.concatenate([rd[0, rows], rd[1, rows], re[2, rows], re[3, rows]], axis=1)

    for u in GROUPS:
        load_a[u].wait()
        cd[u, 0:R] = jnp.where(low, wc_ref[u], 0.0)
        x1[u, r] = mm(wide(la, slice(B * u, B * (u + 1)), (0, 1)), cd[u, 0:R].reshape(K, B))
    strips = net.gather_x(x1)
    flip = net.swap(b, d, True)
    run(chain(strips, diag, diag, flip))
    for u in range(1, U):
        for h in range(2):
            for v in range(u + 1):
                own[v, B * (2 * u + h):B * (2 * u + h + 1), :] = block(a, h, u, v)
    places = [local(own.at[v, Q * (v + 1):], sy_ref.at[K * v + Q * (v + 1):K * (v + 1), at(B * y)]) for v in range(U - 1)]
    step(strips)
    for load in load_0:
        load.wait()
    inner(net, 0, 0, l0, 0, bv, terms)
    for place in places:
        place.wait()

    def put(k, val):
        s_top[k] = val

    run(strips, net.reduce(acc, fwd, end, 0, Q, put, terms), behind=[chain(diag, e0, diag)])
    run(diag)
    for h in range(2):
        @pl.when(away[h])
        def _():
            trade(h, half_c).start()

        @pl.when(jnp.logical_not(away[h]))
        def _():
            top_back[h] = s_top[h]
    stores.append(local(re, row_e))
    for u in GROUPS:
        w = -mm(wide(re, slice(B * u, B * (u + 1)), (2, 3)), x1[u].reshape(K, B))
        w = jnp.where(low, w, wc_ref[u, r])
        cd[u, R + r] = w
        rd[z, B * u:B * (u + 1), at(B * y)] = w
    rows = net.gather_zy(rd, 0, H, B, H - B)
    step(rows)
    run(net.gather_x(cd, first=R), behind=[chain(rows, e1, rows, e0)])
    stores.append(local(cd.at[:, pl.ds(U * z, U)], w_ref.at[0:U, z]))
    out = net.spread_z((lambda k: cd.at[:, pl.ds(U * k + 2 * net.core, 2)], lambda k: w_ref.at[0:U, k, half]))
    step(flip)
    flip = net.swap(d, back, False)
    step(flip)

    for q in range(2):
        load_b[q].wait()
        x2[2 * q:2 * q + 2, r] = mm(wide(lb, slice(Q * q, Q * (q + 1))), cd[2 * q].reshape(N, B)).reshape(2, B, B)
    run(net.gather_x(x2), behind=[chain(e1, rows, e2, e1, e0)])
    run(rows)
    stores.append(local(rd, row_d))
    for q in range(2):
        at_u = slice(B * (2 * q + 1), B * (2 * q + 2))
        tops = (mm(wide(re, at_u, (0, 1)), x2[2 * q].reshape(K, B)), mm(odd(at_u), x2[2 * q:2 * q + 2].reshape(N, B)))
        for i, w in enumerate(tops):
            co[2 * q + i, r] = -w
            ro[z, B * (2 * q + i):B * (2 * q + i + 1), at(B * y)] = -w
    rows = net.gather_zy(ro, 0, H, Q)
    step(rows)
    step(out)
    strips = net.gather_x(co)
    step(strips)

    step(flip)
    for h in range(2):
        own[0, B * h:B * (h + 1), :] = s_top[h]
    for s in range(2):
        @pl.when(away[s])
        def _():
            trade(s, s).wait_recv()
        for u in GROUPS:
            for v in range(u + 1):
                at_t = slice(B * (2 * v + s), B * (2 * v + s + 1))
                val = (block(back, s, u, v) if u else top_back[s]).T
                own[u, at_t, :] = own[u, at_t, :] + val if u == v else val
    places = [local(own.at[v, 0:Q * (v + 1)], sy_ref.at[K * v:K * v + Q * (v + 1), at(B * y)]) for v in GROUPS]
    run(strips, behind=[chain(rows, e2, rows, out)])
    for place in places:
        place.wait()
    step(late)
    parts = []
    for q in range(2):
        stores.append(local(co.at[2 * q + z // 2, pl.ds(U * lax.rem(z, 2), U)], w_ref.at[U + q, z]))
        parts.append((lambda k, q=q: co.at[2 * q + k // 2, pl.ds(U * lax.rem(k, 2) + 2 * net.core, 2)],
                      lambda k, q=q: w_ref.at[U + q, k, half]))
    out_o = net.spread_z(*parts)

    load_c.wait()
    x3[:, r] = mm(wide(l1, ALL), jnp.concatenate([co[0:2].reshape(N, B), cd[1].reshape(N, B)], 1)).reshape(U, B, Q)
    x3[:, r, :, :B] = x3[:, r, :, :B] + mm(wide(l0, slice(H, K)), cd[0].reshape(N, B)).reshape(U, B, B)
    run(net.gather_x(x3), behind=[chain(rows, late, out, e2)])
    run(rows)
    step(out_o)
    stores.append(local(ro, row_o))
    for i in GROUPS:
        u = 2 + i // 2
        at_u = slice(B * u, B * (u + 1))
        if i % 2 == 0:
            w = mm(wide(re, at_u, (0, 1)), x3[i].reshape(K, Q))
        else:
            w = mm(odd(at_u), x3[i - 1:i + 1].reshape(N, Q))
        if i >= 2:
            w = w + mm(wide(ro, slice(B * i, B * (i + 1))), x3[0:2].reshape(N, Q))
        c3[i, r] = -w
    run(net.gather_x(c3), behind=[chain(late, out_o)])
    run(late, out_o)
    stores.append(local(c3, col_3))
    for h in range(2):
        @pl.when(away[h])
        def _():
            trade(h, half_c).wait_send()
    for copy in stores:
        copy.wait()
    net.drain()


def product_kernel(sy_ref, w_ref, c3_ref, m_ref, own_ref, sy, w, c3, wide_w, acc, fwd, end, dma_sems, send_sems, recv_sems):
    net = Net(send_sems, recv_sems)
    z = net.z
    start = [slice(K * v, K * v + Q * (v + 1)) for v in range(U - 1)]
    rest = [slice(K * v + Q * (v + 1), K * (v + 1)) for v in range(U - 1)] + [slice(3 * K, U * K)]
    loads = [(c3_ref, c3), *[(sy_ref.at[some], sy.at[some]) for some in (*start, *rest)], (w_ref, w)]
    loads = [pltpu.make_async_copy(a, b, dma_sems.at[k]) for k, (a, b) in enumerate(loads)]
    for load in loads:
        load.start()
    for load in loads[:U]:
        load.wait()
    net.barrier(*net.zy, net.far_z, net.partner)
    half = pl.ds(2 * net.core, 2)
    parts = []
    for v in range(2):
        wide_w[v, z] = c3[2 * v + z // 2, pl.ds(U * lax.rem(z, 2), U)]
        parts.append((lambda k, v=v: c3.at[2 * v + k // 2, pl.ds(U * lax.rem(k, 2) + 2 * net.core, 2)],
                      lambda k, v=v: wide_w.at[v, k, half]))
    out = net.spread_z(*parts)
    step(out)
    own_ref[...] = c3[:, net.r]
    m0, m1, m2 = moves = [net.gather_y(sy, K * v, Q * (v + 1)) for v in range(U - 1)]
    run(chain(m2, m1))
    m_ref[...] = jnp.zeros_like(m_ref)

    def block(v, col):
        if v >= 2 and col < 2:
            some = [wide_w[v - 2, k, :, :, B * col:B * (col + 1)] for k in GROUPS]
        else:
            some = [w[v if v == col else U + v // 2, k] for k in GROUPS]
        return jnp.concatenate([x.reshape(H, B) for x in some], axis=1)

    def terms(u, col, groups, more=False):
        part = sum(mm(sy[K * v + Q * u:K * v + Q * (u + 1), :], block(v, col)) for v in groups)
        for k in GROUPS:
            place = k, slice(Q * u, Q * (u + 1)), slice(B * col, B * (col + 1))
            val = part[:, B * k:B * (k + 1)]
            acc[place] = acc[place] + val if more else val

    def sum_of(u):
        def put(k, val):
            m_ref[Q * u + B * k:Q * u + B * (k + 1), :B * (u + 1)] = val

        return net.reduce(acc, fwd, end, Q * u, Q, put, width=B * (u + 1))

    for load in loads[U:]:
        load.wait()
    sums = []
    for u in GROUPS[::-1]:
        for col in range(u + 1):
            terms(u, col, range(col, U if col >= 2 else 2))
        if u == 3:
            run(chain(m2, m0, m1, m2, out))
            run(out)
        for col in range(min(u + 1, 2)):
            terms(u, col, range(2, U), True)
        for s in sums:
            step(s)
        sums.append(sum_of(u))
        step(sums[-1])
        run(chain(m1, m0))
    run(*moves, *sums)
    net.drain()


def gradient_kernel(x_ref, own_ref, re_ref, rd_ref, ro_ref, t_ref,
                    wr, terms, acc, fwd, end, dma_sems, send_sems, recv_sems):
    net = Net(send_sems, recv_sems)
    loads = [[(re_ref.at[0:2, B * u:B * (u + 1)], wr.at[0:2, OFF[u]:OFF[u] + B]),
              *[(ref.at[zs, B * u:B * (u + 1)], wr.at[zs, OFF[u] + B:OFF[u] + Q])
                for ref, zs in ((rd_ref, slice(0, 2)), (re_ref, slice(2, U)))]] for u in GROUPS]
    loads[2] += [(ro_ref.at[:, Q:], wr.at[:, OFF[2] + Q:OFF[3]])]
    loads[0] += [(ro_ref.at[:, :Q], wr.at[:, Q:H])]
    sems = iter(range(16))
    loads = [[pltpu.make_async_copy(a, b, dma_sems.at[next(sems)]) for a, b in some] for some in loads]
    for some in loads[::-1]:
        for load in some:
            load.start()
    net.barrier(net.right, net.left, net.partner, *net.zy)
    for i in GROUPS:
        for k, top in enumerate((H, OFF[1] + Q)):
            wr[net.z, top + B * i:top + B * (i + 1), at(B * net.y)] = own_ref[i, :, B * k:B * (k + 1)]
    rows_0, rows_1 = net.gather_zy(wr, H, H, Q), net.gather_zy(wr, OFF[1] + Q, H, Q)
    step(rows_1)
    step(rows_0)

    def half_of(u, h, top=0, rows=K):
        width = B * (u + 1)
        some = slice(OFF[u] + top, min(OFF[u] + top + rows, OFF[u] + K - Q * u))
        these = slice(Q * u + top, Q * u + top + some.stop - some.start)

        def two(x, _):
            a, b = wr[2 * h + x // 2, some, at(Q * lax.rem(x, 2), Q)], x_ref[these, :width]
            part = mm_t(a, b) if u else mm_t(b, a)
            for e in range(2):
                place = x, e, slice(Q * u + B * h, Q * u + B * (h + 1)), slice(0, width)
                val = part[B * e:B * (e + 1)] if u else part[:, B * e:B * (e + 1)].T
                terms[place] = terms[place] + val if top else val
            return 0

        lax.fori_loop(0, U, two, 0)

    def sum_of(u):
        wr[2:, OFF[u]:OFF[u] + B] = jnp.zeros((2, B, H), jnp.float32)
        for load in loads[u]:
            load.wait()
        for top in ((0,) if u else (0, H)):
            for h in range(2):
                half_of(u, h, top, K if u else H)
                yield

        def put(k, val):
            t_ref[B * (2 * u + k):B * (2 * u + k + 1), :B * (u + 1)] = val

        yield from net.reduce(acc, fwd, end, Q * u, Q, put, terms, B * (u + 1))

    s0, s1, s2, s3 = [sum_of(u) for u in GROUPS]
    run(chain(s3, s3, s3, rows_1, s2, s3, rows_1, s2, rows_1, s3, s2, rows_1, s2, s3, rows_0, s1, s2, s1, s1, rows_0, s0, s1, s2,
              s0, s1, rows_0, s1, rows_0, s0, s0, s0, s0, s0, s0))
    run(s2, s1, s0)
    net.drain()


def call(kernel, ident, flops, args, in_specs, outs, out_specs, scratch, sems):
    return pl.pallas_call(
        kernel,
        out_shape=[jax.ShapeDtypeStruct(s, jnp.float32) for s in outs],
        in_specs=in_specs,
        out_specs=out_specs,
        scratch_shapes=[*(pltpu.VMEM(s, jnp.float32) for s in scratch), *(pltpu.SemaphoreType.DMA(s) for s in sems)],
        compiler_params=pltpu.CompilerParams(collective_id=ident, has_side_effects=True, vmem_limit_bytes=67 * 10 ** 6),
        cost_estimate=pl.CostEstimate(flops=flops, bytes_accessed=K, transcendentals=0),
    )(*args)


def solution(mesh):
    def local_pass(fac, bar):
        panel, rows, column = (U, ROWS, H), (U, H, H), (U, R, B, B)
        wide_col, cut = (U, R, B, Q), (2, R, (ROWS - Q) // (2 * R), B)
        lr, wc, a, b = call(
            front_kernel, 0, 1, (fac, bar), [VM] * 2, (panel, column, cut, cut), [HB] + [VM] * 3,
            (panel, (R, B, K), (R, B, K), (U, Q, Q), (U, 2, ROWS, B), (U, ROWS, B), (2, ROWS // 2, B), (U, ROWS // 2, B)),
            ((U,), (144,), (144,)))
        sy, w, row_e, row_d, row_o, col_3 = call(
            levels_kernel, 1, 1, (lr, bar, wc, a, b), [HB, HB, VM, VM, VM],
            ((U * K, H), (6, U, U, B, B), rows, rows, rows, wide_col), [HB] * 6,
            ((U, K, B), cut, cut, (2, B, B), (2, B, B), (2, H, H), rows, (U, K, H), rows, (K, B), (U, 2 * R, B, B), rows, rows, column, rows,
             wide_col, column, column, wide_col, (U, 2, Q, B), (U, Q, B), (2, B, B), (U, B, B)),
            ((48,), (208,), (208,), (2,), (2,)))
        m, own = call(
            product_kernel, 2, 1, (sy, w, col_3), [HB] * 3, ((K, H), (U, B, Q)), [VM] * 2,
            ((U * K, H), (6, U, U, B, B), wide_col, (2, U, U, B, Q), (U, K, H), (2, H, H), (U, H, H)), ((16,), (48,), (48,)))
        out, = call(
            gradient_kernel, 3, 1, (m, own, row_e, row_d, row_o), [VM] * 2 + [HB] * 3, ((K, H),), [VM],
            (panel, (U, 2, K, H), (U, K, H), (2, H, H), (U, H, H)), ((16,), (64,), (64,)))
        row, col = lax.broadcasted_iota(jnp.int32, (K, 1), 0), lax.broadcasted_iota(jnp.int32, (1, H), 1)
        row_all = (row // B * R + lax.axis_index('row')) * B + row % B
        col_all = (col // B * 2 * R + lax.axis_index('col')) * B + col % B
        return jnp.where(row_all > col_all, out, jnp.where(row_all == col_all, 0.5 * out, 0.0))

    spec = P(('batch', 'row'), 'col')
    return jax.shard_map(local_pass, mesh=mesh, in_specs=(spec, spec), out_specs=spec, check_vma=False)
```

```python
import jax
import jax.numpy as jnp
from jax import lax
from jax.experimental import pallas as pl
from jax.experimental.pallas import tpu as pltpu
from jax.sharding import PartitionSpec as P

B, Q, H, K, N = 128, 256, 512, 1024, 2048
U, R = 4, 8
GROUPS = tuple(range(U))
OFF = tuple(K * u - B * u * (u - 1) for u in GROUPS)
ROWS = OFF[-1] + Q
HI = lax.Precision.HIGHEST
MESH = pl.DeviceIdType.MESH
VM = pl.BlockSpec(memory_space=pltpu.VMEM)
HB = pl.BlockSpec(memory_space=pl.ANY)
ALL = slice(None)


def mm(a, b):
    return jnp.dot(a, b, precision=HI, preferred_element_type=jnp.float32)


def mm_t(a, b):
    return lax.dot_general(a, b, (((0,), (0,)), ((), ())), precision=HI, preferred_element_type=jnp.float32)


def mod4(v):
    return lax.rem(v + U, U)


def at(start, size=B):
    return pl.ds(start if isinstance(start, int) else pl.multiple_of(start, B), size)


def group(u):
    return slice(OFF[u], OFF[u] + K - Q * u)


def wide(ref, rows, zs=GROUPS):
    return jnp.concatenate([ref[z, rows] for z in zs], axis=1)


def phi(block, ahead):
    diff = B * ahead + lax.broadcasted_iota(jnp.int32, (B, B), 0) - lax.broadcasted_iota(jnp.int32, (B, B), 1)
    return jnp.where(diff > 0, block, jnp.where(diff == 0, 0.5 * block, 0.0))


def step(g):
    return next(g, g) is not g


def run(*gathers, behind=()):
    live = list(gathers)
    while live:
        live = [g for g in live if step(g)]
        for g in behind:
            step(g)


def chain(*gathers):
    for g in gathers:
        step(g)
        yield


class Net:
    def __init__(self, send_sems, recv_sems):
        self.send_sems, self.recv_sems = send_sems, recv_sems
        self.r, self.c = lax.axis_index('row'), lax.axis_index('col')
        self.x, self.core = self.r // 2, lax.rem(self.r, 2)
        self.z, self.y = self.c // U, lax.rem(self.c, U)
        self.right, self.left = self.device(x=mod4(self.x + 1)), self.device(x=mod4(self.x - 1))
        self.partner = self.device(core=1 - self.core)
        self.zy = [self.device(y=mod4(self.y + 1)), self.device(y=mod4(self.y - 1)),
                   self.device(z=mod4(self.z + 1)), self.device(z=mod4(self.z - 1))]
        self.far_z = self.device(z=mod4(self.z + 2))
        self.copies = []

    def device(self, **place):
        x, core, y, z = [place.get(k, getattr(self, k)) for k in ('x', 'core', 'y', 'z')]
        return {'col': U * z + y, 'row': 2 * x + core}

    def barrier(self, *peers):
        sem = pltpu.get_barrier_semaphore()
        for peer in peers:
            pl.semaphore_signal(sem, inc=1, device_id=peer, device_id_type=MESH)
        pl.semaphore_wait(sem, len(peers))

    def line(self):
        places = [(mod4(self.x + d // 2), lax.rem(self.core + d, 2)) for d in range(1, R)]
        return [(self.device(x=x, core=core), 2 * x + core) for x, core in places]

    def plane(self):
        places = [(mod4(self.z + d // U), mod4(self.y + d % U)) for d in range(1, U * U)]
        return [(self.device(z=z, y=y), U * z + y) for z, y in places]

    def copy(self, ref, peer, dst=None):
        k = len(self.copies)
        copy = pltpu.make_async_remote_copy(
            src_ref=ref, dst_ref=ref if dst is None else dst, send_sem=self.send_sems.at[k], recv_sem=self.recv_sems.at[k],
            device_id=peer, device_id_type=MESH)
        copy.start()
        self.copies.append(copy)
        return copy

    def drain(self):
        for copy in self.copies:
            copy.wait_send()

    def gather_x(self, ref, axis=1, first=0):
        half = ref.shape[1 - axis] // 2

        def view(r, part=None):
            other = ALL if part is None else pl.ds(part * half, half)
            return ref.at[(other, first + r) if axis else (r, other)]

        near_r, near_l, far = [2 * mod4(self.x + d) + self.core for d in (1, -1, 2)]
        to_right, to_left = [], []
        for part in range(2):
            to_right.append(self.copy(view(self.r, part), self.right))
            to_left.append(self.copy(view(self.r, 1 - part), self.left))
        over = [self.copy(view(self.r), self.partner)]
        yield
        to_right[0].wait_recv()
        far_0 = self.copy(view(near_l, 0), self.right)
        to_left[0].wait_recv()
        far_1 = self.copy(view(near_r, 1), self.left)
        yield
        to_right[1].wait_recv()
        over.append(self.copy(view(near_l), self.partner))
        to_left[1].wait_recv()
        over.append(self.copy(view(near_r), self.partner))
        far_0.wait_recv()
        over.append(self.copy(view(far, 0), self.partner))
        far_1.wait_recv()
        over.append(self.copy(view(far, 1), self.partner))
        yield
        for copy in over:
            copy.wait_recv()
        yield

    def gather_zy(self, ref, start, count, first, thin=0):
        yp, ym, zp, zm = self.zy
        y, z = self.y, self.z
        y_m, y_p, z_m, z_p = mod4(y - 1), mod4(y + 1), mod4(z - 1), mod4(z + 1)

        def cut(top, size):
            return pl.ds(top, size // 2), pl.ds(top + size // 2, size // 2), pl.ds(top, size)

        a_0, a_1, a_all = cut(start + count - first, first)
        b_0, b_1, b_all = cut(start, count - first)
        c_0, c_1, c_all = cut(start + thin, count - first - thin)
        t_0, t_1, t_all = cut(start, thin)
        front = slice(0, 2)

        def both(zs, rows, to, ys=None, zs_back=None, rows_back=None, ys_back=None):
            lane, lane_back = [ALL if v is None else at(B * v) for v in (ys, ys_back)]
            forth = ref.at[zs, rows, lane]
            back = forth if rows_back is None else ref.at[zs_back, rows_back, lane_back]
            return self.copy(forth, to[0]), self.copy(back, to[1])

        def done(*copies):
            for copy in copies:
                copy.wait_recv()

        on_y, on_z = (yp, ym), (zp, zm)
        a, b = both(z, a_all, on_y, y), both(z, b_all, on_z, y)
        yield
        done(*a)
        a = both(z, a_0, on_y, y_m, z, a_1, y_p)
        done(*b)
        b = both(z_m, b_0, on_z, y, z_p, b_1, y)
        yield
        done(*a)
        a = both(z, a_all, on_z)
        done(*b)
        b = both(ALL, c_all, on_y, y) if count > first + thin else ()
        if thin:
            b += both(front, t_all, on_y, y)
        yield
        done(*a)
        a = both(z_m, a_0, on_z, None, z_p, a_1)
        done(*b)
        b = both(ALL, c_0, on_y, y_m, ALL, c_1, y_p) if count > first + thin else ()
        if thin:
            b += both(front, t_0, on_y, y_m, front, t_1, y_p)
        yield
        done(*a, *b)
        yield

    def gather_y(self, ref, start, count):
        half, y = count // 2, self.y
        yp, ym = self.zy[:2]

        def view(ys, part=None):
            return ref.at[pl.ds(start, count) if part is None else pl.ds(start + part * half, half), at(B * ys)]

        near = self.copy(view(y), yp), self.copy(view(y), ym)
        yield
        near[0].wait_recv()
        far_0 = self.copy(view(mod4(y - 1), 0), yp)
        near[1].wait_recv()
        far_1 = self.copy(view(mod4(y + 1), 1), ym)
        yield
        far_0.wait_recv()
        far_1.wait_recv()
        yield

    def spread_z(self, *parts):
        sent = []
        for d, peer in ((1, self.zy[2]), (-1, self.zy[3]), (2, self.far_z)):
            for src, dst in parts:
                sent.append((self.copy(src(mod4(self.z + d)), peer, dst(self.z)), dst(mod4(self.z - d))))
        yield
        over = []
        for copy, got in sent:
            copy.wait_recv()
            over.append(self.copy(got, self.partner))
        yield
        for copy in over:
            copy.wait_recv()
        yield

    def swap(self, src, dst, across):
        def piece(k):
            return (k // R, lax.rem(k, R)) if across else (ALL, k)

        others, me = (self.plane(), self.c) if across else (self.line(), self.r)
        sent = [self.copy(src.at[piece(place)], peer, dst.at[piece(me)]) for peer, place in others]
        dst[piece(me)] = src[piece(me)]
        yield
        for copy in sent:
            copy.wait_recv()
        yield

    def reduce(self, acc, fwd, end, start, count, put, terms=None, width=None):
        half, lanes = count // 2, ALL if width is None else pl.ds(0, width)
        rows, lo, hi, mid = pl.ds(start, count), pl.ds(start, half), pl.ds(start + half, half), pl.ds(start // 2, half)
        me, right, left = (self.z, *self.zy[2:]) if terms is None else (self.x, self.right, self.left)
        far, nxt, prv = [mod4(me + d) for d in (2, 1, -1)]
        if terms is not None:
            over = self.copy(terms.at[:, 1 - self.core, rows, lanes], self.partner, acc.at[:, rows, lanes])
            yield
            over.wait_recv()

        def settle(k):
            if terms is not None:
                acc[k, rows, lanes] = acc[k, rows, lanes] + terms[k, self.core, rows, lanes]

        def send(k, part, to, ref, slot):
            return self.copy(acc.at[k, part, lanes], to, ref.at[slot, mid, lanes])

        settle(far)
        far_r, far_l = send(far, lo, right, fwd, 0), send(far, hi, left, fwd, 1)
        settle(nxt)
        settle(prv)
        last = [send(nxt, hi, right, end, 0), send(prv, lo, left, end, 1)]
        settle(me)
        yield
        far_r.wait_recv()
        acc[nxt, lo, lanes] = acc[nxt, lo, lanes] + fwd[0, mid, lanes]
        last.append(send(nxt, lo, right, end, 2))
        far_l.wait_recv()
        acc[prv, hi, lanes] = acc[prv, hi, lanes] + fwd[1, mid, lanes]
        last.append(send(prv, hi, left, end, 3))
        yield
        for copy in last:
            copy.wait_recv()
        blocks = count // B
        for k in range(blocks):
            one, two = (1, 2) if 2 * k < blocks else (0, 3)
            row = pl.ds(start // 2 + B * (k % (blocks // 2)), B)
            put(k, acc[me, pl.ds(start + B * k, B), lanes] + (end[one, row, lanes] + end[two, row, lanes]))
        yield


def invert(w_ref, l_ref, tmp_ref):
    row = lax.broadcasted_iota(jnp.int32, (Q, Q), 0)
    col = lax.broadcasted_iota(jnp.int32, (Q, Q), 1)
    w_ref[...] = jnp.zeros_like(w_ref)

    def block(ref, i, j, size):
        return ref[i // B:(i + size) // B, :, j:j + size].reshape(size, size)

    def put(i, j, size, val):
        w_ref[i // B:(i + size) // B, :, j:j + size] = val.reshape(size // B, B, size)

    corners = range(0, K, Q)
    for k in corners:
        a = block(l_ref, k, k, Q)
        diag = jnp.where(row == col, a, 0.0)
        down, across = 1.0 / jnp.sum(diag, axis=1, keepdims=True), 1.0 / jnp.sum(diag, axis=0, keepdims=True)
        low = (row // 2 == col // 2) & (row > col)
        put(k, k, Q, jnp.where(row == col, down, jnp.where(low, -a * down * across, 0.0)))
    size = 2
    while size < Q:
        pair = (row // (2 * size) == col // (2 * size)) & (row // size > col // size)
        for k in corners:
            tmp_ref[k // Q] = mm(jnp.where(pair, block(l_ref, k, k, Q), 0.0), block(w_ref, k, k, Q))
        yield
        for k in corners:
            w = block(w_ref, k, k, Q)
            put(k, k, Q, w - mm(w, tmp_ref[k // Q]))
        yield
        size *= 2
    while size < K:
        for j in range(0, K, 2 * size):
            i = j + size
            part = mm(block(l_ref, i, j, size), block(w_ref, j, j, size))
            put(i, j, size, -mm(block(w_ref, i, i, size), part))
            yield
        size *= 2


def pieces(ref, u, v):
    top, n = B * (u * (u + 1) // 2 + v - 1), ref.shape[2]
    i, low = top // n, top % n
    cut = min(B, n - low)
    first = [(slice(0, cut), (i, slice(low, low + cut)))]
    return first if cut == B else first + [(slice(cut, B), (i + 1, slice(0, B - cut)))]


def inner(net, u, start, panel, top, bar, terms):
    def two(k, _):
        h, x = k // U, lax.rem(k, U)
        a, b = panel[2 * h + x // 2, top:top + K - Q * u, at(Q * lax.rem(x, 2), Q)], bar[Q * u:, :B * (u + 1)]
        p = mm_t(a, b) if u else mm_t(b, a)
        for e in range(2):
            for v in range(u + 1):
                val = p[B * e:B * (e + 1), B * v:B * (v + 1)] if u else p[:, B * e:B * (e + 1)].T
                terms[x, e, at(start + Q * v + B * h), :] = phi(val, 2 * k + e - net.c) if v == u else val
        return 0

    lax.fori_loop(0, R, two, 0)


def front_kernel(l_ref, bar_ref, lr_ref, col_ref, a_ref, b_ref, lv, lss, wss, tmp, terms, acc, fwd, end, dma_sems, send_sems, recv_sems):
    net = Net(send_sems, recv_sems)
    r, c, y, z, core = net.r, net.c, net.y, net.z, net.core
    half, zz = z // 2, lax.rem(z, 2)
    ways = (1, 2, 3)
    others = [net.device(y=mod4(y + d)) for d in ways]
    for u in GROUPS:
        lv[2:, OFF[u]:OFF[u] + B] = jnp.zeros((2, B, H), jnp.float32)
    net.barrier(*[peer for peer, _ in net.line()], *others, *net.zy[2:])

    strip = at(B * (U * zz + y))

    def own(u):
        return at(B * (2 * u + half)), at(B * u)

    sent = [net.copy(l_ref.at[own(mod4(y + d))], other, lss.at[r, :, strip]) for d, other in zip(ways, others)]
    lss[r, :, strip] = l_ref[own(y)]
    for u in GROUPS:
        lv[z, group(u), at(B * y)] = l_ref[Q * u:, B * u:B * (u + 1)]
    g = [net.gather_zy(lv, OFF[u], K - Q * u, (K - Q * u - 96) // 2, B) for u in GROUPS]
    run(chain(g[3], g[2]))
    for copy in sent:
        copy.wait_recv()
    pair = net.copy(lss.at[r, :, at(H * zz, H)], net.device(z=2 * half + 1 - zz))
    run(chain(g[1], g[0], g[3], g[3]))
    pair.wait_recv()

    order = iter([2, 2, 3, 1, 3, 2, 1, 2, 0, 1, 0, 1])
    stores = []

    def tick():
        u = next(order, None)
        if u is not None:
            step(g[u])

    def keep(u):
        stores.append(pltpu.make_async_copy(lv.at[:, group(u)], lr_ref.at[:, group(u)], dma_sems.at[u]))
        stores[-1].start()

    def begin(u):
        start = ROWS - Q * (u + 1) * (u + 2) // 2
        inner(net, u, start, lv, OFF[u], bar_ref, terms)

        def put(k, val):
            v, h = k // 2, k % 2
            for rows, place in pieces(a_ref, u, v):
                a_ref[(h, *place)] = val[rows]

        keep(u)
        return net.reduce(acc, fwd, end, start, Q * (u + 1), put, terms)

    strips = net.gather_x(lss, axis=0)
    step(strips)
    for _ in range(3):
        tick()
    step(strips)
    for _ in range(2):
        tick()
    step(strips)
    s3 = begin(3)
    run(strips)
    step(s3)
    for k, _ in enumerate(invert(wss, lss, tmp)):
        if k % 4 == 1:
            tick()
        if k % 6 == 5:
            step(s3)
    s2 = begin(2)
    step(s2)
    tick()

    sent = [net.copy(wss.at[r, :, at(B * (U * zz + mod4(y + d)))], other, col_ref.at[y, r]) for d, other in zip(ways, others)]
    col_ref[y, r] = wss[r, :, strip]
    step(s2)
    tick()
    tick()
    s1 = begin(1)
    run(chain(s3, s1, s2, s1))
    for copy in sent:
        copy.wait_recv()
    columns = net.gather_x(col_ref)
    flip = net.swap(a_ref, b_ref, False)
    run(chain(columns, s2, s1, g[0], columns, s1, flip, columns, columns, g[0], flip))
    keep(0)
    for copy in stores:
        copy.wait()
    net.drain()


def levels_kernel(lr_ref, bar_ref, wc_ref, a, b, sy_ref, w_ref, row_e, row_d, row_o, col_3,
                  own, d, back, s_top, top_back, la, lb, l0, l1, bv, cd, re, rd, co, ro, c3, x1, x2, x3, terms, acc, fwd, end, dma_sems, send_sems, recv_sems, t_send, t_recv):
    net = Net(send_sems, recv_sems)
    r, c, y, z = net.r, net.c, net.y, net.z
    sems = iter(range(32))

    def local(a, b):
        copy = pltpu.make_async_copy(a, b, dma_sems.at[next(sems)])
        copy.start()
        return copy

    load_a = [local(lr_ref.at[0:2, OFF[u] + B:OFF[u] + Q], la.at[:, B * u:B * (u + 1)]) for u in GROUPS]
    load_0 = [local(lr_ref.at[:, group(0)], l0), local(bar_ref.at[:, 0:B], bv)]
    load_b = [local(lr_ref.at[:, OFF[u] + Q:OFF[u] + H], lb.at[:, B * u:B * (u + 2)]) for u in (0, 2)]
    load_c = local(lr_ref.at[:, OFF[1] + Q:OFF[2]], l1)
    net.barrier(*[peer for peer, _ in net.line() + net.plane()])
    half_c, row_c = c // R, lax.rem(c, R)
    swap = [{'row': row_c, 'col': r + R * h} for h in range(2)]
    away = [(row_c != r) | (half_c != h) for h in range(2)]

    def block(ref, h, u, v):
        return jnp.concatenate([ref[(h, *place)] for _, place in pieces(ref, u, v)], axis=0)

    def trade(h, slot):
        return pltpu.make_async_remote_copy(src_ref=s_top.at[h], dst_ref=top_back.at[slot], send_sem=t_send.at[h],
                                            recv_sem=t_recv.at[slot], device_id=swap[h], device_id_type=MESH)

    low = c < R
    stores = []
    for u in GROUPS:
        re[z, B * u:B * (u + 1), at(B * y)] = wc_ref[u, r]
    diag = net.gather_zy(re, 0, H, Q)
    step(diag)
    early = [net.gather_y(sy_ref, K * v + Q * (v + 1), K - Q * (v + 1)) for v in range(U - 1)]
    late = net.gather_y(sy_ref, 3 * K, K)
    e0, e1, e2 = early
    half = pl.ds(2 * net.core, 2)

    def odd(rows):
        return jnp.concatenate([rd[0, rows], rd[1, rows], re[2, rows], re[3, rows]], axis=1)

    for u in GROUPS:
        load_a[u].wait()
        cd[u, 0:R] = jnp.where(low, wc_ref[u], 0.0)
        x1[u, r] = mm(wide(la, slice(B * u, B * (u + 1)), (0, 1)), cd[u, 0:R].reshape(K, B))
    strips = net.gather_x(x1)
    flip = net.swap(b, d, True)
    run(chain(strips, diag, diag, flip))
    for u in range(1, U):
        for h in range(2):
            for v in range(u + 1):
                own[v, B * (2 * u + h):B * (2 * u + h + 1), :] = block(a, h, u, v)
    places = [local(own.at[v, Q * (v + 1):], sy_ref.at[K * v + Q * (v + 1):K * (v + 1), at(B * y)]) for v in range(U - 1)]
    step(strips)
    for load in load_0:
        load.wait()
    inner(net, 0, 0, l0, 0, bv, terms)
    for place in places:
        place.wait()

    def put(k, val):
        s_top[k] = val

    run(strips, net.reduce(acc, fwd, end, 0, Q, put, terms), behind=[chain(diag, e0, diag)])
    run(diag)
    for h in range(2):
        @pl.when(away[h])
        def _():
            trade(h, half_c).start()

        @pl.when(jnp.logical_not(away[h]))
        def _():
            top_back[h] = s_top[h]
    stores.append(local(re, row_e))
    for u in GROUPS:
        w = -mm(wide(re, slice(B * u, B * (u + 1)), (2, 3)), x1[u].reshape(K, B))
        w = jnp.where(low, w, wc_ref[u, r])
        cd[u, R + r] = w
        rd[z, B * u:B * (u + 1), at(B * y)] = w
    rows = net.gather_zy(rd, 0, H, B, H - B)
    step(rows)
    run(net.gather_x(cd, first=R), behind=[chain(rows, e1, rows, e0)])
    stores.append(local(cd.at[:, pl.ds(U * z, U)], w_ref.at[0:U, z]))
    out = net.spread_z((lambda k: cd.at[:, pl.ds(U * k + 2 * net.core, 2)], lambda k: w_ref.at[0:U, k, half]))
    step(out)
    step(flip)
    flip = net.swap(d, back, False)
    step(flip)

    for q in range(2):
        load_b[q].wait()
        x2[2 * q:2 * q + 2, r] = mm(wide(lb, slice(Q * q, Q * (q + 1))), cd[2 * q].reshape(N, B)).reshape(2, B, B)
    run(net.gather_x(x2), behind=[chain(e1, rows, e2, e1, e0)])
    run(rows)
    stores.append(local(rd, row_d))
    for q in range(2):
        at_u = slice(B * (2 * q + 1), B * (2 * q + 2))
        tops = (mm(wide(re, at_u, (0, 1)), x2[2 * q].reshape(K, B)), mm(odd(at_u), x2[2 * q:2 * q + 2].reshape(N, B)))
        for i, w in enumerate(tops):
            co[2 * q + i, r] = -w
            ro[z, B * (2 * q + i):B * (2 * q + i + 1), at(B * y)] = -w
    rows = net.gather_zy(ro, 0, H, Q)
    step(rows)
    strips = net.gather_x(co)
    step(strips)

    run(strips, behind=[chain(rows, e2, rows, out)])
    parts = []
    for q in range(2):
        stores.append(local(co.at[2 * q + z // 2, pl.ds(U * lax.rem(z, 2), U)], w_ref.at[U + q, z]))
        parts.append((lambda k, q=q: co.at[2 * q + k // 2, pl.ds(U * lax.rem(k, 2) + 2 * net.core, 2)],
                      lambda k, q=q: w_ref.at[U + q, k, half]))
    out_o = net.spread_z(*parts)

    load_c.wait()
    x3[:, r] = mm(wide(l1, ALL), jnp.concatenate([co[0:2].reshape(N, B), cd[1].reshape(N, B)], 1)).reshape(U, B, Q)
    x3[:, r, :, :B] = x3[:, r, :, :B] + mm(wide(l0, slice(H, K)), cd[0].reshape(N, B)).reshape(U, B, B)
    strips = net.gather_x(x3)
    step(strips)

    step(flip)
    for h in range(2):
        own[0, B * h:B * (h + 1), :] = s_top[h]
    for s in range(2):
        @pl.when(away[s])
        def _():
            trade(s, s).wait_recv()
        for u in GROUPS:
            for v in range(u + 1):
                at_t = slice(B * (2 * v + s), B * (2 * v + s + 1))
                val = (block(back, s, u, v) if u else top_back[s]).T
                own[u, at_t, :] = own[u, at_t, :] + val if u == v else val
    places = [local(own.at[v, 0:Q * (v + 1)], sy_ref.at[K * v:K * v + Q * (v + 1), at(B * y)]) for v in GROUPS]
    run(strips, behind=[chain(rows, out, e2)])
    run(rows)
    for place in places:
        place.wait()
    step(late)
    step(out_o)
    stores.append(local(ro, row_o))
    for i in GROUPS:
        u = 2 + i // 2
        at_u = slice(B * u, B * (u + 1))
        if i % 2 == 0:
            w = mm(wide(re, at_u, (0, 1)), x3[i].reshape(K, Q))
        else:
            w = mm(odd(at_u), x3[i - 1:i + 1].reshape(N, Q))
        if i >= 2:
            w = w + mm(wide(ro, slice(B * i, B * (i + 1))), x3[0:2].reshape(N, Q))
        c3[i, r] = -w
    run(net.gather_x(c3), behind=[chain(late, out_o)])
    run(late, out_o)
    stores.append(local(c3, col_3))
    for h in range(2):
        @pl.when(away[h])
        def _():
            trade(h, half_c).wait_send()
    for copy in stores:
        copy.wait()
    net.drain()


def product_kernel(sy_ref, w_ref, c3_ref, m_ref, own_ref, sy, w, c3, wide_w, acc, fwd, end, dma_sems, send_sems, recv_sems):
    net = Net(send_sems, recv_sems)
    z = net.z
    start = [slice(K * v, K * v + Q * (v + 1)) for v in range(U - 1)]
    rest = [slice(K * v + Q * (v + 1), K * (v + 1)) for v in range(U - 1)] + [slice(3 * K, U * K)]
    loads = [(c3_ref, c3), *[(sy_ref.at[some], sy.at[some]) for some in (*start, *rest)], (w_ref, w)]
    loads = [pltpu.make_async_copy(a, b, dma_sems.at[k]) for k, (a, b) in enumerate(loads)]
    for load in loads:
        load.start()
    for load in loads[:U]:
        load.wait()
    net.barrier(*net.zy, net.far_z, net.partner)
    half = pl.ds(2 * net.core, 2)
    parts = []
    for v in range(2):
        wide_w[v, z] = c3[2 * v + z // 2, pl.ds(U * lax.rem(z, 2), U)]
        parts.append((lambda k, v=v: c3.at[2 * v + k // 2, pl.ds(U * lax.rem(k, 2) + 2 * net.core, 2)],
                      lambda k, v=v: wide_w.at[v, k, half]))
    out = net.spread_z(*parts)
    step(out)
    own_ref[...] = c3[:, net.r]
    m0, m1, m2 = moves = [net.gather_y(sy, K * v, Q * (v + 1)) for v in range(U - 1)]
    run(chain(m2, m1))
    m_ref[...] = jnp.zeros_like(m_ref)

    def block(v, col):
        if v >= 2 and col < 2:
            some = [wide_w[v - 2, k, :, :, B * col:B * (col + 1)] for k in GROUPS]
        else:
            some = [w[v if v == col else U + v // 2, k] for k in GROUPS]
        return jnp.concatenate([x.reshape(H, B) for x in some], axis=1)

    def terms(u, col, groups, more=False):
        part = sum(mm(sy[K * v + Q * u:K * v + Q * (u + 1), :], block(v, col)) for v in groups)
        for k in GROUPS:
            place = k, slice(Q * u, Q * (u + 1)), slice(B * col, B * (col + 1))
            val = part[:, B * k:B * (k + 1)]
            acc[place] = acc[place] + val if more else val

    def sum_of(u):
        def put(k, val):
            m_ref[Q * u + B * k:Q * u + B * (k + 1), :B * (u + 1)] = val

        return net.reduce(acc, fwd, end, Q * u, Q, put, width=B * (u + 1))

    for load in loads[U:]:
        load.wait()
    sums = []
    for u in GROUPS[::-1]:
        for col in range(u + 1):
            terms(u, col, range(col, U if col >= 2 else 2))
        if u == 3:
            run(chain(m2, m0, m1, m2, out))
            run(out)
        for col in range(min(u + 1, 2)):
            terms(u, col, range(2, U), True)
        for s in sums:
            step(s)
        sums.append(sum_of(u))
        step(sums[-1])
        run(chain(m1, m0))
    run(*moves, *sums)
    net.drain()


def gradient_kernel(x_ref, own_ref, re_ref, rd_ref, ro_ref, t_ref,
                    wr, terms, acc, fwd, end, dma_sems, send_sems, recv_sems):
    net = Net(send_sems, recv_sems)
    loads = [[(re_ref.at[0:2, B * u:B * (u + 1)], wr.at[0:2, OFF[u]:OFF[u] + B]),
              *[(ref.at[zs, B * u:B * (u + 1)], wr.at[zs, OFF[u] + B:OFF[u] + Q])
                for ref, zs in ((rd_ref, slice(0, 2)), (re_ref, slice(2, U)))]] for u in GROUPS]
    loads[2] += [(ro_ref.at[:, Q:], wr.at[:, OFF[2] + Q:OFF[3]])]
    loads[0] += [(ro_ref.at[:, :Q], wr.at[:, Q:H])]
    sems = iter(range(16))
    loads = [[pltpu.make_async_copy(a, b, dma_sems.at[next(sems)]) for a, b in some] for some in loads]
    for some in loads[::-1]:
        for load in some:
            load.start()
    net.barrier(net.right, net.left, net.partner, *net.zy)
    for i in GROUPS:
        for k, top in enumerate((H, OFF[1] + Q)):
            wr[net.z, top + B * i:top + B * (i + 1), at(B * net.y)] = own_ref[i, :, B * k:B * (k + 1)]
    rows_0, rows_1 = net.gather_zy(wr, H, H, Q), net.gather_zy(wr, OFF[1] + Q, H, Q)
    step(rows_1)
    step(rows_0)

    def half_of(u, h, top=0, rows=K):
        width = B * (u + 1)
        some = slice(OFF[u] + top, min(OFF[u] + top + rows, OFF[u] + K - Q * u))
        these = slice(Q * u + top, Q * u + top + some.stop - some.start)

        def two(x, _):
            a, b = wr[2 * h + x // 2, some, at(Q * lax.rem(x, 2), Q)], x_ref[these, :width]
            part = mm_t(a, b) if u else mm_t(b, a)
            for e in range(2):
                place = x, e, slice(Q * u + B * h, Q * u + B * (h + 1)), slice(0, width)
                val = part[B * e:B * (e + 1)] if u else part[:, B * e:B * (e + 1)].T
                terms[place] = terms[place] + val if top else val
            return 0

        lax.fori_loop(0, U, two, 0)

    def sum_of(u):
        wr[2:, OFF[u]:OFF[u] + B] = jnp.zeros((2, B, H), jnp.float32)
        for load in loads[u]:
            load.wait()
        for top in ((0,) if u else (0, H)):
            for h in range(2):
                half_of(u, h, top, K if u else H)
                yield

        def put(k, val):
            t_ref[B * (2 * u + k):B * (2 * u + k + 1), :B * (u + 1)] = val

        yield from net.reduce(acc, fwd, end, Q * u, Q, put, terms, B * (u + 1))

    s0, s1, s2, s3 = [sum_of(u) for u in GROUPS]
    run(chain(s3, s3, s3, rows_1, s2, s3, rows_1, s2, rows_1, s3, s2, rows_1, s2, s3, rows_0, s1, s2, s1, s1, rows_0, s0, s1, s2,
              s0, s1, rows_0, s1, rows_0, s0, s0, s0, s0, s0, s0))
    run(s2, s1, s0)
    net.drain()


def call(kernel, ident, flops, args, in_specs, outs, out_specs, scratch, sems):
    return pl.pallas_call(
        kernel,
        out_shape=[jax.ShapeDtypeStruct(s, jnp.float32) for s in outs],
        in_specs=in_specs,
        out_specs=out_specs,
        scratch_shapes=[*(pltpu.VMEM(s, jnp.float32) for s in scratch), *(pltpu.SemaphoreType.DMA(s) for s in sems)],
        compiler_params=pltpu.CompilerParams(collective_id=ident, has_side_effects=True, vmem_limit_bytes=67 * 10 ** 6),
        cost_estimate=pl.CostEstimate(flops=flops, bytes_accessed=K, transcendentals=0),
    )(*args)


def solution(mesh):
    def local_pass(fac, bar):
        panel, rows, column = (U, ROWS, H), (U, H, H), (U, R, B, B)
        wide_col, cut = (U, R, B, Q), (2, R, (ROWS - Q) // (2 * R), B)
        lr, wc, a, b = call(
            front_kernel, 0, 1, (fac, bar), [VM] * 2, (panel, column, cut, cut), [HB] + [VM] * 3,
            (panel, (R, B, K), (R, B, K), (U, Q, Q), (U, 2, ROWS, B), (U, ROWS, B), (2, ROWS // 2, B), (U, ROWS // 2, B)),
            ((U,), (144,), (144,)))
        sy, w, row_e, row_d, row_o, col_3 = call(
            levels_kernel, 1, 1, (lr, bar, wc, a, b), [HB, HB, VM, VM, VM],
            ((U * K, H), (6, U, U, B, B), rows, rows, rows, wide_col), [HB] * 6,
            ((U, K, B), cut, cut, (2, B, B), (2, B, B), (2, H, H), rows, (U, K, H), rows, (K, B), (U, 2 * R, B, B), rows, rows, column, rows,
             wide_col, column, column, wide_col, (U, 2, Q, B), (U, Q, B), (2, B, B), (U, B, B)),
            ((48,), (208,), (208,), (2,), (2,)))
        m, own = call(
            product_kernel, 2, 1, (sy, w, col_3), [HB] * 3, ((K, H), (U, B, Q)), [VM] * 2,
            ((U * K, H), (6, U, U, B, B), wide_col, (2, U, U, B, Q), (U, K, H), (2, H, H), (U, H, H)), ((16,), (48,), (48,)))
        out, = call(
            gradient_kernel, 3, 1, (m, own, row_e, row_d, row_o), [VM] * 2 + [HB] * 3, ((K, H),), [VM],
            (panel, (U, 2, K, H), (U, K, H), (2, H, H), (U, H, H)), ((16,), (64,), (64,)))
        row, col = lax.broadcasted_iota(jnp.int32, (K, 1), 0), lax.broadcasted_iota(jnp.int32, (1, H), 1)
        row_all = (row // B * R + lax.axis_index('row')) * B + row % B
        col_all = (col // B * 2 * R + lax.axis_index('col')) * B + col % B
        return jnp.where(row_all > col_all, out, jnp.where(row_all == col_all, 0.5 * out, 0.0))

    spec = P(('batch', 'row'), 'col')
    return jax.shard_map(local_pass, mesh=mesh, in_specs=(spec, spec), out_specs=spec, check_vma=False)
```

```python
import jax
import jax.numpy as jnp
from jax import lax
from jax.experimental import pallas as pl
from jax.experimental.pallas import tpu as pltpu
from jax.sharding import PartitionSpec as P

B, Q, H, K, N = 128, 256, 512, 1024, 2048
U, R = 4, 8
GROUPS = tuple(range(U))
OFF = tuple(K * u - B * u * (u - 1) for u in GROUPS)
ROWS = OFF[-1] + Q
HI = lax.Precision.HIGHEST
MESH = pl.DeviceIdType.MESH
VM = pl.BlockSpec(memory_space=pltpu.VMEM)
HB = pl.BlockSpec(memory_space=pl.ANY)
ALL = slice(None)


def mm(a, b):
    return jnp.dot(a, b, precision=HI, preferred_element_type=jnp.float32)


def mm_t(a, b):
    return lax.dot_general(a, b, (((0,), (0,)), ((), ())), precision=HI, preferred_element_type=jnp.float32)


def mod4(v):
    return lax.rem(v + U, U)


def at(start, size=B):
    return pl.ds(start if isinstance(start, int) else pl.multiple_of(start, B), size)


def group(u):
    return slice(OFF[u], OFF[u] + K - Q * u)


def wide(ref, rows, zs=GROUPS):
    return jnp.concatenate([ref[z, rows] for z in zs], axis=1)


def phi(block, ahead):
    diff = B * ahead + lax.broadcasted_iota(jnp.int32, (B, B), 0) - lax.broadcasted_iota(jnp.int32, (B, B), 1)
    return jnp.where(diff > 0, block, jnp.where(diff == 0, 0.5 * block, 0.0))


def step(g):
    return next(g, g) is not g


def run(*gathers, behind=()):
    live = list(gathers)
    while live:
        live = [g for g in live if step(g)]
        for g in behind:
            step(g)


def chain(*gathers):
    for g in gathers:
        step(g)
        yield


class Net:
    def __init__(self, send_sems, recv_sems):
        self.send_sems, self.recv_sems = send_sems, recv_sems
        self.r, self.c = lax.axis_index('row'), lax.axis_index('col')
        self.x, self.core = self.r // 2, lax.rem(self.r, 2)
        self.z, self.y = self.c // U, lax.rem(self.c, U)
        self.right, self.left = self.device(x=mod4(self.x + 1)), self.device(x=mod4(self.x - 1))
        self.partner = self.device(core=1 - self.core)
        self.zy = [self.device(y=mod4(self.y + 1)), self.device(y=mod4(self.y - 1)),
                   self.device(z=mod4(self.z + 1)), self.device(z=mod4(self.z - 1))]
        self.far_z = self.device(z=mod4(self.z + 2))
        self.copies = []

    def device(self, **place):
        x, core, y, z = [place.get(k, getattr(self, k)) for k in ('x', 'core', 'y', 'z')]
        return {'col': U * z + y, 'row': 2 * x + core}

    def barrier(self, *peers):
        sem = pltpu.get_barrier_semaphore()
        for peer in peers:
            pl.semaphore_signal(sem, inc=1, device_id=peer, device_id_type=MESH)
        return lambda: pl.semaphore_wait(sem, len(peers))

    def line(self):
        places = [(mod4(self.x + d // 2), lax.rem(self.core + d, 2)) for d in range(1, R)]
        return [(self.device(x=x, core=core), 2 * x + core) for x, core in places]

    def plane(self):
        places = [(mod4(self.z + d // U), mod4(self.y + d % U)) for d in range(1, U * U)]
        return [(self.device(z=z, y=y), U * z + y) for z, y in places]

    def copy(self, ref, peer, dst=None):
        k = len(self.copies)
        copy = pltpu.make_async_remote_copy(
            src_ref=ref, dst_ref=ref if dst is None else dst, send_sem=self.send_sems.at[k], recv_sem=self.recv_sems.at[k],
            device_id=peer, device_id_type=MESH)
        copy.start()
        self.copies.append(copy)
        return copy

    def drain(self):
        for copy in self.copies:
            copy.wait_send()

    def gather_x(self, ref, axis=1, first=0):
        half = ref.shape[1 - axis] // 2

        def view(r, part=None):
            other = ALL if part is None else pl.ds(part * half, half)
            return ref.at[(other, first + r) if axis else (r, other)]

        near_r, near_l, far = [2 * mod4(self.x + d) + self.core for d in (1, -1, 2)]
        to_right, to_left = [], []
        for part in range(2):
            to_right.append(self.copy(view(self.r, part), self.right))
            to_left.append(self.copy(view(self.r, 1 - part), self.left))
        over = [self.copy(view(self.r), self.partner)]
        yield
        to_right[0].wait_recv()
        far_0 = self.copy(view(near_l, 0), self.right)
        to_left[0].wait_recv()
        far_1 = self.copy(view(near_r, 1), self.left)
        yield
        to_right[1].wait_recv()
        over.append(self.copy(view(near_l), self.partner))
        to_left[1].wait_recv()
        over.append(self.copy(view(near_r), self.partner))
        far_0.wait_recv()
        over.append(self.copy(view(far, 0), self.partner))
        far_1.wait_recv()
        over.append(self.copy(view(far, 1), self.partner))
        yield
        for copy in over:
            copy.wait_recv()
        yield

    def gather_zy(self, ref, start, count, first, thin=0):
        yp, ym, zp, zm = self.zy
        y, z = self.y, self.z
        y_m, y_p, z_m, z_p = mod4(y - 1), mod4(y + 1), mod4(z - 1), mod4(z + 1)

        def cut(top, size):
            return pl.ds(top, size // 2), pl.ds(top + size // 2, size // 2), pl.ds(top, size)

        a_0, a_1, a_all = cut(start + count - first, first)
        b_0, b_1, b_all = cut(start, count - first)
        c_0, c_1, c_all = cut(start + thin, count - first - thin)
        t_0, t_1, t_all = cut(start, thin)
        front = slice(0, 2)

        def both(zs, rows, to, ys=None, zs_back=None, rows_back=None, ys_back=None):
            lane, lane_back = [ALL if v is None else at(B * v) for v in (ys, ys_back)]
            forth = ref.at[zs, rows, lane]
            back = forth if rows_back is None else ref.at[zs_back, rows_back, lane_back]
            return self.copy(forth, to[0]), self.copy(back, to[1])

        def done(*copies):
            for copy in copies:
                copy.wait_recv()

        on_y, on_z = (yp, ym), (zp, zm)
        a, b = both(z, a_all, on_y, y), both(z, b_all, on_z, y)
        yield
        done(*a)
        a = both(z, a_0, on_y, y_m, z, a_1, y_p)
        done(*b)
        b = both(z_m, b_0, on_z, y, z_p, b_1, y)
        yield
        done(*a)
        a = both(z, a_all, on_z)
        done(*b)
        b = both(ALL, c_all, on_y, y) if count > first + thin else ()
        if thin:
            b += both(front, t_all, on_y, y)
        yield
        done(*a)
        a = both(z_m, a_0, on_z, None, z_p, a_1)
        done(*b)
        b = both(ALL, c_0, on_y, y_m, ALL, c_1, y_p) if count > first + thin else ()
        if thin:
            b += both(front, t_0, on_y, y_m, front, t_1, y_p)
        yield
        done(*a, *b)
        yield

    def gather_y(self, ref, start, count):
        half, y = count // 2, self.y
        yp, ym = self.zy[:2]

        def view(ys, part=None):
            return ref.at[pl.ds(start, count) if part is None else pl.ds(start + part * half, half), at(B * ys)]

        near = self.copy(view(y), yp), self.copy(view(y), ym)
        yield
        near[0].wait_recv()
        far_0 = self.copy(view(mod4(y - 1), 0), yp)
        near[1].wait_recv()
        far_1 = self.copy(view(mod4(y + 1), 1), ym)
        yield
        far_0.wait_recv()
        far_1.wait_recv()
        yield

    def spread_z(self, *parts):
        sent = []
        for d, peer in ((1, self.zy[2]), (-1, self.zy[3]), (2, self.far_z)):
            for src, dst in parts:
                sent.append((self.copy(src(mod4(self.z + d)), peer, dst(self.z)), dst(mod4(self.z - d))))
        yield
        over = []
        for copy, got in sent:
            copy.wait_recv()
            over.append(self.copy(got, self.partner))
        yield
        for copy in over:
            copy.wait_recv()
        yield

    def swap(self, src, dst, across):
        def piece(k):
            return (k // R, lax.rem(k, R)) if across else (ALL, k)

        others, me = (self.plane(), self.c) if across else (self.line(), self.r)
        sent = [self.copy(src.at[piece(place)], peer, dst.at[piece(me)]) for peer, place in others]
        dst[piece(me)] = src[piece(me)]
        yield
        for copy in sent:
            copy.wait_recv()
        yield

    def reduce(self, acc, fwd, end, start, count, put, terms=None, width=None):
        half, lanes = count // 2, ALL if width is None else pl.ds(0, width)
        rows, lo, hi, mid = pl.ds(start, count), pl.ds(start, half), pl.ds(start + half, half), pl.ds(start // 2, half)
        me, right, left = (self.z, *self.zy[2:]) if terms is None else (self.x, self.right, self.left)
        far, nxt, prv = [mod4(me + d) for d in (2, 1, -1)]
        if terms is not None:
            over = self.copy(terms.at[:, 1 - self.core, rows, lanes], self.partner, acc.at[:, rows, lanes])
            yield
            over.wait_recv()

        def settle(k):
            if terms is not None:
                acc[k, rows, lanes] = acc[k, rows, lanes] + terms[k, self.core, rows, lanes]

        def send(k, part, to, ref, slot):
            return self.copy(acc.at[k, part, lanes], to, ref.at[slot, mid, lanes])

        settle(far)
        far_r, far_l = send(far, lo, right, fwd, 0), send(far, hi, left, fwd, 1)
        settle(nxt)
        settle(prv)
        last = [send(nxt, hi, right, end, 0), send(prv, lo, left, end, 1)]
        settle(me)
        yield
        far_r.wait_recv()
        acc[nxt, lo, lanes] = acc[nxt, lo, lanes] + fwd[0, mid, lanes]
        last.append(send(nxt, lo, right, end, 2))
        far_l.wait_recv()
        acc[prv, hi, lanes] = acc[prv, hi, lanes] + fwd[1, mid, lanes]
        last.append(send(prv, hi, left, end, 3))
        yield
        for copy in last:
            copy.wait_recv()
        blocks = count // B
        for k in range(blocks):
            one, two = (1, 2) if 2 * k < blocks else (0, 3)
            row = pl.ds(start // 2 + B * (k % (blocks // 2)), B)
            put(k, acc[me, pl.ds(start + B * k, B), lanes] + (end[one, row, lanes] + end[two, row, lanes]))
        yield


def invert(w_ref, l_ref, tmp_ref):
    row = lax.broadcasted_iota(jnp.int32, (Q, Q), 0)
    col = lax.broadcasted_iota(jnp.int32, (Q, Q), 1)
    w_ref[...] = jnp.zeros_like(w_ref)

    def block(ref, i, j, size):
        return ref[i // B:(i + size) // B, :, j:j + size].reshape(size, size)

    def put(i, j, size, val):
        w_ref[i // B:(i + size) // B, :, j:j + size] = val.reshape(size // B, B, size)

    corners = range(0, K, Q)
    for k in corners:
        a = block(l_ref, k, k, Q)
        diag = jnp.where(row == col, a, 0.0)
        down, across = 1.0 / jnp.sum(diag, axis=1, keepdims=True), 1.0 / jnp.sum(diag, axis=0, keepdims=True)
        low = (row // 2 == col // 2) & (row > col)
        put(k, k, Q, jnp.where(row == col, down, jnp.where(low, -a * down * across, 0.0)))
    size = 2
    while size < Q:
        pair = (row // (2 * size) == col // (2 * size)) & (row // size > col // size)
        for k in corners:
            tmp_ref[k // Q] = mm(jnp.where(pair, block(l_ref, k, k, Q), 0.0), block(w_ref, k, k, Q))
        yield
        for k in corners:
            w = block(w_ref, k, k, Q)
            put(k, k, Q, w - mm(w, tmp_ref[k // Q]))
        yield
        size *= 2
    while size < K:
        for j in range(0, K, 2 * size):
            i = j + size
            part = mm(block(l_ref, i, j, size), block(w_ref, j, j, size))
            put(i, j, size, -mm(block(w_ref, i, i, size), part))
            yield
        size *= 2


def pieces(ref, u, v):
    top, n = B * (u * (u + 1) // 2 + v - 1), ref.shape[2]
    i, low = top // n, top % n
    cut = min(B, n - low)
    first = [(slice(0, cut), (i, slice(low, low + cut)))]
    return first if cut == B else first + [(slice(cut, B), (i + 1, slice(0, B - cut)))]


def inner(net, u, start, panel, top, bar, terms):
    def two(k, _):
        h, x = k // U, lax.rem(k, U)
        a, b = panel[2 * h + x // 2, top:top + K - Q * u, at(Q * lax.rem(x, 2), Q)], bar[Q * u:, :B * (u + 1)]
        p = mm_t(a, b) if u else mm_t(b, a)
        for e in range(2):
            for v in range(u + 1):
                val = p[B * e:B * (e + 1), B * v:B * (v + 1)] if u else p[:, B * e:B * (e + 1)].T
                terms[x, e, at(start + Q * v + B * h), :] = phi(val, 2 * k + e - net.c) if v == u else val
        return 0

    lax.fori_loop(0, R, two, 0)


def front_kernel(l_ref, bar_ref, lr_ref, col_ref, a_ref, b_ref, lv, lss, wss, tmp, terms, acc, fwd, end, dma_sems, send_sems, recv_sems):
    net = Net(send_sems, recv_sems)
    r, c, y, z, core = net.r, net.c, net.y, net.z, net.core
    half, zz = z // 2, lax.rem(z, 2)
    ways = (1, 2, 3)
    others = [net.device(y=mod4(y + d)) for d in ways]
    for u in GROUPS:
        lv[2:, OFF[u]:OFF[u] + B] = jnp.zeros((2, B, H), jnp.float32)
    ready = net.barrier(*[peer for peer, _ in net.line()], *others, *net.zy[2:])
    for u in GROUPS:
        lv[z, group(u), at(B * y)] = l_ref[Q * u:, B * u:B * (u + 1)]
    ready()

    strip = at(B * (U * zz + y))

    def own(u):
        return at(B * (2 * u + half)), at(B * u)

    sent = [net.copy(l_ref.at[own(mod4(y + d))], other, lss.at[r, :, strip]) for d, other in zip(ways, others)]
    lss[r, :, strip] = l_ref[own(y)]
    g = [net.gather_zy(lv, OFF[u], K - Q * u, (K - Q * u - 96) // 2, B) for u in GROUPS]
    run(chain(g[3], g[2]))
    for copy in sent:
        copy.wait_recv()
    pair = net.copy(lss.at[r, :, at(H * zz, H)], net.device(z=2 * half + 1 - zz))
    run(chain(g[1], g[0], g[3], g[3]))
    pair.wait_recv()

    order = iter([2, 2, 3, 1, 3, 2, 1, 2, 0, 1, 0, 1])
    stores = []

    def tick():
        u = next(order, None)
        if u is not None:
            step(g[u])

    def keep(u):
        stores.append(pltpu.make_async_copy(lv.at[:, group(u)], lr_ref.at[:, group(u)], dma_sems.at[u]))
        stores[-1].start()

    def begin(u):
        start = ROWS - Q * (u + 1) * (u + 2) // 2
        inner(net, u, start, lv, OFF[u], bar_ref, terms)

        def put(k, val):
            v, h = k // 2, k % 2
            for rows, place in pieces(a_ref, u, v):
                a_ref[(h, *place)] = val[rows]

        keep(u)
        return net.reduce(acc, fwd, end, start, Q * (u + 1), put, terms)

    strips = net.gather_x(lss, axis=0)
    step(strips)
    for _ in range(3):
        tick()
    step(strips)
    for _ in range(2):
        tick()
    step(strips)
    s3 = begin(3)
    run(strips)
    step(s3)
    for k, _ in enumerate(invert(wss, lss, tmp)):
        if k % 4 == 1:
            tick()
        if k % 6 == 5:
            step(s3)
    s2 = begin(2)
    step(s2)
    tick()

    sent = [net.copy(wss.at[r, :, at(B * (U * zz + mod4(y + d)))], other, col_ref.at[y, r]) for d, other in zip(ways, others)]
    col_ref[y, r] = wss[r, :, strip]
    step(s2)
    tick()
    tick()
    s1 = begin(1)
    run(chain(s3, s1, s2, s1))
    for copy in sent:
        copy.wait_recv()
    columns = net.gather_x(col_ref)
    flip = net.swap(a_ref, b_ref, False)
    run(chain(columns, s2, s1, g[0], columns, s1, flip, columns, columns, g[0], flip))
    keep(0)
    for copy in stores:
        copy.wait()
    net.drain()


def levels_kernel(lr_ref, bar_ref, wc_ref, a_ref, b_ref, sy_ref, w_ref, row_e, row_d, row_o, col_3,
                  own, a, b, d, back, s_top, top_back, la, lb, l0, l1, bv, cd, re, rd, co, ro, c3, x1, x2, x3, terms, acc, fwd, end, dma_sems, send_sems, recv_sems, t_send, t_recv):
    net = Net(send_sems, recv_sems)
    r, c, y, z = net.r, net.c, net.y, net.z
    sems = iter(range(32))

    def local(a, b):
        copy = pltpu.make_async_copy(a, b, dma_sems.at[next(sems)])
        copy.start()
        return copy

    load_a = [local(lr_ref.at[0:2, OFF[u] + B:OFF[u] + Q], la.at[:, B * u:B * (u + 1)]) for u in GROUPS]
    load_0 = [local(lr_ref.at[:, group(0)], l0), local(bar_ref.at[:, 0:B], bv)]
    load_s = [local(a_ref, a), local(b_ref, b)]
    load_b = [local(lr_ref.at[:, OFF[u] + Q:OFF[u] + H], lb.at[:, B * u:B * (u + 2)]) for u in (0, 2)]
    load_c = local(lr_ref.at[:, OFF[1] + Q:OFF[2]], l1)
    ready = net.barrier(*[peer for peer, _ in net.line() + net.plane()])
    half_c, row_c = c // R, lax.rem(c, R)
    swap = [{'row': row_c, 'col': r + R * h} for h in range(2)]
    away = [(row_c != r) | (half_c != h) for h in range(2)]

    def block(ref, h, u, v):
        return jnp.concatenate([ref[(h, *place)] for _, place in pieces(ref, u, v)], axis=0)

    def trade(h, slot):
        return pltpu.make_async_remote_copy(src_ref=s_top.at[h], dst_ref=top_back.at[slot], send_sem=t_send.at[h],
                                            recv_sem=t_recv.at[slot], device_id=swap[h], device_id_type=MESH)

    low = c < R
    stores = []
    for u in GROUPS:
        re[z, B * u:B * (u + 1), at(B * y)] = wc_ref[u, r]
    for u in GROUPS:
        cd[u, 0:R] = jnp.where(low, wc_ref[u], 0.0)
    ready()
    diag = net.gather_zy(re, 0, H, Q)
    step(diag)
    early = [net.gather_y(sy_ref, K * v + Q * (v + 1), K - Q * (v + 1)) for v in range(U - 1)]
    late = net.gather_y(sy_ref, 3 * K, K)
    e0, e1, e2 = early
    half = pl.ds(2 * net.core, 2)

    def odd(rows):
        return jnp.concatenate([rd[0, rows], rd[1, rows], re[2, rows], re[3, rows]], axis=1)

    for u in GROUPS:
        load_a[u].wait()
        x1[u, r] = mm(wide(la, slice(B * u, B * (u + 1)), (0, 1)), cd[u, 0:R].reshape(K, B))
    strips = net.gather_x(x1)
    flip = net.swap(b, d, True)
    for load in load_s:
        load.wait()
    run(chain(strips, diag, diag, flip))
    for u in range(1, U):
        for h in range(2):
            for v in range(u + 1):
                own[v, B * (2 * u + h):B * (2 * u + h + 1), :] = block(a, h, u, v)
    places = [local(own.at[v, Q * (v + 1):], sy_ref.at[K * v + Q * (v + 1):K * (v + 1), at(B * y)]) for v in range(U - 1)]
    step(strips)
    for load in load_0:
        load.wait()
    inner(net, 0, 0, l0, 0, bv, terms)
    for place in places:
        place.wait()

    def put(k, val):
        s_top[k] = val

    run(strips, net.reduce(acc, fwd, end, 0, Q, put, terms), behind=[chain(diag, e0, diag)])
    run(diag)
    for h in range(2):
        @pl.when(away[h])
        def _():
            trade(h, half_c).start()

        @pl.when(jnp.logical_not(away[h]))
        def _():
            top_back[h] = s_top[h]
    stores.append(local(re, row_e))
    for u in GROUPS:
        w = -mm(wide(re, slice(B * u, B * (u + 1)), (2, 3)), x1[u].reshape(K, B))
        w = jnp.where(low, w, wc_ref[u, r])
        cd[u, R + r] = w
        rd[z, B * u:B * (u + 1), at(B * y)] = w
    rows = net.gather_zy(rd, 0, H, B, H - B)
    step(rows)
    run(net.gather_x(cd, first=R), behind=[chain(rows, rows, e1, e0)])
    stores.append(local(cd.at[:, pl.ds(U * z, U)], w_ref.at[0:U, z]))
    out = net.spread_z((lambda k: cd.at[:, pl.ds(U * k + 2 * net.core, 2)], lambda k: w_ref.at[0:U, k, half]))
    step(out)
    step(flip)
    flip = net.swap(d, back, False)
    step(flip)

    for q in range(2):
        load_b[q].wait()
        x2[2 * q:2 * q + 2, r] = mm(wide(lb, slice(Q * q, Q * (q + 1))), cd[2 * q].reshape(N, B)).reshape(2, B, B)
    run(net.gather_x(x2), behind=[chain(e1, rows, e2, e1, e0)])
    run(rows)
    stores.append(local(rd, row_d))
    for q in range(2):
        at_u = slice(B * (2 * q + 1), B * (2 * q + 2))
        tops = (mm(wide(re, at_u, (0, 1)), x2[2 * q].reshape(K, B)), mm(odd(at_u), x2[2 * q:2 * q + 2].reshape(N, B)))
        for i, w in enumerate(tops):
            co[2 * q + i, r] = -w
            ro[z, B * (2 * q + i):B * (2 * q + i + 1), at(B * y)] = -w
    rows = net.gather_zy(ro, 0, H, Q)
    step(rows)
    strips = net.gather_x(co)
    step(strips)

    run(strips, behind=[chain(rows, e2, rows, out)])
    parts = []
    for q in range(2):
        stores.append(local(co.at[2 * q + z // 2, pl.ds(U * lax.rem(z, 2), U)], w_ref.at[U + q, z]))
        parts.append((lambda k, q=q: co.at[2 * q + k // 2, pl.ds(U * lax.rem(k, 2) + 2 * net.core, 2)],
                      lambda k, q=q: w_ref.at[U + q, k, half]))
    out_o = net.spread_z(*parts)

    load_c.wait()
    x3[:, r] = mm(wide(l1, ALL), jnp.concatenate([co[0:2].reshape(N, B), cd[1].reshape(N, B)], 1)).reshape(U, B, Q)
    x3[:, r, :, :B] = x3[:, r, :, :B] + mm(wide(l0, slice(H, K)), cd[0].reshape(N, B)).reshape(U, B, B)
    strips = net.gather_x(x3)
    step(strips)

    step(flip)
    for h in range(2):
        own[0, B * h:B * (h + 1), :] = s_top[h]
    for s in range(2):
        @pl.when(away[s])
        def _():
            trade(s, s).wait_recv()
        for u in GROUPS:
            for v in range(u + 1):
                at_t = slice(B * (2 * v + s), B * (2 * v + s + 1))
                val = (block(back, s, u, v) if u else top_back[s]).T
                own[u, at_t, :] = own[u, at_t, :] + val if u == v else val
    places = [local(own.at[v, 0:Q * (v + 1)], sy_ref.at[K * v:K * v + Q * (v + 1), at(B * y)]) for v in GROUPS]
    run(strips, behind=[chain(rows, out, e2)])
    run(rows)
    for place in places:
        place.wait()
    step(late)
    step(out_o)
    stores.append(local(ro, row_o))
    for i in GROUPS:
        u = 2 + i // 2
        at_u = slice(B * u, B * (u + 1))
        if i % 2 == 0:
            w = mm(wide(re, at_u, (0, 1)), x3[i].reshape(K, Q))
        else:
            w = mm(odd(at_u), x3[i - 1:i + 1].reshape(N, Q))
        if i >= 2:
            w = w + mm(wide(ro, slice(B * i, B * (i + 1))), x3[0:2].reshape(N, Q))
        c3[i, r] = -w
    run(net.gather_x(c3), behind=[chain(late, out_o)])
    run(late, out_o)
    stores.append(local(c3, col_3))
    for h in range(2):
        @pl.when(away[h])
        def _():
            trade(h, half_c).wait_send()
    for copy in stores:
        copy.wait()
    net.drain()


def product_kernel(sy_ref, w_ref, c3_ref, m_ref, own_ref, sy, w, c3, wide_w, acc, fwd, end, dma_sems, send_sems, recv_sems):
    net = Net(send_sems, recv_sems)
    z = net.z
    start = [slice(K * v, K * v + Q * (v + 1)) for v in range(U - 1)]
    rest = [slice(K * v + Q * (v + 1), K * (v + 1)) for v in range(U - 1)] + [slice(3 * K, U * K)]
    loads = [(c3_ref, c3), *[(sy_ref.at[some], sy.at[some]) for some in (*start, *rest)], (w_ref, w)]
    loads = [pltpu.make_async_copy(a, b, dma_sems.at[k]) for k, (a, b) in enumerate(loads)]
    for load in loads:
        load.start()
    for load in loads[:U]:
        load.wait()
    ready = net.barrier(*net.zy, net.far_z, net.partner)
    half = pl.ds(2 * net.core, 2)
    parts = []
    for v in range(2):
        wide_w[v, z] = c3[2 * v + z // 2, pl.ds(U * lax.rem(z, 2), U)]
        parts.append((lambda k, v=v: c3.at[2 * v + k // 2, pl.ds(U * lax.rem(k, 2) + 2 * net.core, 2)],
                      lambda k, v=v: wide_w.at[v, k, half]))
    ready()
    out = net.spread_z(*parts)
    step(out)
    own_ref[...] = c3[:, net.r]
    m0, m1, m2 = moves = [net.gather_y(sy, K * v, Q * (v + 1)) for v in range(U - 1)]
    run(chain(m2, m1))
    m_ref[...] = jnp.zeros_like(m_ref)

    def block(v, col):
        if v >= 2 and col < 2:
            some = [wide_w[v - 2, k, :, :, B * col:B * (col + 1)] for k in GROUPS]
        else:
            some = [w[v if v == col else U + v // 2, k] for k in GROUPS]
        return jnp.concatenate([x.reshape(H, B) for x in some], axis=1)

    def terms(u, col, groups, more=False):
        part = sum(mm(sy[K * v + Q * u:K * v + Q * (u + 1), :], block(v, col)) for v in groups)
        for k in GROUPS:
            place = k, slice(Q * u, Q * (u + 1)), slice(B * col, B * (col + 1))
            val = part[:, B * k:B * (k + 1)]
            acc[place] = acc[place] + val if more else val

    def sum_of(u):
        def put(k, val):
            m_ref[Q * u + B * k:Q * u + B * (k + 1), :B * (u + 1)] = val

        return net.reduce(acc, fwd, end, Q * u, Q, put, width=B * (u + 1))

    for load in loads[U:]:
        load.wait()
    sums = []
    for u in GROUPS[::-1]:
        for col in range(u + 1):
            terms(u, col, range(col, U if col >= 2 else 2))
        if u == 3:
            run(chain(m2, m0, m1, m2, out))
            run(out)
        for col in range(min(u + 1, 2)):
            terms(u, col, range(2, U), True)
        for s in sums:
            step(s)
        sums.append(sum_of(u))
        step(sums[-1])
        run(chain(m1, m0))
    run(*moves, *sums)
    net.drain()


def gradient_kernel(x_ref, own_ref, re_ref, rd_ref, ro_ref, t_ref,
                    wr, terms, acc, fwd, end, dma_sems, send_sems, recv_sems):
    net = Net(send_sems, recv_sems)
    loads = [[(re_ref.at[0:2, B * u:B * (u + 1)], wr.at[0:2, OFF[u]:OFF[u] + B]),
              *[(ref.at[zs, B * u:B * (u + 1)], wr.at[zs, OFF[u] + B:OFF[u] + Q])
                for ref, zs in ((rd_ref, slice(0, 2)), (re_ref, slice(2, U)))]] for u in GROUPS]
    loads[2] += [(ro_ref.at[:, Q:], wr.at[:, OFF[2] + Q:OFF[3]])]
    loads[0] += [(ro_ref.at[:, :Q], wr.at[:, Q:H])]
    sems = iter(range(16))
    loads = [[pltpu.make_async_copy(a, b, dma_sems.at[next(sems)]) for a, b in some] for some in loads]
    for some in loads[::-1]:
        for load in some:
            load.start()
    ready = net.barrier(net.right, net.left, net.partner, *net.zy)
    for i in GROUPS:
        for k, top in enumerate((H, OFF[1] + Q)):
            wr[net.z, top + B * i:top + B * (i + 1), at(B * net.y)] = own_ref[i, :, B * k:B * (k + 1)]
    ready()
    rows_0, rows_1 = net.gather_zy(wr, H, H, Q), net.gather_zy(wr, OFF[1] + Q, H, Q)
    step(rows_1)
    step(rows_0)

    def half_of(u, h, top=0, rows=K):
        width = B * (u + 1)
        some = slice(OFF[u] + top, min(OFF[u] + top + rows, OFF[u] + K - Q * u))
        these = slice(Q * u + top, Q * u + top + some.stop - some.start)

        def two(x, _):
            a, b = wr[2 * h + x // 2, some, at(Q * lax.rem(x, 2), Q)], x_ref[these, :width]
            part = mm_t(a, b) if u else mm_t(b, a)
            for e in range(2):
                place = x, e, slice(Q * u + B * h, Q * u + B * (h + 1)), slice(0, width)
                val = part[B * e:B * (e + 1)] if u else part[:, B * e:B * (e + 1)].T
                terms[place] = terms[place] + val if top else val
            return 0

        lax.fori_loop(0, U, two, 0)

    def sum_of(u):
        wr[2:, OFF[u]:OFF[u] + B] = jnp.zeros((2, B, H), jnp.float32)
        for load in loads[u]:
            load.wait()
        for top in ((0,) if u else (0, H)):
            for h in range(2):
                half_of(u, h, top, K if u else H)
                yield

        def put(k, val):
            t_ref[B * (2 * u + k):B * (2 * u + k + 1), :B * (u + 1)] = val

        yield from net.reduce(acc, fwd, end, Q * u, Q, put, terms, B * (u + 1))

    s0, s1, s2, s3 = [sum_of(u) for u in GROUPS]
    run(chain(s3, s3, s3, rows_1, s2, s3, rows_1, s2, rows_1, s3, s2, rows_1, s2, s3, rows_0, s1, s2, s1, s1, rows_0, s0, s1, s2,
              s0, s1, rows_0, s1, rows_0, s0, s0, s0, s0, s0, s0))
    run(s2, s1, s0)
    net.drain()


def call(kernel, ident, flops, args, in_specs, outs, out_specs, scratch, sems):
    return pl.pallas_call(
        kernel,
        out_shape=[jax.ShapeDtypeStruct(s, jnp.float32) for s in outs],
        in_specs=in_specs,
        out_specs=out_specs,
        scratch_shapes=[*(pltpu.VMEM(s, jnp.float32) for s in scratch), *(pltpu.SemaphoreType.DMA(s) for s in sems)],
        compiler_params=pltpu.CompilerParams(collective_id=ident, has_side_effects=True, vmem_limit_bytes=67 * 10 ** 6),
        cost_estimate=pl.CostEstimate(flops=flops, bytes_accessed=K, transcendentals=0),
    )(*args)


def solution(mesh):
    def local_pass(fac, bar):
        panel, rows, column = (U, ROWS, H), (U, H, H), (U, R, B, B)
        wide_col, cut = (U, R, B, Q), (2, R, (ROWS - Q) // (2 * R), B)
        lr, wc, a, b = call(
            front_kernel, 0, 1, (fac, bar), [VM] * 2, (panel, column, cut, cut), [HB] + [VM] * 3,
            (panel, (R, B, K), (R, B, K), (U, Q, Q), (U, 2, ROWS, B), (U, ROWS, B), (2, ROWS // 2, B), (U, ROWS // 2, B)),
            ((U,), (144,), (144,)))
        sy, w, row_e, row_d, row_o, col_3 = call(
            levels_kernel, 1, 1, (lr, bar, wc, a, b), [HB, HB, VM, HB, HB],
            ((U * K, H), (6, U, U, B, B), rows, rows, rows, wide_col), [HB] * 6,
            ((U, K, B), cut, cut, cut, cut, (2, B, B), (2, B, B), (2, H, H), rows, (U, K, H), rows, (K, B), (U, 2 * R, B, B), rows, rows, column, rows,
             wide_col, column, column, wide_col, (U, 2, Q, B), (U, Q, B), (2, B, B), (U, B, B)),
            ((48,), (208,), (208,), (2,), (2,)))
        m, own = call(
            product_kernel, 2, 1, (sy, w, col_3), [HB] * 3, ((K, H), (U, B, Q)), [VM] * 2,
            ((U * K, H), (6, U, U, B, B), wide_col, (2, U, U, B, Q), (U, K, H), (2, H, H), (U, H, H)), ((16,), (48,), (48,)))
        out, = call(
            gradient_kernel, 3, 1, (m, own, row_e, row_d, row_o), [VM] * 2 + [HB] * 3, ((K, H),), [VM],
            (panel, (U, 2, K, H), (U, K, H), (2, H, H), (U, H, H)), ((16,), (64,), (64,)))
        row, col = lax.broadcasted_iota(jnp.int32, (K, 1), 0), lax.broadcasted_iota(jnp.int32, (1, H), 1)
        row_all = (row // B * R + lax.axis_index('row')) * B + row % B
        col_all = (col // B * 2 * R + lax.axis_index('col')) * B + col % B
        return jnp.where(row_all > col_all, out, jnp.where(row_all == col_all, 0.5 * out, 0.0))

    spec = P(('batch', 'row'), 'col')
    return jax.shard_map(local_pass, mesh=mesh, in_specs=(spec, spec), out_specs=spec, check_vma=False)
```

```python
import jax
import jax.numpy as jnp
from jax import lax
from jax.experimental import pallas as pl
from jax.experimental.pallas import tpu as pltpu
from jax.sharding import PartitionSpec as P

B, Q, H, K, N = 128, 256, 512, 1024, 2048
U, R = 4, 8
GROUPS = tuple(range(U))
OFF = tuple(K * u - B * u * (u - 1) for u in GROUPS)
ROWS = OFF[-1] + Q
HI = lax.Precision.HIGHEST
MESH = pl.DeviceIdType.MESH
VM = pl.BlockSpec(memory_space=pltpu.VMEM)
HB = pl.BlockSpec(memory_space=pl.ANY)
ALL = slice(None)


def mm(a, b):
    return jnp.dot(a, b, precision=HI, preferred_element_type=jnp.float32)


def mm_t(a, b):
    return lax.dot_general(a, b, (((0,), (0,)), ((), ())), precision=HI, preferred_element_type=jnp.float32)


def mod4(v):
    return lax.rem(v + U, U)


def at(start, size=B):
    return pl.ds(start if isinstance(start, int) else pl.multiple_of(start, B), size)


def group(u):
    return slice(OFF[u], OFF[u] + K - Q * u)


def wide(ref, rows, zs=GROUPS):
    return jnp.concatenate([ref[z, rows] for z in zs], axis=1)


def phi(block, ahead):
    diff = B * ahead + lax.broadcasted_iota(jnp.int32, (B, B), 0) - lax.broadcasted_iota(jnp.int32, (B, B), 1)
    return jnp.where(diff > 0, block, jnp.where(diff == 0, 0.5 * block, 0.0))


def step(g):
    return next(g, g) is not g


def run(*gathers, behind=()):
    live = list(gathers)
    while live:
        live = [g for g in live if step(g)]
        for g in behind:
            step(g)


def chain(*gathers):
    for g in gathers:
        step(g)
        yield


class Net:
    def __init__(self, send_sems, recv_sems):
        self.send_sems, self.recv_sems = send_sems, recv_sems
        self.r, self.c = lax.axis_index('row'), lax.axis_index('col')
        self.x, self.core = self.r // 2, lax.rem(self.r, 2)
        self.z, self.y = self.c // U, lax.rem(self.c, U)
        self.right, self.left = self.device(x=mod4(self.x + 1)), self.device(x=mod4(self.x - 1))
        self.partner = self.device(core=1 - self.core)
        self.zy = [self.device(y=mod4(self.y + 1)), self.device(y=mod4(self.y - 1)),
                   self.device(z=mod4(self.z + 1)), self.device(z=mod4(self.z - 1))]
        self.far_z = self.device(z=mod4(self.z + 2))
        self.copies = []

    def device(self, **place):
        x, core, y, z = [place.get(k, getattr(self, k)) for k in ('x', 'core', 'y', 'z')]
        return {'col': U * z + y, 'row': 2 * x + core}

    def barrier(self, *peers):
        sem = pltpu.get_barrier_semaphore()
        for peer in peers:
            pl.semaphore_signal(sem, inc=1, device_id=peer, device_id_type=MESH)
        return lambda: pl.semaphore_wait(sem, len(peers))

    def line(self):
        places = [(mod4(self.x + d // 2), lax.rem(self.core + d, 2)) for d in range(1, R)]
        return [(self.device(x=x, core=core), 2 * x + core) for x, core in places]

    def plane(self):
        places = [(mod4(self.z + d // U), mod4(self.y + d % U)) for d in range(1, U * U)]
        return [(self.device(z=z, y=y), U * z + y) for z, y in places]

    def copy(self, ref, peer, dst=None):
        k = len(self.copies)
        copy = pltpu.make_async_remote_copy(
            src_ref=ref, dst_ref=ref if dst is None else dst, send_sem=self.send_sems.at[k], recv_sem=self.recv_sems.at[k],
            device_id=peer, device_id_type=MESH)
        copy.start()
        self.copies.append(copy)
        return copy

    def drain(self):
        for copy in self.copies:
            copy.wait_send()

    def gather_x(self, ref, axis=1, first=0):
        half = ref.shape[1 - axis] // 2

        def view(r, part=None):
            other = ALL if part is None else pl.ds(part * half, half)
            return ref.at[(other, first + r) if axis else (r, other)]

        near_r, near_l, far = [2 * mod4(self.x + d) + self.core for d in (1, -1, 2)]
        to_right, to_left = [], []
        for part in range(2):
            to_right.append(self.copy(view(self.r, part), self.right))
            to_left.append(self.copy(view(self.r, 1 - part), self.left))
        over = [self.copy(view(self.r), self.partner)]
        yield
        to_right[0].wait_recv()
        far_0 = self.copy(view(near_l, 0), self.right)
        to_left[0].wait_recv()
        far_1 = self.copy(view(near_r, 1), self.left)
        yield
        to_right[1].wait_recv()
        over.append(self.copy(view(near_l), self.partner))
        to_left[1].wait_recv()
        over.append(self.copy(view(near_r), self.partner))
        far_0.wait_recv()
        over.append(self.copy(view(far, 0), self.partner))
        far_1.wait_recv()
        over.append(self.copy(view(far, 1), self.partner))
        yield
        for copy in over:
            copy.wait_recv()
        yield

    def gather_zy(self, ref, start, count, first, thin=0):
        yp, ym, zp, zm = self.zy
        y, z = self.y, self.z
        y_m, y_p, z_m, z_p = mod4(y - 1), mod4(y + 1), mod4(z - 1), mod4(z + 1)

        def cut(top, size):
            return pl.ds(top, size // 2), pl.ds(top + size // 2, size // 2), pl.ds(top, size)

        a_0, a_1, a_all = cut(start + count - first, first)
        b_0, b_1, b_all = cut(start, count - first)
        c_0, c_1, c_all = cut(start + thin, count - first - thin)
        t_0, t_1, t_all = cut(start, thin)
        front = slice(0, 2)

        def both(zs, rows, to, ys=None, zs_back=None, rows_back=None, ys_back=None):
            lane, lane_back = [ALL if v is None else at(B * v) for v in (ys, ys_back)]
            forth = ref.at[zs, rows, lane]
            back = forth if rows_back is None else ref.at[zs_back, rows_back, lane_back]
            return self.copy(forth, to[0]), self.copy(back, to[1])

        def done(*copies):
            for copy in copies:
                copy.wait_recv()

        on_y, on_z = (yp, ym), (zp, zm)
        a, b = both(z, a_all, on_y, y), both(z, b_all, on_z, y)
        yield
        done(*a)
        a = both(z, a_0, on_y, y_m, z, a_1, y_p)
        done(*b)
        b = both(z_m, b_0, on_z, y, z_p, b_1, y)
        yield
        done(*a)
        a = both(z, a_all, on_z)
        done(*b)
        b = both(ALL, c_all, on_y, y) if count > first + thin else ()
        if thin:
            b += both(front, t_all, on_y, y)
        yield
        done(*a)
        a = both(z_m, a_0, on_z, None, z_p, a_1)
        done(*b)
        b = both(ALL, c_0, on_y, y_m, ALL, c_1, y_p) if count > first + thin else ()
        if thin:
            b += both(front, t_0, on_y, y_m, front, t_1, y_p)
        yield
        done(*a, *b)
        yield

    def gather_y(self, ref, start, count):
        half, y = count // 2, self.y
        yp, ym = self.zy[:2]

        def view(ys, part=None):
            return ref.at[pl.ds(start, count) if part is None else pl.ds(start + part * half, half), at(B * ys)]

        near = self.copy(view(y), yp), self.copy(view(y), ym)
        yield
        near[0].wait_recv()
        far_0 = self.copy(view(mod4(y - 1), 0), yp)
        near[1].wait_recv()
        far_1 = self.copy(view(mod4(y + 1), 1), ym)
        yield
        far_0.wait_recv()
        far_1.wait_recv()
        yield

    def spread_z(self, *parts):
        sent = []
        for d, peer in ((1, self.zy[2]), (-1, self.zy[3]), (2, self.far_z)):
            for src, dst in parts:
                sent.append((self.copy(src(mod4(self.z + d)), peer, dst(self.z)), dst(mod4(self.z - d))))
        yield
        over = []
        for copy, got in sent:
            copy.wait_recv()
            over.append(self.copy(got, self.partner))
        yield
        for copy in over:
            copy.wait_recv()
        yield

    def swap(self, src, dst, across):
        def piece(k):
            return (k // R, lax.rem(k, R)) if across else (ALL, k)

        others, me = (self.plane(), self.c) if across else (self.line(), self.r)
        sent = [self.copy(src.at[piece(place)], peer, dst.at[piece(me)]) for peer, place in others]
        dst[piece(me)] = src[piece(me)]
        yield
        for copy in sent:
            copy.wait_recv()
        yield

    def reduce(self, acc, fwd, end, start, count, put, terms=None, width=None):
        half, lanes = count // 2, ALL if width is None else pl.ds(0, width)
        rows, lo, hi, mid = pl.ds(start, count), pl.ds(start, half), pl.ds(start + half, half), pl.ds(start // 2, half)
        me, right, left = (self.z, *self.zy[2:]) if terms is None else (self.x, self.right, self.left)
        far, nxt, prv = [mod4(me + d) for d in (2, 1, -1)]
        if terms is not None:
            over = self.copy(terms.at[:, 1 - self.core, rows, lanes], self.partner, acc.at[:, rows, lanes])
            yield
            over.wait_recv()

        def settle(k):
            if terms is not None:
                acc[k, rows, lanes] = acc[k, rows, lanes] + terms[k, self.core, rows, lanes]

        def send(k, part, to, ref, slot):
            return self.copy(acc.at[k, part, lanes], to, ref.at[slot, mid, lanes])

        settle(far)
        far_r, far_l = send(far, lo, right, fwd, 0), send(far, hi, left, fwd, 1)
        settle(nxt)
        settle(prv)
        last = [send(nxt, hi, right, end, 0), send(prv, lo, left, end, 1)]
        settle(me)
        yield
        far_r.wait_recv()
        acc[nxt, lo, lanes] = acc[nxt, lo, lanes] + fwd[0, mid, lanes]
        last.append(send(nxt, lo, right, end, 2))
        far_l.wait_recv()
        acc[prv, hi, lanes] = acc[prv, hi, lanes] + fwd[1, mid, lanes]
        last.append(send(prv, hi, left, end, 3))
        yield
        for copy in last:
            copy.wait_recv()
        blocks = count // B
        for k in range(blocks):
            one, two = (1, 2) if 2 * k < blocks else (0, 3)
            row = pl.ds(start // 2 + B * (k % (blocks // 2)), B)
            put(k, acc[me, pl.ds(start + B * k, B), lanes] + (end[one, row, lanes] + end[two, row, lanes]))
        yield


def invert(w_ref, l_ref, tmp_ref):
    row = lax.broadcasted_iota(jnp.int32, (Q, Q), 0)
    col = lax.broadcasted_iota(jnp.int32, (Q, Q), 1)
    w_ref[...] = jnp.zeros_like(w_ref)

    def block(ref, i, j, size):
        return ref[i // B:(i + size) // B, :, j:j + size].reshape(size, size)

    def put(i, j, size, val):
        w_ref[i // B:(i + size) // B, :, j:j + size] = val.reshape(size // B, B, size)

    corners = range(0, K, Q)
    for k in corners:
        a = block(l_ref, k, k, Q)
        diag = jnp.where(row == col, a, 0.0)
        down, across = 1.0 / jnp.sum(diag, axis=1, keepdims=True), 1.0 / jnp.sum(diag, axis=0, keepdims=True)
        low = (row // 2 == col // 2) & (row > col)
        put(k, k, Q, jnp.where(row == col, down, jnp.where(low, -a * down * across, 0.0)))
    size = 2
    while size < Q:
        pair = (row // (2 * size) == col // (2 * size)) & (row // size > col // size)
        for k in corners:
            tmp_ref[k // Q] = mm(jnp.where(pair, block(l_ref, k, k, Q), 0.0), block(w_ref, k, k, Q))
        yield
        for k in corners:
            w = block(w_ref, k, k, Q)
            put(k, k, Q, w - mm(w, tmp_ref[k // Q]))
        yield
        size *= 2
    while size < K:
        for j in range(0, K, 2 * size):
            i = j + size
            part = mm(block(l_ref, i, j, size), block(w_ref, j, j, size))
            put(i, j, size, -mm(block(w_ref, i, i, size), part))
            yield
        size *= 2


def pieces(ref, u, v):
    top, n = B * (u * (u + 1) // 2 + v - 1), ref.shape[2]
    i, low = top // n, top % n
    cut = min(B, n - low)
    first = [(slice(0, cut), (i, slice(low, low + cut)))]
    return first if cut == B else first + [(slice(cut, B), (i + 1, slice(0, B - cut)))]


def inner(net, u, start, panel, top, bar, terms):
    def two(k, _):
        h, x = k // U, lax.rem(k, U)
        a, b = panel[2 * h + x // 2, top:top + K - Q * u, at(Q * lax.rem(x, 2), Q)], bar[Q * u:, :B * (u + 1)]
        p = mm_t(a, b) if u else mm_t(b, a)
        for e in range(2):
            for v in range(u + 1):
                val = p[B * e:B * (e + 1), B * v:B * (v + 1)] if u else p[:, B * e:B * (e + 1)].T
                terms[x, e, at(start + Q * v + B * h), :] = phi(val, 2 * k + e - net.c) if v == u else val
        return 0

    lax.fori_loop(0, R, two, 0)


def front_kernel(l_ref, bar_ref, lr_ref, col_ref, a_ref, b_ref, bar, lv, lss, wss, tmp, terms, acc, fwd, end, dma_sems, send_sems, recv_sems):
    net = Net(send_sems, recv_sems)
    r, c, y, z, core = net.r, net.c, net.y, net.z, net.core
    load = pltpu.make_async_copy(bar_ref, bar, dma_sems.at[U])
    load.start()
    half, zz = z // 2, lax.rem(z, 2)
    ways = (1, 2, 3)
    others = [net.device(y=mod4(y + d)) for d in ways]
    for u in GROUPS:
        lv[2:, OFF[u]:OFF[u] + B] = jnp.zeros((2, B, H), jnp.float32)
    ready = net.barrier(*[peer for peer, _ in net.line()], *others, *net.zy[2:])
    for u in GROUPS:
        lv[z, group(u), at(B * y)] = l_ref[Q * u:, B * u:B * (u + 1)]
    ready()

    strip = at(B * (U * zz + y))

    def own(u):
        return at(B * (2 * u + half)), at(B * u)

    sent = [net.copy(l_ref.at[own(mod4(y + d))], other, lss.at[r, :, strip]) for d, other in zip(ways, others)]
    lss[r, :, strip] = l_ref[own(y)]
    g = [net.gather_zy(lv, OFF[u], K - Q * u, (K - Q * u - 96) // 2, B) for u in GROUPS]
    run(chain(g[3], g[2]))
    for copy in sent:
        copy.wait_recv()
    pair = net.copy(lss.at[r, :, at(H * zz, H)], net.device(z=2 * half + 1 - zz))
    run(chain(g[1], g[0], g[3], g[3]))
    pair.wait_recv()

    order = iter([2, 2, 3, 1, 3, 2, 1, 2, 0, 1, 0, 1])
    stores = []

    def tick():
        u = next(order, None)
        if u is not None:
            step(g[u])

    def keep(u):
        stores.append(pltpu.make_async_copy(lv.at[:, group(u)], lr_ref.at[:, group(u)], dma_sems.at[u]))
        stores[-1].start()

    def begin(u):
        start = ROWS - Q * (u + 1) * (u + 2) // 2
        inner(net, u, start, lv, OFF[u], bar, terms)

        def put(k, val):
            v, h = k // 2, k % 2
            for rows, place in pieces(a_ref, u, v):
                a_ref[(h, *place)] = val[rows]

        keep(u)
        return net.reduce(acc, fwd, end, start, Q * (u + 1), put, terms)

    strips = net.gather_x(lss, axis=0)
    step(strips)
    for _ in range(3):
        tick()
    step(strips)
    for _ in range(2):
        tick()
    step(strips)
    load.wait()
    s3 = begin(3)
    run(strips)
    step(s3)
    for k, _ in enumerate(invert(wss, lss, tmp)):
        if k % 4 == 1:
            tick()
        if k % 6 == 5:
            step(s3)
    s2 = begin(2)
    step(s2)
    tick()

    sent = [net.copy(wss.at[r, :, at(B * (U * zz + mod4(y + d)))], other, col_ref.at[y, r]) for d, other in zip(ways, others)]
    col_ref[y, r] = wss[r, :, strip]
    step(s2)
    tick()
    tick()
    s1 = begin(1)
    run(chain(s3, s1, s2, s1))
    for copy in sent:
        copy.wait_recv()
    columns = net.gather_x(col_ref)
    flip = net.swap(a_ref, b_ref, False)
    run(chain(columns, s2, s1, g[0], columns, s1, flip, columns, columns, g[0], flip))
    keep(0)
    for copy in stores:
        copy.wait()
    net.drain()


def levels_kernel(lr_ref, bar_ref, wc_ref, a_ref, b_ref, sy_ref, w_ref, row_e, row_d, row_o, col_3,
                  own, a, b, d, back, s_top, top_back, la, lb, l0, l1, bv, cd, re, rd, co, ro, c3, x1, x2, x3, terms, acc, fwd, end, dma_sems, send_sems, recv_sems, t_send, t_recv):
    net = Net(send_sems, recv_sems)
    r, c, y, z = net.r, net.c, net.y, net.z
    sems = iter(range(32))

    def local(a, b):
        copy = pltpu.make_async_copy(a, b, dma_sems.at[next(sems)])
        copy.start()
        return copy

    load_a = [local(lr_ref.at[0:2, OFF[u] + B:OFF[u] + Q], la.at[:, B * u:B * (u + 1)]) for u in GROUPS]
    load_0 = [local(lr_ref.at[:, group(0)], l0), local(bar_ref.at[:, 0:B], bv)]
    load_s = [local(a_ref, a), local(b_ref, b)]
    load_b = [local(lr_ref.at[:, OFF[u] + Q:OFF[u] + H], lb.at[:, B * u:B * (u + 2)]) for u in (0, 2)]
    load_c = local(lr_ref.at[:, OFF[1] + Q:OFF[2]], l1)
    ready = net.barrier(*[peer for peer, _ in net.line() + net.plane()])
    half_c, row_c = c // R, lax.rem(c, R)
    swap = [{'row': row_c, 'col': r + R * h} for h in range(2)]
    away = [(row_c != r) | (half_c != h) for h in range(2)]

    def block(ref, h, u, v):
        return jnp.concatenate([ref[(h, *place)] for _, place in pieces(ref, u, v)], axis=0)

    def trade(h, slot):
        return pltpu.make_async_remote_copy(src_ref=s_top.at[h], dst_ref=top_back.at[slot], send_sem=t_send.at[h],
                                            recv_sem=t_recv.at[slot], device_id=swap[h], device_id_type=MESH)

    low = c < R
    stores = []
    for u in GROUPS:
        re[z, B * u:B * (u + 1), at(B * y)] = wc_ref[u, r]
    for u in GROUPS:
        cd[u, 0:R] = jnp.where(low, wc_ref[u], 0.0)
    ready()
    diag = net.gather_zy(re, 0, H, Q)
    step(diag)
    early = [net.gather_y(sy_ref, K * v + Q * (v + 1), K - Q * (v + 1)) for v in range(U - 1)]
    late = net.gather_y(sy_ref, 3 * K, K)
    e0, e1, e2 = early
    half = pl.ds(2 * net.core, 2)

    def odd(rows):
        return jnp.concatenate([rd[0, rows], rd[1, rows], re[2, rows], re[3, rows]], axis=1)

    for u in GROUPS:
        load_a[u].wait()
        x1[u, r] = mm(wide(la, slice(B * u, B * (u + 1)), (0, 1)), cd[u, 0:R].reshape(K, B))
    strips = net.gather_x(x1)
    flip = net.swap(b, d, True)
    for load in load_s:
        load.wait()
    run(chain(strips, diag, diag, flip))
    for u in range(1, U):
        for h in range(2):
            for v in range(u + 1):
                own[v, B * (2 * u + h):B * (2 * u + h + 1), :] = block(a, h, u, v)
    places = [local(own.at[v, Q * (v + 1):], sy_ref.at[K * v + Q * (v + 1):K * (v + 1), at(B * y)]) for v in range(U - 1)]
    step(strips)
    for load in load_0:
        load.wait()
    inner(net, 0, 0, l0, 0, bv, terms)
    for place in places:
        place.wait()

    def put(k, val):
        s_top[k] = val

    run(strips, net.reduce(acc, fwd, end, 0, Q, put, terms), behind=[chain(diag, e0, diag)])
    run(diag)
    for h in range(2):
        @pl.when(away[h])
        def _():
            trade(h, half_c).start()

        @pl.when(jnp.logical_not(away[h]))
        def _():
            top_back[h] = s_top[h]
    stores.append(local(re, row_e))
    for u in GROUPS:
        w = -mm(wide(re, slice(B * u, B * (u + 1)), (2, 3)), x1[u].reshape(K, B))
        w = jnp.where(low, w, wc_ref[u, r])
        cd[u, R + r] = w
        rd[z, B * u:B * (u + 1), at(B * y)] = w
    rows = net.gather_zy(rd, 0, H, B, H - B)
    step(rows)
    run(net.gather_x(cd, first=R), behind=[chain(rows, rows, e1, e0)])
    stores.append(local(cd.at[:, pl.ds(U * z, U)], w_ref.at[0:U, z]))
    out = net.spread_z((lambda k: cd.at[:, pl.ds(U * k + 2 * net.core, 2)], lambda k: w_ref.at[0:U, k, half]))
    step(out)
    step(flip)
    flip = net.swap(d, back, False)
    step(flip)

    for q in range(2):
        load_b[q].wait()
        x2[2 * q:2 * q + 2, r] = mm(wide(lb, slice(Q * q, Q * (q + 1))), cd[2 * q].reshape(N, B)).reshape(2, B, B)
    run(net.gather_x(x2), behind=[chain(e1, rows, e2, e1, e0)])
    run(rows)
    stores.append(local(rd, row_d))
    for q in range(2):
        at_u = slice(B * (2 * q + 1), B * (2 * q + 2))
        tops = (mm(wide(re, at_u, (0, 1)), x2[2 * q].reshape(K, B)), mm(odd(at_u), x2[2 * q:2 * q + 2].reshape(N, B)))
        for i, w in enumerate(tops):
            co[2 * q + i, r] = -w
            ro[z, B * (2 * q + i):B * (2 * q + i + 1), at(B * y)] = -w
    rows = net.gather_zy(ro, 0, H, Q)
    step(rows)
    strips = net.gather_x(co)
    step(strips)

    run(strips, behind=[chain(rows, e2, rows, out)])
    parts = []
    for q in range(2):
        stores.append(local(co.at[2 * q + z // 2, pl.ds(U * lax.rem(z, 2), U)], w_ref.at[U + q, z]))
        parts.append((lambda k, q=q: co.at[2 * q + k // 2, pl.ds(U * lax.rem(k, 2) + 2 * net.core, 2)],
                      lambda k, q=q: w_ref.at[U + q, k, half]))
    out_o = net.spread_z(*parts)

    load_c.wait()
    x3[:, r] = mm(wide(l1, ALL), jnp.concatenate([co[0:2].reshape(N, B), cd[1].reshape(N, B)], 1)).reshape(U, B, Q)
    x3[:, r, :, :B] = x3[:, r, :, :B] + mm(wide(l0, slice(H, K)), cd[0].reshape(N, B)).reshape(U, B, B)
    strips = net.gather_x(x3)
    step(strips)

    step(flip)
    for h in range(2):
        own[0, B * h:B * (h + 1), :] = s_top[h]
    for s in range(2):
        @pl.when(away[s])
        def _():
            trade(s, s).wait_recv()
        for u in GROUPS:
            for v in range(u + 1):
                at_t = slice(B * (2 * v + s), B * (2 * v + s + 1))
                val = (block(back, s, u, v) if u else top_back[s]).T
                own[u, at_t, :] = own[u, at_t, :] + val if u == v else val
    places = [local(own.at[v, 0:Q * (v + 1)], sy_ref.at[K * v:K * v + Q * (v + 1), at(B * y)]) for v in GROUPS]
    run(strips, behind=[chain(rows, out, e2)])
    run(rows)
    for place in places:
        place.wait()
    step(late)
    step(out_o)
    stores.append(local(ro, row_o))
    for i in GROUPS:
        u = 2 + i // 2
        at_u = slice(B * u, B * (u + 1))
        if i % 2 == 0:
            w = mm(wide(re, at_u, (0, 1)), x3[i].reshape(K, Q))
        else:
            w = mm(odd(at_u), x3[i - 1:i + 1].reshape(N, Q))
        if i >= 2:
            w = w + mm(wide(ro, slice(B * i, B * (i + 1))), x3[0:2].reshape(N, Q))
        c3[i, r] = -w
    run(net.gather_x(c3), behind=[chain(late, out_o)])
    run(late, out_o)
    stores.append(local(c3, col_3))
    for h in range(2):
        @pl.when(away[h])
        def _():
            trade(h, half_c).wait_send()
    for copy in stores:
        copy.wait()
    net.drain()


def product_kernel(sy_ref, w_ref, c3_ref, m_ref, own_ref, sy, w, c3, wide_w, acc, fwd, end, dma_sems, send_sems, recv_sems):
    net = Net(send_sems, recv_sems)
    z = net.z
    start = [slice(K * v, K * v + Q * (v + 1)) for v in range(U - 1)]
    rest = [slice(K * v + Q * (v + 1), K * (v + 1)) for v in range(U - 1)] + [slice(3 * K, U * K)]
    loads = [(c3_ref, c3), *[(sy_ref.at[some], sy.at[some]) for some in (*start, *rest)], (w_ref, w)]
    loads = [pltpu.make_async_copy(a, b, dma_sems.at[k]) for k, (a, b) in enumerate(loads)]
    for load in loads:
        load.start()
    for load in loads[:U]:
        load.wait()
    ready = net.barrier(*net.zy, net.far_z, net.partner)
    half = pl.ds(2 * net.core, 2)
    parts = []
    for v in range(2):
        wide_w[v, z] = c3[2 * v + z // 2, pl.ds(U * lax.rem(z, 2), U)]
        parts.append((lambda k, v=v: c3.at[2 * v + k // 2, pl.ds(U * lax.rem(k, 2) + 2 * net.core, 2)],
                      lambda k, v=v: wide_w.at[v, k, half]))
    ready()
    out = net.spread_z(*parts)
    step(out)
    own_ref[...] = c3[:, net.r]
    m0, m1, m2 = moves = [net.gather_y(sy, K * v, Q * (v + 1)) for v in range(U - 1)]
    run(chain(m2, m1))
    m_ref[...] = jnp.zeros_like(m_ref)

    def block(v, col):
        if v >= 2 and col < 2:
            some = [wide_w[v - 2, k, :, :, B * col:B * (col + 1)] for k in GROUPS]
        else:
            some = [w[v if v == col else U + v // 2, k] for k in GROUPS]
        return jnp.concatenate([x.reshape(H, B) for x in some], axis=1)

    def terms(u, col, groups, more=False):
        part = sum(mm(sy[K * v + Q * u:K * v + Q * (u + 1), :], block(v, col)) for v in groups)
        for k in GROUPS:
            place = k, slice(Q * u, Q * (u + 1)), slice(B * col, B * (col + 1))
            val = part[:, B * k:B * (k + 1)]
            acc[place] = acc[place] + val if more else val

    def sum_of(u):
        def put(k, val):
            m_ref[Q * u + B * k:Q * u + B * (k + 1), :B * (u + 1)] = val

        return net.reduce(acc, fwd, end, Q * u, Q, put, width=B * (u + 1))

    for load in loads[U:]:
        load.wait()
    sums = []
    for u in GROUPS[::-1]:
        for col in range(u + 1):
            terms(u, col, range(col, U if col >= 2 else 2))
        if u == 3:
            run(chain(m2, m0, m1, m2, out))
            run(out)
        for col in range(min(u + 1, 2)):
            terms(u, col, range(2, U), True)
        for s in sums:
            step(s)
        sums.append(sum_of(u))
        step(sums[-1])
        run(chain(m1, m0))
    run(*moves, *sums)
    net.drain()


def gradient_kernel(x_ref, own_ref, re_ref, rd_ref, ro_ref, t_ref,
                    wr, terms, acc, fwd, end, dma_sems, send_sems, recv_sems):
    net = Net(send_sems, recv_sems)
    loads = [[(re_ref.at[0:2, B * u:B * (u + 1)], wr.at[0:2, OFF[u]:OFF[u] + B]),
              *[(ref.at[zs, B * u:B * (u + 1)], wr.at[zs, OFF[u] + B:OFF[u] + Q])
                for ref, zs in ((rd_ref, slice(0, 2)), (re_ref, slice(2, U)))]] for u in GROUPS]
    loads[2] += [(ro_ref.at[:, Q:], wr.at[:, OFF[2] + Q:OFF[3]])]
    loads[0] += [(ro_ref.at[:, :Q], wr.at[:, Q:H])]
    sems = iter(range(16))
    loads = [[pltpu.make_async_copy(a, b, dma_sems.at[next(sems)]) for a, b in some] for some in loads]
    for some in loads[::-1]:
        for load in some:
            load.start()
    ready = net.barrier(net.right, net.left, net.partner, *net.zy)
    for i in GROUPS:
        for k, top in enumerate((H, OFF[1] + Q)):
            wr[net.z, top + B * i:top + B * (i + 1), at(B * net.y)] = own_ref[i, :, B * k:B * (k + 1)]
    ready()
    rows_0, rows_1 = net.gather_zy(wr, H, H, Q), net.gather_zy(wr, OFF[1] + Q, H, Q)
    step(rows_1)
    step(rows_0)

    def half_of(u, h, top=0, rows=K):
        width = B * (u + 1)
        some = slice(OFF[u] + top, min(OFF[u] + top + rows, OFF[u] + K - Q * u))
        these = slice(Q * u + top, Q * u + top + some.stop - some.start)

        def two(x, _):
            a, b = wr[2 * h + x // 2, some, at(Q * lax.rem(x, 2), Q)], x_ref[these, :width]
            part = mm_t(a, b) if u else mm_t(b, a)
            for e in range(2):
                place = x, e, slice(Q * u + B * h, Q * u + B * (h + 1)), slice(0, width)
                val = part[B * e:B * (e + 1)] if u else part[:, B * e:B * (e + 1)].T
                terms[place] = terms[place] + val if top else val
            return 0

        lax.fori_loop(0, U, two, 0)

    def sum_of(u):
        wr[2:, OFF[u]:OFF[u] + B] = jnp.zeros((2, B, H), jnp.float32)
        for load in loads[u]:
            load.wait()
        for top in ((0,) if u else (0, H)):
            for h in range(2):
                half_of(u, h, top, K if u else H)
                yield

        def put(k, val):
            t_ref[B * (2 * u + k):B * (2 * u + k + 1), :B * (u + 1)] = val

        yield from net.reduce(acc, fwd, end, Q * u, Q, put, terms, B * (u + 1))

    s0, s1, s2, s3 = [sum_of(u) for u in GROUPS]
    run(chain(s3, s3, s3, rows_1, s2, s3, rows_1, s2, rows_1, s3, s2, rows_1, s2, s3, rows_0, s1, s2, s1, s1, rows_0, s0, s1, s2,
              s0, s1, rows_0, s1, rows_0, s0, s0, s0, s0, s0, s0))
    run(s2, s1, s0)
    net.drain()


def call(kernel, ident, flops, args, in_specs, outs, out_specs, scratch, sems):
    return pl.pallas_call(
        kernel,
        out_shape=[jax.ShapeDtypeStruct(s, jnp.float32) for s in outs],
        in_specs=in_specs,
        out_specs=out_specs,
        scratch_shapes=[*(pltpu.VMEM(s, jnp.float32) for s in scratch), *(pltpu.SemaphoreType.DMA(s) for s in sems)],
        compiler_params=pltpu.CompilerParams(collective_id=ident, has_side_effects=True, vmem_limit_bytes=67 * 10 ** 6),
        cost_estimate=pl.CostEstimate(flops=flops, bytes_accessed=K, transcendentals=0),
    )(*args)


def solution(mesh):
    def local_pass(fac, bar):
        panel, rows, column = (U, ROWS, H), (U, H, H), (U, R, B, B)
        wide_col, cut = (U, R, B, Q), (2, R, (ROWS - Q) // (2 * R), B)
        lr, wc, a, b = call(
            front_kernel, 0, 1, (fac, bar), [VM, HB], (panel, column, cut, cut), [HB] + [VM] * 3,
            ((K, H), panel, (R, B, K), (R, B, K), (U, Q, Q), (U, 2, ROWS, B), (U, ROWS, B), (2, ROWS // 2, B), (U, ROWS // 2, B)),
            ((U + 1,), (144,), (144,)))
        sy, w, row_e, row_d, row_o, col_3 = call(
            levels_kernel, 1, 1, (lr, bar, wc, a, b), [HB, HB, VM, HB, HB],
            ((U * K, H), (6, U, U, B, B), rows, rows, rows, wide_col), [HB] * 6,
            ((U, K, B), cut, cut, cut, cut, (2, B, B), (2, B, B), (2, H, H), rows, (U, K, H), rows, (K, B), (U, 2 * R, B, B), rows, rows, column, rows,
             wide_col, column, column, wide_col, (U, 2, Q, B), (U, Q, B), (2, B, B), (U, B, B)),
            ((48,), (208,), (208,), (2,), (2,)))
        m, own = call(
            product_kernel, 2, 1, (sy, w, col_3), [HB] * 3, ((K, H), (U, B, Q)), [VM] * 2,
            ((U * K, H), (6, U, U, B, B), wide_col, (2, U, U, B, Q), (U, K, H), (2, H, H), (U, H, H)), ((16,), (48,), (48,)))
        out, = call(
            gradient_kernel, 3, 1, (m, own, row_e, row_d, row_o), [VM] * 2 + [HB] * 3, ((K, H),), [VM],
            (panel, (U, 2, K, H), (U, K, H), (2, H, H), (U, H, H)), ((16,), (64,), (64,)))
        row, col = lax.broadcasted_iota(jnp.int32, (K, 1), 0), lax.broadcasted_iota(jnp.int32, (1, H), 1)
        row_all = (row // B * R + lax.axis_index('row')) * B + row % B
        col_all = (col // B * 2 * R + lax.axis_index('col')) * B + col % B
        return jnp.where(row_all > col_all, out, jnp.where(row_all == col_all, 0.5 * out, 0.0))

    spec = P(('batch', 'row'), 'col')
    return jax.shard_map(local_pass, mesh=mesh, in_specs=(spec, spec), out_specs=spec, check_vma=False)
```
